16 devices in a mesh: dp: 4 (over z, y), sp: 4 (over x, core).
Axes of the slice: x: 2, y: 2, z: 2, core: 2. Of those that a mesh axis runs over, the one named last changes fastest.
Arguments:
- resid: float32 [16, 256, 1536], P('dp', 'sp'), parts along dimension 0
- pre_norm: float32 [2, 1536], replicated
- w_in: bfloat16 [2, 1536, 6448], replicated
- conv_w: float32 [2, 3328, 4], replicated
- conv_b: float32 [2, 3328], replicated
- dt_bias: float32 [2, 48], replicated
- a_log: float32 [2, 48], replicated
- d_skip: float32 [2, 48], replicated
- gate_norm: float32 [2, 1, 3072], replicated
- w_out: bfloat16 [2, 3072, 1536], replicated
Outputs:
- output 1: float32 [16, 256, 1536], P('dp', 'sp'), parts along dimension 0
- output 2: float32 [16, 2, 48, 64, 128], P('dp', None, 'sp'), parts along dimension 0
- output 3: bfloat16 [16, 2, 3328, 3], P('dp'), parts along dimension 0
There are 4 independent parts. The reference program is written for one: setup_inputs(seed, part) draws one part's arguments, and reference() takes and returns one part's arrays. A program takes and returns all parts, laid end to end along the dimension named above; an argument that names none is the same for every part.
All inputs are finite; a program needn't handle non-finite values.
Results may differ from the reference program's by a relative error of at most 0.017486.
Values are sent between devices in bfloat16 or wider.
A program may use at most 1 GiB of HBM per device.

```python
import jax
import jax.numpy as jnp
from jax import lax

D_MODEL = 1536
D_INNER = 3072
NUM_HEADS = 48
HEAD_DIM = 64
NUM_GROUPS = 1
D_STATE = 128
BATCH = 4
SEQ_LEN = 256
LAYERS = 2
CONV_WIDTH = 4
CHUNK = 256

CONV_DIM = D_INNER + 2 * NUM_GROUPS * D_STATE
IN_DIM = D_INNER + CONV_DIM + NUM_HEADS
PER_GROUP = NUM_HEADS // NUM_GROUPS
GROUP_WIDTH = D_INNER // NUM_GROUPS
EPSILON = 1e-5


def setup_inputs(seed: int = 0, part: int = 0) -> dict:
    key = jax.random.key(seed)
    keys = jax.random.split(key, 9)
    part_key = jax.random.fold_in(key, part)
    resid = jax.random.normal(part_key, (BATCH, SEQ_LEN, D_MODEL), jnp.float32)
    pre_norm = jax.random.uniform(keys[0], (LAYERS, D_MODEL), jnp.float32, 0.5, 1.5)
    w_in = (jax.random.normal(keys[1], (LAYERS, D_MODEL, IN_DIM), jnp.float32) * D_MODEL ** -0.5).astype(jnp.bfloat16)
    bc_weight = 1.5 * (SEQ_LEN * D_STATE) ** -0.25
    column_scale = jnp.concatenate([jnp.full((D_INNER,), 0.5, jnp.float32), jnp.full((2 * NUM_GROUPS * D_STATE,), bc_weight, jnp.float32)])
    conv_w = jax.random.normal(keys[2], (LAYERS, CONV_DIM, CONV_WIDTH), jnp.float32) * column_scale[:, None]
    conv_b = jax.random.normal(keys[3], (LAYERS, CONV_DIM), jnp.float32) * 0.5 * column_scale
    dt_bias = jax.random.uniform(keys[4], (LAYERS, NUM_HEADS), jnp.float32, -1.0, 1.0)
    a_log = jnp.log(jax.random.uniform(keys[5], (LAYERS, NUM_HEADS), jnp.float32, 0.5, 2.0) / SEQ_LEN)
    d_skip = jax.random.uniform(keys[6], (LAYERS, NUM_HEADS), jnp.float32, 0.5, 1.5)
    gate_norm = jax.random.uniform(keys[7], (LAYERS, NUM_GROUPS, GROUP_WIDTH), jnp.float32, 0.5, 1.5)
    w_out = (jax.random.normal(keys[8], (LAYERS, D_INNER, D_MODEL), jnp.float32) * D_INNER ** -0.5).astype(jnp.bfloat16)
    return {'resid': resid, 'pre_norm': pre_norm, 'w_in': w_in, 'conv_w': conv_w, 'conv_b': conv_b, 'dt_bias': dt_bias, 'a_log': a_log, 'd_skip': d_skip, 'gate_norm': gate_norm, 'w_out': w_out}


def rms_norm(values, gain_vec):
    mean_sq = jnp.mean(values * values, axis=-1, keepdims=True)
    return values * lax.rsqrt(mean_sq + EPSILON) * gain_vec


def ssd_sequence(x_sequence, dt_sequence, b_sequence, c_sequence, a_neg):
    n_chunks = SEQ_LEN // CHUNK
    x_scaled = (x_sequence * dt_sequence[:, :, None]).reshape(n_chunks, CHUNK, NUM_GROUPS, PER_GROUP, HEAD_DIM)
    log_decay = (dt_sequence * a_neg).reshape(n_chunks, CHUNK, NUM_GROUPS, PER_GROUP)
    b_chunks = b_sequence.reshape(n_chunks, CHUNK, NUM_GROUPS, D_STATE)
    c_chunks = c_sequence.reshape(n_chunks, CHUNK, NUM_GROUPS, D_STATE)
    causal = jnp.arange(CHUNK)[:, None] >= jnp.arange(CHUNK)[None, :]

    def chunk_step(state, chunk_data):
        x_chunk, log_chunk, b_chunk, c_chunk = chunk_data
        cum_log = jnp.cumsum(log_chunk, axis=0)
        cum_heads = jnp.transpose(cum_log, (1, 2, 0))
        log_diff = cum_heads[:, :, :, None] - cum_heads[:, :, None, :]
        decay_mat = jnp.exp(jnp.where(causal, log_diff, -jnp.inf))
        scores = jnp.einsum('tgn,sgn->gts', c_chunk, b_chunk)
        mix_mat = decay_mat * scores[:, None]
        y_intra = jnp.einsum('ghts,sghp->tghp', mix_mat, x_chunk)
        y_inter = jnp.einsum('tgn,ghpn->tghp', c_chunk, state) * jnp.exp(cum_log)[:, :, :, None]
        to_end = jnp.exp(cum_log[-1] - cum_log)
        new_state = state * jnp.exp(cum_log[-1])[:, :, None, None] + jnp.einsum('sghp,sgn->ghpn', x_chunk * to_end[:, :, :, None], b_chunk)
        return new_state, y_intra + y_inter

    state_zero = jnp.zeros((NUM_GROUPS, PER_GROUP, HEAD_DIM, D_STATE), jnp.float32)
    final, y_chunks = lax.scan(chunk_step, state_zero, (x_scaled, log_decay, b_chunks, c_chunks))
    return y_chunks.reshape(SEQ_LEN, NUM_HEADS, HEAD_DIM), final.reshape(NUM_HEADS, HEAD_DIM, D_STATE)


def mamba_layer(resid, pre_w, w_in_l, conv_w_l, conv_b_l, dt_b, a_log_l, d_l, gate_w, w_out_l):
    normed = rms_norm(resid, pre_w).astype(jnp.bfloat16)
    projected = jnp.dot(normed.reshape(-1, D_MODEL), w_in_l, preferred_element_type=jnp.float32).astype(jnp.bfloat16).reshape(BATCH, SEQ_LEN, IN_DIM)
    gate_z = projected[:, :, :D_INNER]
    xbc = projected[:, :, D_INNER:D_INNER + CONV_DIM]
    dt_raw = projected[:, :, D_INNER + CONV_DIM:]
    padded = jnp.pad(xbc, ((0, 0), (CONV_WIDTH - 1, 0), (0, 0))).astype(jnp.float32)
    conv_out = conv_b_l + sum(padded[:, tap_index:tap_index + SEQ_LEN] * conv_w_l[:, tap_index] for tap_index in range(CONV_WIDTH))
    activated = jax.nn.silu(conv_out).astype(jnp.bfloat16)
    x_act = activated[:, :, :D_INNER].reshape(BATCH, SEQ_LEN, NUM_HEADS, HEAD_DIM)
    b_act = activated[:, :, D_INNER:D_INNER + NUM_GROUPS * D_STATE].reshape(BATCH, SEQ_LEN, NUM_GROUPS, D_STATE)
    c_act = activated[:, :, D_INNER + NUM_GROUPS * D_STATE:].reshape(BATCH, SEQ_LEN, NUM_GROUPS, D_STATE)
    delta = jax.nn.softplus(dt_raw.astype(jnp.float32) + dt_b).astype(jnp.bfloat16)
    a_neg = -jnp.exp(a_log_l)

    def one_sequence(seq_parts):
        x_part, dt_part, b_part, c_part = seq_parts
        return ssd_sequence(x_part.astype(jnp.float32), dt_part.astype(jnp.float32), b_part.astype(jnp.float32), c_part.astype(jnp.float32), a_neg)

    y_ssm, final = lax.map(one_sequence, (x_act, delta, b_act, c_act))
    y_full = (y_ssm + d_l[:, None] * x_act.astype(jnp.float32)).astype(jnp.bfloat16)
    gated = y_full.astype(jnp.float32).reshape(BATCH, SEQ_LEN, D_INNER) * jax.nn.silu(gate_z.astype(jnp.float32))
    grouped = gated.reshape(BATCH, SEQ_LEN, NUM_GROUPS, GROUP_WIDTH)
    normed_y = (grouped * lax.rsqrt(jnp.mean(grouped * grouped, axis=-1, keepdims=True) + EPSILON) * gate_w).astype(jnp.bfloat16)
    out_proj = jnp.dot(normed_y.reshape(-1, D_INNER), w_out_l, preferred_element_type=jnp.float32).reshape(BATCH, SEQ_LEN, D_MODEL)
    tail_rows = jnp.swapaxes(xbc[:, SEQ_LEN - (CONV_WIDTH - 1):], 1, 2)
    return resid + out_proj, final, tail_rows


def reference(resid, pre_norm, w_in, conv_w, conv_b, dt_bias, a_log, d_skip, gate_norm, w_out):
    def layer_step(carry, layer_weights):
        pre_w, w_in_l, conv_w_l, conv_b_l, dt_b, a_log_l, d_l, gate_w, w_out_l = layer_weights
        new_resid, final, tail_rows = mamba_layer(carry, pre_w, w_in_l, conv_w_l, conv_b_l, dt_b, a_log_l, d_l, gate_w, w_out_l)
        return new_resid, (final, tail_rows)

    out_resid, (finals, tails) = lax.scan(layer_step, resid, (pre_norm, w_in, conv_w, conv_b, dt_bias, a_log, d_skip, gate_norm, w_out))
    return out_resid, jnp.swapaxes(finals, 0, 1), jnp.swapaxes(tails, 0, 1)
```

```python
import jax
import jax.numpy as jnp
from jax import lax
from jax.experimental import pallas as pl
from jax.experimental.pallas import tpu as pltpu
from jax.sharding import PartitionSpec as P

F32 = jnp.float32
BF16 = jnp.bfloat16
EPSILON = 1e-5
LAYERS = 2
NB = 4
SEG = 64
BLK = 128
HALO = 16
EXT = BLK + HALO
ROWS = HALO + 2 * BLK
D_MODEL = 1536
D_INNER = 3072
CONV_DIM = 3328
HEADS = 48
HALF = 768
LOC = 1536
ACT = LOC + 256
PAIRS = 12
NT = (((1,), (1,)), ((), ()))


def dot(a, b):
    return jnp.dot(a, b, preferred_element_type=F32)


def dot_nt(a, b):
    return lax.dot_general(a, b, NT, preferred_element_type=F32)


def round_bf16(v):
    return v.astype(BF16).astype(F32)


def silu(v):
    half = 0.5 * v
    return half * jnp.tanh(half) + half


def head_row(i):
    return i if i < 12 else i + 12


def kernel(resid_ref, pre_ref, w_in_ref, cw_ref, cb_ref, dtb_ref, alog_ref, dskip_ref, gw_ref, w_out_ref,
           r_out, ssm_out, tail_out,
           hbuf, sz, wz, wx, wbc, wout, raw, act_o, act_r, yloc, ybuf, yrecv, gn, stg, tails, tail_o, tail_r,
           cum_o, cumt_o, cumt_r, dtt_o, dtt_r, cwl, prm,
           wsem, hsend, hrecv, ysend, yrecv_sem, tsend, trecv, osem):
    me = lax.axis_index('sp')
    chip = me // 2
    core = me % 2
    partner = chip * 2 + (1 - core)
    other = (1 - chip) * 2 + core
    chip_f = chip.astype(F32)
    core_f = core.astype(F32)

    def weight_copies(l):
        zc = [pltpu.make_async_copy(w_in_ref.at[l, pl.ds(HALF * j, HALF), :], wz.at[pl.ds(HALF * j, HALF), :], wsem.at[j]) for j in range(4)]
        xc = [pltpu.make_async_copy(w_in_ref.at[l, pl.ds(pl.multiple_of(D_INNER + LOC * b + HALF * core, 16), HALF), :], wx.at[pl.ds(HALF * b, HALF), :], wsem.at[4 + b]) for b in range(2)]
        bc = pltpu.make_async_copy(w_in_ref.at[l, pl.ds(2 * D_INNER, 304), :], wbc.at[pl.ds(0, 304), :], wsem.at[6])
        oc = pltpu.make_async_copy(w_out_ref.at[l], wout, wsem.at[7])
        return zc, xc, bc, oc

    zc0, xc0, bc0, oc0 = weight_copies(0)
    for c in zc0 + xc0 + [bc0, oc0]:
        c.start()

    barrier = pltpu.get_barrier_semaphore()
    for step in range(1, 4):
        pl.semaphore_signal(barrier, inc=1, device_id={'sp': (me + step) % 4}, device_id_type=pl.DeviceIdType.MESH)

    hbuf[:, 0:HALO, :] = jnp.zeros((LAYERS * NB, HALO, D_MODEL), BF16)
    wbc[304:384, :] = jnp.zeros((80, D_MODEL), BF16)
    prm[...] = jnp.zeros((8, 128), F32)
    r_out[...] = resid_ref[...]
    pl.semaphore_wait(barrier, 3)

    own_row = pl.multiple_of(HALO + BLK * chip + SEG * core, 16)
    oth_row = pl.multiple_of(HALO + BLK * (1 - chip) + SEG * core, 16)
    own_blk = pl.multiple_of(BLK * chip, 16)
    oth_blk = pl.multiple_of(BLK * (1 - chip), 16)

    iota_r = lax.broadcasted_iota(jnp.int32, (BLK, BLK), 0)
    iota_c = lax.broadcasted_iota(jnp.int32, (BLK, BLK), 1)

    def remote(src, dst, ssem, rsem, dev):
        return pltpu.make_async_remote_copy(src_ref=src, dst_ref=dst, send_sem=ssem, recv_sem=rsem, device_id={'sp': dev}, device_id_type=pl.DeviceIdType.MESH)

    def layer(l, carry):
        lb = NB * l
        tri = (iota_r >= iota_c).astype(F32)
        low = iota_c < 64

        def norm_body(p, c):
            v = r_out[p]
            ms = jnp.mean(v * v, axis=-1, keepdims=True)
            hbuf[lb + p, pl.ds(own_row, SEG), :] = (v * lax.rsqrt(ms + EPSILON) * pre_ref[l]).astype(BF16)
            return c
        lax.fori_loop(0, NB, norm_body, 0)

        def hslice(p0, n, row, size):
            return hbuf.at[pl.ds(lb + p0, n), pl.ds(row, size), :]

        def same(idx, p0, n, row, size, dev):
            s = hslice(p0, n, row, size)
            return remote(s, s, hsend.at[l, idx], hrecv.at[l, idx], dev)

        c_par = same(0, 0, NB, own_row, SEG, partner)
        c_tail = same(1, 0, NB, own_row + 48, 16, other)
        c_r0 = same(2, 0, 2, own_row, 48, other)
        c_r1 = same(3, 2, 2, own_row, 48, other)
        f_tail = same(4, 0, NB, oth_row + 48, 16, partner)
        f_r0 = same(5, 0, 2, oth_row, 48, partner)
        f_r1 = same(6, 2, 2, oth_row, 48, partner)
        c_tail.start()
        c_par.start()
        c_r0.start()
        c_r1.start()

        zc, xc, bc, oc = weight_copies(l)
        znx, xnx, bnx, onx = weight_copies(1)

        for b in range(2):
            src = pl.multiple_of(LOC * b + HALF * core, 128)
            cwl[0:4, HALF * b:HALF * (b + 1)] = cw_ref[l, :, pl.ds(src, HALF)]
            cwl[4:5, HALF * b:HALF * (b + 1)] = cb_ref[l, :, pl.ds(src, HALF)]
        cwl[0:4, LOC:ACT] = cw_ref[l, :, D_INNER:CONV_DIM]
        cwl[4:5, LOC:ACT] = cb_ref[l, :, D_INNER:CONV_DIM]
        prm[0:1, 0:HEADS] = dtb_ref[l]
        prm[1:2, 0:HEADS] = -jnp.exp(alog_ref[l])

        for c in zc:
            c.wait()

        def z_body(n, c):
            lhs = hbuf[pl.ds(lb, NB), pl.ds(own_row, SEG), :].reshape(NB * SEG, D_MODEL)
            z = round_bf16(dot_nt(lhs, wz[pl.ds(pl.multiple_of(512 * n, 512), 512), :]))
            sz[:, :, pl.ds(pl.multiple_of(512 * n, 512), 512)] = silu(z).reshape(NB, SEG, 512)
            return c
        lax.fori_loop(0, 6, z_body, 0)

        @pl.when(l == 0)
        def _():
            for c in znx:
                c.start()

        def conv_chunk(act, i, p, src_col, dst_col, width):
            for s in range(width // 128):
                cols = pl.ds(src_col + 128 * s, 128)
                dcol = pl.ds(dst_col + 128 * s if isinstance(dst_col, int) else pl.multiple_of(dst_col + 128 * s, 128), 128)
                acc = cwl[0:1, dcol] * raw[i, 13:141, cols]
                for k in range(1, 4):
                    acc = acc + cwl[k:k + 1, dcol] * raw[i, 13 + k:141 + k, cols]
                act[p, :, dcol] = silu(acc + cwl[4:5, dcol]).astype(BF16)

        def block(p0, np_, row, act, tail, cumt, dtt, cum):
            def lhs():
                return hbuf[pl.ds(lb + p0, np_), pl.ds(row, EXT), :].reshape(np_ * EXT, D_MODEL)

            raw[0:np_, :, 0:384] = round_bf16(dot_nt(lhs(), wbc[...])).reshape(np_, EXT, 384)

            def bc_body(i, c):
                p = p0 + i
                tail[p, :, LOC:ACT] = raw[i, BLK:EXT, 0:256].astype(BF16)
                conv_chunk(act, i, p, 0, LOC, 256)
                v = raw[i, HALO:EXT, 256:384] + prm[0:1, :]
                dt = round_bf16(jnp.maximum(v, 0.0) + jnp.log1p(jnp.exp(-jnp.abs(v))))
                logs = dt * prm[1:2, :]
                dt = dt * (1.0 - core_f) + pltpu.roll(dt, 116, 1) * core_f
                logs = logs * (1.0 - core_f) + pltpu.roll(logs, 116, 1) * core_f
                cums = jnp.dot(tri, logs, precision=lax.Precision.HIGHEST, preferred_element_type=F32)
                cumt[p] = cums.T[0:40]
                dtt[p] = dt.T[0:40]
                if cum is not None:
                    cum[p] = cums
                return c
            lax.fori_loop(0, np_, bc_body, 0)

            def x_body(n, c):
                col = pl.multiple_of(512 * n, 512)
                raw[0:np_, :, :] = round_bf16(dot_nt(lhs(), wx[pl.ds(col, 512), :])).reshape(np_, EXT, 512)

                def conv_body(i, cc):
                    tail[p0 + i, :, pl.ds(col, 512)] = raw[i, BLK:EXT, :].astype(BF16)
                    conv_chunk(act, i, p0 + i, 0, col, 512)
                    return cc
                lax.fori_loop(0, np_, conv_body, 0)
                return c
            lax.fori_loop(0, 3, x_body, 0)

        c_par.wait_recv()
        c_tail.wait_recv()
        f_tail.start()
        bc.wait()
        for c in xc:
            c.wait()
        f_tail.wait_recv()
        block(0, NB, own_blk, act_o, tail_o, cumt_o, dtt_o, cum_o)
        c_r0.wait_recv()
        f_r0.start()

        def intra_body(p, c):
            cb = act_o[p, :, LOC + 128:ACT]
            scores = dot_nt(cb, act_o[p, :, LOC:LOC + 128]) * tri
            for j in range(PAIRS):
                mats = []
                for i in (2 * j, 2 * j + 1):
                    h = head_row(i)
                    col = jnp.broadcast_to(cum_o[p, :, h:h + 1], (BLK, BLK))
                    mats.append(jnp.exp(jnp.minimum(col - cumt_o[p, h:h + 1, :], 0.0)) * (scores * dtt_o[p, h:h + 1, :]))
                xp = act_o[p, :, 128 * j:128 * (j + 1)].astype(F32)
                rhs = jnp.concatenate([jnp.where(low, xp, 0.0), jnp.where(low, 0.0, xp)], axis=0)
                blk = (0 if j < 6 else 24) + 12 * core + (2 * j) % 12
                dv = jnp.where(low[0:1], dskip_ref[l, blk], dskip_ref[l, blk + 1])
                yloc[p, :, 128 * j:128 * (j + 1)] = dot(jnp.concatenate(mats, axis=1), rhs) + dv * xp
            return c
        lax.fori_loop(0, NB, intra_body, 0)

        def y_copy(p):
            src = ybuf.at[p, pl.ds(pl.multiple_of(SEG * (1 - core), 16), SEG), :]
            return remote(src, yrecv.at[lb + p], ysend.at[l, p], yrecv_sem.at[l, p], partner)

        def out_copy(p, ll):
            return pltpu.make_async_copy(stg.at[p], ssm_out.at[p, ll], osem.at[p])

        def decays(p, h, cumt, dtt, extra):
            row = cumt[p, pl.ds(h, 1), :]
            return dtt[p, pl.ds(h, 1), :] * jnp.exp(row[:, 127:128] - row + extra)

        def inter_body(p, c):
            bt = act_r[p, :, LOC:LOC + 128].astype(F32).T
            cf = act_o[p, :, LOC + 128:ACT].astype(F32)
            for j in range(PAIRS):
                ha, hb = head_row(2 * j), head_row(2 * j + 1)
                lhs = jnp.concatenate([bt * decays(p, h, cumt_r, dtt_r, 0.0) for h in (ha, hb)], axis=1)
                xp = act_r[p, :, 128 * j:128 * (j + 1)].astype(F32)
                rhs = jnp.concatenate([jnp.where(low, xp, 0.0), jnp.where(low, 0.0, xp)], axis=0)
                state = dot(lhs, rhs)
                ca = jnp.broadcast_to(cum_o[p, :, ha:ha + 1], (BLK, BLK))
                cb = jnp.broadcast_to(cum_o[p, :, hb:hb + 1], (BLK, BLK))
                y = yloc[p, :, 128 * j:128 * (j + 1)] + chip_f * (dot(cf, state) * jnp.exp(jnp.where(low, ca, cb)))
                ybuf[p, :, 128 * j:128 * (j + 1)] = y.astype(BF16)
            y_copy(p).start()

            @pl.when(l > 0)
            def _():
                out_copy(p, 0).wait()
            bto = act_o[p, :, LOC:LOC + 128].astype(F32).T

            def final_body(q, cc):
                h = 24 * chip + 2 * q
                cols = pl.ds(pl.multiple_of(128 * (6 * chip + q), 128), 128)
                left, right = [], []
                for hh in (h, h + 1):
                    end_o = cumt_o[p, pl.ds(hh, 1), :][:, 127:128]
                    end_r = cumt_r[p, pl.ds(hh, 1), :][:, 127:128]
                    left.append(bto * decays(p, hh, cumt_o, dtt_o, end_r * (1.0 - chip_f)))
                    right.append(bt * decays(p, hh, cumt_r, dtt_r, end_o * chip_f))
                xo = act_o[p, :, cols].astype(F32)
                xr = act_r[p, :, cols].astype(F32)
                rhs = jnp.concatenate([jnp.where(low, xo, 0.0), jnp.where(low, 0.0, xo), jnp.where(low, xr, 0.0), jnp.where(low, 0.0, xr)], axis=0)
                state = dot(jnp.concatenate(left + right, axis=1), rhs)
                stg[p, pl.ds(2 * q, 2)] = state.T.reshape(2, 64, 128)
                return cc
            lax.fori_loop(0, 6, final_body, 0)
            out_copy(p, l).start()
            return c

        c_r1.wait_recv()
        f_r1.start()
        f_r0.wait_recv()
        block(0, 2, oth_blk, act_r, tail_r, cumt_r, dtt_r, None)
        lax.fori_loop(0, 2, inter_body, 0)
        f_r1.wait_recv()
        block(2, 2, oth_blk, act_r, tail_r, cumt_r, dtt_r, None)
        lax.fori_loop(2, NB, inter_body, 0)

        @pl.when(l == 0)
        def _():
            for c in xnx + [bnx]:
                c.start()

        def put_tail(src):
            for b in range(2):
                tails[l, :, :, pl.ds(pl.multiple_of(LOC * b + HALF * core, 128), HALF)] = src[:, :, HALF * b:HALF * (b + 1)]
            tails[l, :, :, D_INNER:CONV_DIM] = src[:, :, LOC:ACT]

        @pl.when(chip == 1)
        def _():
            put_tail(tail_o)

        @pl.when(chip == 0)
        def _():
            put_tail(tail_r)
        t_copies = []
        for b in range(2):
            ts = tails.at[l, :, :, pl.ds(pl.multiple_of(LOC * b + HALF * core, 128), HALF)]
            t_copies.append(remote(ts, ts, tsend.at[l, b], trecv.at[l, b], partner))
        for c in t_copies:
            c.start()

        def gate_body(p, c):
            y_copy(p).wait()
            total = jnp.zeros((SEG, 1), F32)
            for b in range(2):
                for own in range(2):
                    cols = pl.ds(pl.multiple_of(LOC * b + HALF * (core if own else 1 - core), 128), HALF)
                    if own:
                        y = ybuf[p, pl.ds(pl.multiple_of(SEG * core, 16), SEG), HALF * b:HALF * (b + 1)]
                    else:
                        y = yrecv[lb + p, :, HALF * b:HALF * (b + 1)]
                    g = y.astype(F32) * sz[p, :, cols]
                    sz[p, :, cols] = g
                    total = total + jnp.sum(g * g, axis=-1, keepdims=True)
            scale = lax.rsqrt(total * (1.0 / D_INNER) + EPSILON)
            for b in range(4):
                cols = slice(HALF * b, HALF * (b + 1))
                gn[p, :, cols] = (sz[p, :, cols] * scale * gw_ref[l, :, cols]).astype(BF16)
            return c
        lax.fori_loop(0, NB, gate_body, 0)

        oc.wait()

        def out_body(n, c):
            cols = pl.ds(pl.multiple_of(512 * n, 512), 512)
            o = dot(gn[...].reshape(NB * SEG, D_INNER), wout[:, cols])
            r_out[:, :, cols] = r_out[:, :, cols] + o.reshape(NB, SEG, 512)
            return c
        lax.fori_loop(0, 3, out_body, 0)

        @pl.when(l == 0)
        def _():
            onx.start()

        for c in [c_par, c_tail, c_r0, c_r1, f_tail, f_r0, f_r1]:
            c.wait_send()
        for c in t_copies:
            c.wait()
        return carry

    lax.fori_loop(0, LAYERS, layer, 0)
    for p in range(NB):
        pltpu.make_async_copy(stg.at[p], ssm_out.at[p, LAYERS - 1], osem.at[p]).wait()
    tail_out[...] = tails[...]


def solution(mesh):
    vmem = pl.BlockSpec(memory_space=pltpu.VMEM)
    hbm = pl.BlockSpec(memory_space=pl.ANY)
    smem = pl.BlockSpec(memory_space=pltpu.SMEM)

    def forward(resid, pre_norm, w_in, conv_w, conv_b, dt_bias, a_log, d_skip, gate_norm, w_out):
        r, ssm, tails = pl.pallas_call(
            kernel,
            out_shape=(
                jax.ShapeDtypeStruct((NB, SEG, D_MODEL), F32),
                jax.ShapeDtypeStruct((NB, LAYERS, 12, 64, 128), F32),
                jax.ShapeDtypeStruct((LAYERS, NB, 16, CONV_DIM), BF16),
            ),
            in_specs=[vmem, vmem, hbm, vmem, vmem, vmem, vmem, smem, vmem, hbm],
            out_specs=(vmem, hbm, vmem),
            scratch_shapes=[
                pltpu.VMEM((LAYERS * NB, ROWS, D_MODEL), BF16),
                pltpu.VMEM((NB, SEG, D_INNER), F32),
                pltpu.VMEM((D_INNER, D_MODEL), BF16),
                pltpu.VMEM((LOC, D_MODEL), BF16),
                pltpu.VMEM((384, D_MODEL), BF16),
                pltpu.VMEM((D_INNER, D_MODEL), BF16),
                pltpu.VMEM((NB, EXT, 512), F32),
                pltpu.VMEM((NB, BLK, ACT), BF16),
                pltpu.VMEM((NB, BLK, ACT), BF16),
                pltpu.VMEM((NB, BLK, LOC), F32),
                pltpu.VMEM((NB, BLK, LOC), BF16),
                pltpu.VMEM((LAYERS * NB, SEG, LOC), BF16),
                pltpu.VMEM((NB, SEG, D_INNER), BF16),
                pltpu.VMEM((NB, 12, 64, 128), F32),
                pltpu.VMEM((LAYERS, NB, 16, CONV_DIM), BF16),
                pltpu.VMEM((NB, 16, ACT), BF16),
                pltpu.VMEM((NB, 16, ACT), BF16),
                pltpu.VMEM((NB, BLK, BLK), F32),
                pltpu.VMEM((NB, 40, BLK), F32),
                pltpu.VMEM((NB, 40, BLK), F32),
                pltpu.VMEM((NB, 40, BLK), F32),
                pltpu.VMEM((NB, 40, BLK), F32),
                pltpu.VMEM((8, ACT), F32),
                pltpu.VMEM((8, 128), F32),
                pltpu.SemaphoreType.DMA((8,)),
                pltpu.SemaphoreType.DMA((LAYERS, 7)),
                pltpu.SemaphoreType.DMA((LAYERS, 7)),
                pltpu.SemaphoreType.DMA((LAYERS, NB)),
                pltpu.SemaphoreType.DMA((LAYERS, NB)),
                pltpu.SemaphoreType.DMA((LAYERS, 2)),
                pltpu.SemaphoreType.DMA((LAYERS, 2)),
                pltpu.SemaphoreType.DMA((NB,)),
            ],
            compiler_params=pltpu.CompilerParams(collective_id=0, has_side_effects=True, vmem_limit_bytes=67043328),
        )(resid, pre_norm.reshape(LAYERS, 1, D_MODEL), jnp.swapaxes(w_in, 1, 2), jnp.swapaxes(conv_w, 1, 2), conv_b.reshape(LAYERS, 1, CONV_DIM),
          dt_bias.reshape(LAYERS, 1, HEADS), a_log.reshape(LAYERS, 1, HEADS), d_skip, gate_norm, w_out)
        conv_state = jnp.transpose(tails[:, :, 13:16, :], (1, 0, 3, 2))
        return r, ssm, conv_state

    return jax.shard_map(forward, mesh=mesh, in_specs=(P('dp', 'sp', None), P(), P(), P(), P(), P(), P(), P(), P(), P()), out_specs=(P('dp', 'sp', None), P('dp', None, 'sp', None, None), P('dp', None, None, None)), check_vma=False)
```

```python
import jax
import jax.numpy as jnp
from jax import lax
from jax.experimental import pallas as pl
from jax.experimental.pallas import tpu as pltpu
from jax.sharding import PartitionSpec as P

F32 = jnp.float32
BF16 = jnp.bfloat16
EPSILON = 1e-5
LAYERS = 2
NB = 4
SEG = 64
BLK = 128
HALO = 16
EXT = BLK + HALO
ROWS = HALO + 2 * BLK
D_MODEL = 1536
D_INNER = 3072
CONV_DIM = 3328
HEADS = 48
HALF = 768
LOC = 1536
ACT = LOC + 256
PAIRS = 12
NT = (((1,), (1,)), ((), ()))


def dot(a, b):
    return jnp.dot(a, b, preferred_element_type=F32)


def dot_nt(a, b):
    return lax.dot_general(a, b, NT, preferred_element_type=F32)


def round_bf16(v):
    return v.astype(BF16).astype(F32)


def silu(v):
    half = 0.5 * v
    return half * jnp.tanh(half) + half


def head_row(i):
    return i if i < 12 else i + 12


def kernel(resid_ref, pre_ref, w_in_ref, cw_ref, cb_ref, dtb_ref, alog_ref, dskip_ref, gw_ref, w_out_ref,
           r_out, ssm_out, tail_out,
           hbuf, sz, wz, wx, wbc, wout, raw, act_o, act_r, yloc, ybuf, yrecv, gn, stg, tails, tail_o, tail_r,
           cum_o, cumt_o, cumt_r, dtt_o, dtt_r, cwl, prm,
           wsem, hsend, hrecv, ysend, yrecv_sem, tsend, trecv, osem):
    me = lax.axis_index('sp')
    chip = me // 2
    core = me % 2
    partner = chip * 2 + (1 - core)
    other = (1 - chip) * 2 + core
    chip_f = chip.astype(F32)
    core_f = core.astype(F32)

    def weight_copies(l):
        xc = [pltpu.make_async_copy(w_in_ref.at[l, pl.ds(pl.multiple_of(D_INNER + LOC * b + HALF * core, 16), HALF), :], wx.at[pl.ds(HALF * b, HALF), :], wsem.at[6 + b]) for b in range(2)]
        bc = pltpu.make_async_copy(w_in_ref.at[l, pl.ds(2 * D_INNER, 304), :], wbc.at[pl.ds(0, 304), :], wsem.at[8])
        oc = pltpu.make_async_copy(w_out_ref.at[l], wout, wsem.at[9])
        return xc, bc, oc

    def z_copy(l, n):
        rows = pl.ds(pl.multiple_of(512 * n, 16), 512)
        return pltpu.make_async_copy(w_in_ref.at[l, rows, :], wz.at[rows, :], wsem.at[n])

    xc0, bc0, oc0 = weight_copies(0)
    for n in range(6):
        z_copy(0, n).start()

    barrier = pltpu.get_barrier_semaphore()
    for step in range(1, 4):
        pl.semaphore_signal(barrier, inc=1, device_id={'sp': (me + step) % 4}, device_id_type=pl.DeviceIdType.MESH)

    hbuf[:, 0:HALO, :] = jnp.zeros((LAYERS * NB, HALO, D_MODEL), BF16)
    wbc[304:384, :] = jnp.zeros((80, D_MODEL), BF16)
    prm[...] = jnp.zeros((8, 128), F32)
    r_out[...] = resid_ref[...]
    for c in [bc0] + xc0:
        c.start()
    with jax.named_scope('barrier'):
        pl.semaphore_wait(barrier, 3)

    own_row = pl.multiple_of(HALO + BLK * chip + SEG * core, 16)
    oth_row = pl.multiple_of(HALO + BLK * (1 - chip) + SEG * core, 16)
    own_blk = pl.multiple_of(BLK * chip, 16)
    oth_blk = pl.multiple_of(BLK * (1 - chip), 16)

    iota_r = lax.broadcasted_iota(jnp.int32, (BLK, BLK), 0)
    iota_c = lax.broadcasted_iota(jnp.int32, (BLK, BLK), 1)

    def remote(src, dst, ssem, rsem, dev):
        return pltpu.make_async_remote_copy(src_ref=src, dst_ref=dst, send_sem=ssem, recv_sem=rsem, device_id={'sp': dev}, device_id_type=pl.DeviceIdType.MESH)

    def layer(l, carry):
        lb = NB * l
        tri = (iota_r >= iota_c).astype(F32)
        low = iota_c < 64

        def norm_body(p, c):
            v = r_out[p]
            ms = jnp.mean(v * v, axis=-1, keepdims=True)
            hbuf[lb + p, pl.ds(own_row, SEG), :] = (v * lax.rsqrt(ms + EPSILON) * pre_ref[pl.ds(l, 1), :]).astype(BF16)
            return c
        with jax.named_scope('norm'):
            lax.fori_loop(0, NB, norm_body, 0)

        def hslice(p0, n, row, size):
            return hbuf.at[pl.ds(lb + p0, n), pl.ds(row, size), :]

        def same(idx, p0, n, row, size, dev):
            s = hslice(p0, n, row, size)
            return remote(s, s, hsend.at[l, idx], hrecv.at[l, idx], dev)

        c_par = same(0, 0, NB, own_row, SEG, partner)
        c_tail = same(1, 0, NB, own_row + 48, 16, other)
        c_r0 = same(2, 0, 2, own_row, 48, other)
        c_r1 = same(3, 2, 2, own_row, 48, other)
        f_tail = same(4, 0, NB, oth_row + 48, 16, partner)
        f_r0 = same(5, 0, 2, oth_row, 48, partner)
        f_r1 = same(6, 2, 2, oth_row, 48, partner)
        c_tail.start()
        c_par.start()
        c_r0.start()
        c_r1.start()

        xc, bc, oc = weight_copies(l)
        xnx, bnx, onx = weight_copies(1)

        for b in range(2):
            src = pl.multiple_of(LOC * b + HALF * core, 128)
            cwl[0:4, HALF * b:HALF * (b + 1)] = cw_ref[l, :, pl.ds(src, HALF)]
            cwl[4:5, HALF * b:HALF * (b + 1)] = cb_ref[pl.ds(l, 1), pl.ds(src, HALF)]
        cwl[0:4, LOC:ACT] = cw_ref[l, :, D_INNER:CONV_DIM]
        cwl[4:5, LOC:ACT] = cb_ref[pl.ds(l, 1), D_INNER:CONV_DIM]
        prm[0:1, 0:HEADS] = dtb_ref[pl.ds(l, 1), :]
        prm[1:2, 0:HEADS] = -jnp.exp(alog_ref[pl.ds(l, 1), :])

        def z_body(n, c):
            z_copy(l, n).wait()
            lhs = hbuf[pl.ds(lb, NB), pl.ds(own_row, SEG), :].reshape(NB * SEG, D_MODEL)
            z = round_bf16(dot_nt(lhs, wz[pl.ds(pl.multiple_of(512 * n, 512), 512), :]))
            sz[:, :, pl.ds(pl.multiple_of(512 * n, 512), 512)] = silu(z).reshape(NB, SEG, 512)
            return c
        with jax.named_scope('zproj'):
            lax.fori_loop(0, 6, z_body, 0)

        @pl.when(l == 0)
        def _():
            oc.start()
            for n in range(6):
                z_copy(1, n).start()

        def conv_chunk(act, i, p, src_col, dst_col, width):
            for s in range(width // 128):
                cols = pl.ds(src_col + 128 * s, 128)
                dcol = pl.ds(dst_col + 128 * s if isinstance(dst_col, int) else pl.multiple_of(dst_col + 128 * s, 128), 128)
                acc = cwl[0:1, dcol] * raw[i, 13:141, cols]
                for k in range(1, 4):
                    acc = acc + cwl[k:k + 1, dcol] * raw[i, 13 + k:141 + k, cols]
                act[p, :, dcol] = silu(acc + cwl[4:5, dcol]).astype(BF16)

        def block(p0, np_, row, act, tail, cumt, dtt, cum):
            def lhs():
                return hbuf[pl.ds(lb + p0, np_), pl.ds(row, EXT), :].reshape(np_ * EXT, D_MODEL)

            raw[0:np_, :, 0:384] = round_bf16(dot_nt(lhs(), wbc[...])).reshape(np_, EXT, 384)

            def bc_body(i, c):
                p = p0 + i
                tail[p, :, LOC:ACT] = raw[i, BLK:EXT, 0:256].astype(BF16)
                conv_chunk(act, i, p, 0, LOC, 256)
                v = raw[i, HALO:EXT, 256:384] + prm[0:1, :]
                dt = round_bf16(jnp.maximum(v, 0.0) + jnp.log1p(jnp.exp(-jnp.abs(v))))
                logs = dt * prm[1:2, :]
                dt = dt * (1.0 - core_f) + pltpu.roll(dt, 116, 1) * core_f
                logs = logs * (1.0 - core_f) + pltpu.roll(logs, 116, 1) * core_f
                cums = jnp.dot(tri, logs, precision=lax.Precision.HIGHEST, preferred_element_type=F32)
                cumt[p] = cums.T[0:40]
                dtt[p] = dt.T[0:40]
                if cum is not None:
                    cum[p] = cums
                return c
            lax.fori_loop(0, np_, bc_body, 0)

            def x_body(n, c):
                col = pl.multiple_of(512 * n, 512)
                raw[0:np_, :, :] = round_bf16(dot_nt(lhs(), wx[pl.ds(col, 512), :])).reshape(np_, EXT, 512)

                def conv_body(i, cc):
                    tail[p0 + i, :, pl.ds(col, 512)] = raw[i, BLK:EXT, :].astype(BF16)
                    conv_chunk(act, i, p0 + i, 0, col, 512)
                    return cc
                lax.fori_loop(0, np_, conv_body, 0)
                return c
            lax.fori_loop(0, 3, x_body, 0)

        with jax.named_scope('wait_h'):
            c_par.wait_recv()
            c_tail.wait_recv()
            f_tail.start()
        with jax.named_scope('wait_wx'):
            bc.wait()
            for c in xc:
                c.wait()
        with jax.named_scope('wait_tail'):
            f_tail.wait_recv()
        with jax.named_scope('own_block'):
            block(0, NB, own_blk, act_o, tail_o, cumt_o, dtt_o, cum_o)
        with jax.named_scope('wait_r0'):
            c_r0.wait_recv()
            f_r0.start()

        def intra_body(p, c):
            cb = act_o[p, :, LOC + 128:ACT]
            scores = dot_nt(cb, act_o[p, :, LOC:LOC + 128]) * tri
            for j in range(PAIRS):
                mats = []
                for i in (2 * j, 2 * j + 1):
                    h = head_row(i)
                    col = jnp.broadcast_to(cum_o[p, :, h:h + 1], (BLK, BLK))
                    mats.append(jnp.exp(jnp.minimum(col - cumt_o[p, h:h + 1, :], 0.0)) * (scores * dtt_o[p, h:h + 1, :]))
                xp = act_o[p, :, 128 * j:128 * (j + 1)].astype(F32)
                rhs = jnp.concatenate([jnp.where(low, xp, 0.0), jnp.where(low, 0.0, xp)], axis=0)
                blk = (0 if j < 6 else 24) + 12 * core + (2 * j) % 12
                dv = jnp.where(low[0:1], dskip_ref[l, blk], dskip_ref[l, blk + 1])
                yloc[p, :, 128 * j:128 * (j + 1)] = dot(jnp.concatenate(mats, axis=1), rhs) + dv * xp
            return c
        with jax.named_scope('intra'):
            lax.fori_loop(0, NB, intra_body, 0)

        def y_copy(p):
            src = ybuf.at[p, pl.ds(pl.multiple_of(SEG * (1 - core), 16), SEG), :]
            return remote(src, yrecv.at[lb + p], ysend.at[l, p], yrecv_sem.at[l, p], partner)

        def out_copy(p, ll):
            return pltpu.make_async_copy(stg.at[p], ssm_out.at[p, ll], osem.at[p])

        def decays(p, h, cumt, dtt, extra):
            row = cumt[p, pl.ds(h, 1), :]
            return dtt[p, pl.ds(h, 1), :] * jnp.exp(row[:, 127:128] - row + extra)

        def inter_body(p, c):
            bt = act_r[p, :, LOC:LOC + 128].astype(F32).T
            cf = act_o[p, :, LOC + 128:ACT].astype(F32)
            for j in range(PAIRS):
                ha, hb = head_row(2 * j), head_row(2 * j + 1)
                lhs = jnp.concatenate([bt * decays(p, h, cumt_r, dtt_r, 0.0) for h in (ha, hb)], axis=1)
                xp = act_r[p, :, 128 * j:128 * (j + 1)].astype(F32)
                rhs = jnp.concatenate([jnp.where(low, xp, 0.0), jnp.where(low, 0.0, xp)], axis=0)
                state = dot(lhs, rhs)
                ca = jnp.broadcast_to(cum_o[p, :, ha:ha + 1], (BLK, BLK))
                cb = jnp.broadcast_to(cum_o[p, :, hb:hb + 1], (BLK, BLK))
                y = yloc[p, :, 128 * j:128 * (j + 1)] + chip_f * (dot(cf, state) * jnp.exp(jnp.where(low, ca, cb)))
                ybuf[p, :, 128 * j:128 * (j + 1)] = y.astype(BF16)
            y_copy(p).start()

            @pl.when(l > 0)
            def _():
                out_copy(p, 0).wait()
            bto = act_o[p, :, LOC:LOC + 128].astype(F32).T

            def final_body(q, cc):
                h = 24 * chip + 2 * q
                cols = pl.ds(pl.multiple_of(128 * (6 * chip + q), 128), 128)
                left, right = [], []
                for hh in (h, h + 1):
                    end_o = cumt_o[p, pl.ds(hh, 1), :][:, 127:128]
                    end_r = cumt_r[p, pl.ds(hh, 1), :][:, 127:128]
                    left.append(bto * decays(p, hh, cumt_o, dtt_o, end_r * (1.0 - chip_f)))
                    right.append(bt * decays(p, hh, cumt_r, dtt_r, end_o * chip_f))
                xo = act_o[p, :, cols].astype(F32)
                xr = act_r[p, :, cols].astype(F32)
                rhs = jnp.concatenate([jnp.where(low, xo, 0.0), jnp.where(low, 0.0, xo), jnp.where(low, xr, 0.0), jnp.where(low, 0.0, xr)], axis=0)
                state = dot(jnp.concatenate(left + right, axis=1), rhs)
                stg[p, pl.ds(2 * q, 2)] = state.T.reshape(2, 64, 128)
                return cc
            lax.fori_loop(0, 6, final_body, 0)
            out_copy(p, l).start()
            return c

        with jax.named_scope('wait_f0'):
            f_r0.wait_recv()
        with jax.named_scope('oth_block0'):
            block(0, 2, oth_blk, act_r, tail_r, cumt_r, dtt_r, None)
        with jax.named_scope('inter0'):
            lax.fori_loop(0, 2, inter_body, 0)
        with jax.named_scope('wait_r1'):
            c_r1.wait_recv()
            f_r1.start()
            f_r1.wait_recv()
        with jax.named_scope('oth_block1'):
            block(2, 2, oth_blk, act_r, tail_r, cumt_r, dtt_r, None)
        with jax.named_scope('inter1'):
            lax.fori_loop(2, NB, inter_body, 0)

        @pl.when(l == 0)
        def _():
            for c in xnx + [bnx]:
                c.start()

        def put_tail(src):
            for b in range(2):
                tails[l, :, :, pl.ds(pl.multiple_of(LOC * b + HALF * core, 128), HALF)] = src[:, :, HALF * b:HALF * (b + 1)]
            tails[l, :, :, D_INNER:CONV_DIM] = src[:, :, LOC:ACT]

        @pl.when(chip == 1)
        def _():
            put_tail(tail_o)

        @pl.when(chip == 0)
        def _():
            put_tail(tail_r)
        t_copies = []
        for b in range(2):
            ts = tails.at[l, :, :, pl.ds(pl.multiple_of(LOC * b + HALF * core, 128), HALF)]
            t_copies.append(remote(ts, ts, tsend.at[l, b], trecv.at[l, b], partner))
        for c in t_copies:
            c.start()

        def gate_body(p, c):
            y_copy(p).wait()
            total = jnp.zeros((SEG, 1), F32)
            for b in range(2):
                for own in range(2):
                    cols = pl.ds(pl.multiple_of(LOC * b + HALF * (core if own else 1 - core), 128), HALF)
                    if own:
                        y = ybuf[p, pl.ds(pl.multiple_of(SEG * core, 16), SEG), HALF * b:HALF * (b + 1)]
                    else:
                        y = yrecv[lb + p, :, HALF * b:HALF * (b + 1)]
                    g = y.astype(F32) * sz[p, :, cols]
                    sz[p, :, cols] = g
                    total = total + jnp.sum(g * g, axis=-1, keepdims=True)
            scale = lax.rsqrt(total * (1.0 / D_INNER) + EPSILON)
            for b in range(4):
                cols = slice(HALF * b, HALF * (b + 1))
                gn[p, :, cols] = (sz[p, :, cols] * scale * gw_ref[l, :, cols]).astype(BF16)
            return c
        with jax.named_scope('gate'):
            lax.fori_loop(0, NB, gate_body, 0)

        with jax.named_scope('wait_wout'):
            oc.wait()

        def out_body(n, c):
            cols = pl.ds(pl.multiple_of(512 * n, 512), 512)
            o = dot(gn[...].reshape(NB * SEG, D_INNER), wout[:, cols])
            r_out[:, :, cols] = r_out[:, :, cols] + o.reshape(NB, SEG, 512)
            return c
        with jax.named_scope('outproj'):
            lax.fori_loop(0, 3, out_body, 0)

        @pl.when(l == 0)
        def _():
            onx.start()

        with jax.named_scope('wait_end'):
            for c in [c_par, c_tail, c_r0, c_r1, f_tail, f_r0, f_r1]:
                c.wait_send()
            for c in t_copies:
                c.wait()
        return carry

    lax.fori_loop(0, LAYERS, layer, 0)
    for p in range(NB):
        pltpu.make_async_copy(stg.at[p], ssm_out.at[p, LAYERS - 1], osem.at[p]).wait()
    tail_out[...] = tails[...]


def solution(mesh):
    vmem = pl.BlockSpec(memory_space=pltpu.VMEM)
    hbm = pl.BlockSpec(memory_space=pl.ANY)
    smem = pl.BlockSpec(memory_space=pltpu.SMEM)

    def forward(resid, pre_norm, w_in, conv_w, conv_b, dt_bias, a_log, d_skip, gate_norm, w_out):
        r, ssm, tails = pl.pallas_call(
            kernel,
            out_shape=(
                jax.ShapeDtypeStruct((NB, SEG, D_MODEL), F32),
                jax.ShapeDtypeStruct((NB, LAYERS, 12, 64, 128), F32),
                jax.ShapeDtypeStruct((LAYERS, NB, 16, CONV_DIM), BF16),
            ),
            in_specs=[vmem, vmem, hbm, vmem, vmem, vmem, vmem, smem, vmem, hbm],
            out_specs=(vmem, hbm, vmem),
            scratch_shapes=[
                pltpu.VMEM((LAYERS * NB, ROWS, D_MODEL), BF16),
                pltpu.VMEM((NB, SEG, D_INNER), F32),
                pltpu.VMEM((D_INNER, D_MODEL), BF16),
                pltpu.VMEM((LOC, D_MODEL), BF16),
                pltpu.VMEM((384, D_MODEL), BF16),
                pltpu.VMEM((D_INNER, D_MODEL), BF16),
                pltpu.VMEM((NB, EXT, 512), F32),
                pltpu.VMEM((NB, BLK, ACT), BF16),
                pltpu.VMEM((NB, BLK, ACT), BF16),
                pltpu.VMEM((NB, BLK, LOC), F32),
                pltpu.VMEM((NB, BLK, LOC), BF16),
                pltpu.VMEM((LAYERS * NB, SEG, LOC), BF16),
                pltpu.VMEM((NB, SEG, D_INNER), BF16),
                pltpu.VMEM((NB, 12, 64, 128), F32),
                pltpu.VMEM((LAYERS, NB, 16, CONV_DIM), BF16),
                pltpu.VMEM((NB, 16, ACT), BF16),
                pltpu.VMEM((NB, 16, ACT), BF16),
                pltpu.VMEM((NB, BLK, BLK), F32),
                pltpu.VMEM((NB, 40, BLK), F32),
                pltpu.VMEM((NB, 40, BLK), F32),
                pltpu.VMEM((NB, 40, BLK), F32),
                pltpu.VMEM((NB, 40, BLK), F32),
                pltpu.VMEM((8, ACT), F32),
                pltpu.VMEM((8, 128), F32),
                pltpu.SemaphoreType.DMA((10,)),
                pltpu.SemaphoreType.DMA((LAYERS, 7)),
                pltpu.SemaphoreType.DMA((LAYERS, 7)),
                pltpu.SemaphoreType.DMA((LAYERS, NB)),
                pltpu.SemaphoreType.DMA((LAYERS, NB)),
                pltpu.SemaphoreType.DMA((LAYERS, 2)),
                pltpu.SemaphoreType.DMA((LAYERS, 2)),
                pltpu.SemaphoreType.DMA((NB,)),
            ],
            compiler_params=pltpu.CompilerParams(collective_id=0, has_side_effects=True, vmem_limit_bytes=67043328),
        )(resid, pre_norm, jnp.swapaxes(w_in, 1, 2), jnp.swapaxes(conv_w, 1, 2), conv_b, dt_bias, a_log, d_skip, gate_norm, w_out)
        conv_state = jnp.transpose(tails[:, :, 13:16, :], (1, 0, 3, 2))
        return r, ssm, conv_state

    return jax.shard_map(forward, mesh=mesh, in_specs=(P('dp', 'sp', None), P(), P(), P(), P(), P(), P(), P(), P(), P()), out_specs=(P('dp', 'sp', None), P('dp', None, 'sp', None, None), P('dp', None, None, None)), check_vma=False)
```

```python
import jax
import jax.numpy as jnp
from jax import lax
from jax.experimental import pallas as pl
from jax.experimental.pallas import tpu as pltpu
from jax.sharding import PartitionSpec as P

F32 = jnp.float32
BF16 = jnp.bfloat16
EPSILON = 1e-5
LAYERS = 2
NB = 4
SEG = 64
BLK = 128
HALO = 16
EXT = BLK + HALO
ROWS = HALO + 2 * BLK
D_MODEL = 1536
D_INNER = 3072
CONV_DIM = 3328
HEADS = 48
HALF = 768
LOC = 1536
ACT = LOC + 256
PAIRS = 12
NT = (((1,), (1,)), ((), ()))


def dot(a, b):
    return jnp.dot(a, b, preferred_element_type=F32)


def dot_nt(a, b):
    return lax.dot_general(a, b, NT, preferred_element_type=F32)


def round_bf16(v):
    return v.astype(BF16).astype(F32)


def silu(v):
    half = 0.5 * v
    return half * jnp.tanh(half) + half


def head_row(i):
    return i if i < 12 else i + 12


def kernel(resid_ref, pre_ref, w_in_ref, cw_ref, cb_ref, dtb_ref, alog_ref, dskip_ref, gw_ref, w_out_ref,
           r_out, ssm_out, tail_out,
           hbuf, sz, wz, wx, wbc, wout, rawa, rawb, states, act_o, act_r, yloc, ybuf, yrecv, gn, stg, tails, tail_o, tail_r,
           cum_o, cumt_o, cumt_r, dtt_o, dtt_r, cwl, prm,
           wsem, hsend, hrecv, ysend, yrecv_sem, tsend, trecv, osem):
    me = lax.axis_index('sp')
    chip = me // 2
    core = me % 2
    partner = chip * 2 + (1 - core)
    other = (1 - chip) * 2 + core
    chip_f = chip.astype(F32)
    core_f = core.astype(F32)

    def weight_copies(l):
        xc = [pltpu.make_async_copy(w_in_ref.at[l, pl.ds(pl.multiple_of(D_INNER + LOC * b + HALF * core, 16), HALF), :], wx.at[pl.ds(HALF * b, HALF), :], wsem.at[6 + b]) for b in range(2)]
        bc = pltpu.make_async_copy(w_in_ref.at[l, pl.ds(2 * D_INNER, 304), :], wbc.at[pl.ds(0, 304), :], wsem.at[8])
        oc = pltpu.make_async_copy(w_out_ref.at[l], wout, wsem.at[9])
        return xc, bc, oc

    def z_copy(l, n):
        rows = pl.ds(pl.multiple_of(512 * n, 16), 512)
        return pltpu.make_async_copy(w_in_ref.at[l, rows, :], wz.at[rows, :], wsem.at[n])

    xc0, bc0, oc0 = weight_copies(0)
    for n in range(6):
        z_copy(0, n).start()

    barrier = pltpu.get_barrier_semaphore()
    for step in range(1, 4):
        pl.semaphore_signal(barrier, inc=1, device_id={'sp': (me + step) % 4}, device_id_type=pl.DeviceIdType.MESH)

    hbuf[:, 0:HALO, :] = jnp.zeros((LAYERS * NB, HALO, D_MODEL), BF16)
    wbc[304:384, :] = jnp.zeros((80, D_MODEL), BF16)
    prm[...] = jnp.zeros((8, 128), F32)
    r_out[...] = resid_ref[...]
    for c in [bc0] + xc0:
        c.start()
    with jax.named_scope('barrier'):
        pl.semaphore_wait(barrier, 3)

    own_row = pl.multiple_of(HALO + BLK * chip + SEG * core, 16)
    oth_row = pl.multiple_of(HALO + BLK * (1 - chip) + SEG * core, 16)
    own_blk = pl.multiple_of(BLK * chip, 16)
    oth_blk = pl.multiple_of(BLK * (1 - chip), 16)

    iota_r = lax.broadcasted_iota(jnp.int32, (BLK, BLK), 0)
    iota_c = lax.broadcasted_iota(jnp.int32, (BLK, BLK), 1)

    def remote(src, dst, ssem, rsem, dev):
        return pltpu.make_async_remote_copy(src_ref=src, dst_ref=dst, send_sem=ssem, recv_sem=rsem, device_id={'sp': dev}, device_id_type=pl.DeviceIdType.MESH)

    tri = (iota_r >= iota_c).astype(F32)
    low = iota_c < 64

    def hslice(l, p0, n, row, size):
        return hbuf.at[pl.ds(NB * l + p0, n), pl.ds(row, size), :]

    def same(l, idx, p0, n, row, size, dev):
        ref = hslice(l, p0, n, row, size)
        return remote(ref, ref, hsend.at[l, idx], hrecv.at[l, idx], dev)

    def c_par(l):
        return same(l, 0, 0, NB, own_row, SEG, partner)

    def c_tail(l):
        return same(l, 1, 0, NB, own_row + 48, 16, other)

    def c_half(l, half):
        return same(l, 2 + half, 2 * half, 2, own_row, 48, other)

    def f_tail(l):
        return same(l, 4, 0, NB, oth_row + 48, 16, partner)

    def f_half(l, half):
        return same(l, 5 + half, 2 * half, 2, oth_row, 48, partner)

    def y_copy(l, p):
        src = ybuf.at[p, pl.ds(pl.multiple_of(SEG * (1 - core), 16), SEG), :]
        return remote(src, yrecv.at[NB * l + p], ysend.at[l, p], yrecv_sem.at[l, p], partner)

    def out_copy(l, p):
        return pltpu.make_async_copy(stg.at[p], ssm_out.at[p, l], osem.at[p])

    def tail_copies(l):
        res = []
        for b in range(2):
            ref = tails.at[l, :, :, pl.ds(pl.multiple_of(LOC * b + HALF * core, 128), HALF)]
            res.append(remote(ref, ref, tsend.at[l, b], trecv.at[l, b], partner))
        return res

    def conv_chunk(act, src, groups, i, p, dst):
        for g in range(groups):
            cols = slice(dst + 128 * g, dst + 128 * (g + 1))
            acc = cwl[0:1, cols] * src[g, i, 13:141, :]
            for k in range(1, 4):
                acc = acc + cwl[k:k + 1, cols] * src[g, i, 13 + k:141 + k, :]
            act[p, :, cols] = silu(acc + cwl[4:5, cols]).astype(BF16)

    def block(l, p0, np_, row, act, tail, cumt, dtt, cum):
        def project(w, rows, dst):
            lhs = hbuf[pl.ds(NB * l + p0, np_), pl.ds(row, EXT), :].reshape(np_ * EXT, D_MODEL)
            res = round_bf16(dot_nt(lhs, w[rows, :]))
            for g in range((rows.stop - rows.start) // 128):
                dst[g, 0:np_] = res[:, 128 * g:128 * (g + 1)].reshape(np_, EXT, 128)

        def finish_bc(src):
            for i in range(np_):
                p = p0 + i
                for g in range(2):
                    tail[p, :, LOC + 128 * g:LOC + 128 * (g + 1)] = src[g, i, BLK:EXT, :].astype(BF16)
                conv_chunk(act, src, 2, i, p, LOC)
                v = src[2, i, HALO:EXT, :] + prm[0:1, :]
                dt = round_bf16(jnp.maximum(v, 0.0) + jnp.log1p(jnp.exp(-jnp.abs(v))))
                logs = dt * prm[1:2, :]
                dt = dt * (1.0 - core_f) + pltpu.roll(dt, 116, 1) * core_f
                logs = logs * (1.0 - core_f) + pltpu.roll(logs, 116, 1) * core_f
                cums = jnp.dot(tri, logs, precision=lax.Precision.HIGHEST, preferred_element_type=F32)
                cumt[p] = cums.T[0:40]
                dtt[p] = dt.T[0:40]
                if cum is not None:
                    cum[p] = cums

        def finish_x(src, n):
            for i in range(np_):
                for g in range(4):
                    tail[p0 + i, :, 512 * n + 128 * g:512 * n + 128 * (g + 1)] = src[g, i, BLK:EXT, :].astype(BF16)
                conv_chunk(act, src, 4, i, p0 + i, 512 * n)

        project(wbc, slice(0, 384), rawa)
        project(wx, slice(0, 512), rawb)
        finish_bc(rawa)
        project(wx, slice(512, 1024), rawa)
        finish_x(rawb, 0)
        project(wx, slice(1024, 1536), rawb)
        finish_x(rawa, 1)
        finish_x(rawb, 2)

    zero = jnp.zeros((), BF16)

    def split_pair(xp):
        return [jnp.where(low, xp, zero), jnp.where(low, zero, xp)]

    def decays(p, h, cumt, dtt, extra):
        row = cumt[p, pl.ds(h, 1), :]
        return dtt[p, pl.ds(h, 1), :] * jnp.exp(row[:, 127:128] - row + extra)

    def intra_body(l, p):
        cb = act_o[p, :, LOC + 128:ACT]
        scores = dot_nt(cb, act_o[p, :, LOC:LOC + 128]) * tri
        for j in range(PAIRS):
            mats = []
            for i in (2 * j, 2 * j + 1):
                h = head_row(i)
                col = jnp.broadcast_to(cum_o[p, :, h:h + 1], (BLK, BLK))
                mats.append((jnp.exp(jnp.minimum(col - cumt_o[p, h:h + 1, :], 0.0)) * (scores * dtt_o[p, h:h + 1, :])).astype(BF16))
            xp = act_o[p, :, 128 * j:128 * (j + 1)]
            blk = (0 if j < 6 else 24) + 12 * core + (2 * j) % 12
            dv = jnp.where(low[0:1], dskip_ref[l, blk], dskip_ref[l, blk + 1])
            y = dot(jnp.concatenate(mats, axis=1), jnp.concatenate(split_pair(xp), axis=0)) + dv * xp.astype(F32)
            yloc[p, :, 128 * j:128 * (j + 1)] = y
            ybuf[p, :, 128 * j:128 * (j + 1)] = y.astype(BF16)

        @pl.when(chip == 0)
        def _():
            y_copy(l, p).start()

    def inter_body(l, p):
        bt = act_r[p, :, LOC:LOC + 128].astype(F32).T
        cf = act_o[p, :, LOC + 128:ACT]
        for j in range(PAIRS):
            lhs = jnp.concatenate([(bt * decays(p, h, cumt_r, dtt_r, 0.0)).astype(BF16) for h in (head_row(2 * j), head_row(2 * j + 1))], axis=1)
            states[:, 128 * j:128 * (j + 1)] = dot(lhs, jnp.concatenate(split_pair(act_r[p, :, 128 * j:128 * (j + 1)]), axis=0))
        for jj in range(PAIRS // 2):
            o = dot(cf, states[:, 256 * jj:256 * (jj + 1)].astype(BF16))
            for s in range(2):
                j = 2 * jj + s
                ha, hb = head_row(2 * j), head_row(2 * j + 1)
                ca = jnp.broadcast_to(cum_o[p, :, ha:ha + 1], (BLK, BLK))
                cb = jnp.broadcast_to(cum_o[p, :, hb:hb + 1], (BLK, BLK))
                y = yloc[p, :, 128 * j:128 * (j + 1)] + o[:, 128 * s:128 * (s + 1)] * jnp.exp(jnp.where(low, ca, cb))
                ybuf[p, :, 128 * j:128 * (j + 1)] = y.astype(BF16)
        y_copy(l, p).start()

    def final_body(l, p):
        @pl.when(l > 0)
        def _():
            out_copy(0, p).wait()
        bto = act_o[p, :, LOC:LOC + 128].astype(F32).T
        btr = act_r[p, :, LOC:LOC + 128].astype(F32).T
        for q in range(6):
            h = 24 * chip + 2 * q
            cols = pl.ds(pl.multiple_of(128 * (6 * chip + q), 128), 128)
            left, right = [], []
            for hh in (h, h + 1):
                end_o = cumt_o[p, pl.ds(hh, 1), :][:, 127:128]
                end_r = cumt_r[p, pl.ds(hh, 1), :][:, 127:128]
                left.append((bto * decays(p, hh, cumt_o, dtt_o, end_r * (1.0 - chip_f))).astype(BF16))
                right.append((btr * decays(p, hh, cumt_r, dtt_r, end_o * chip_f)).astype(BF16))
            rhs = jnp.concatenate(split_pair(act_o[p, :, cols]) + split_pair(act_r[p, :, cols]), axis=0)
            state = dot(jnp.concatenate(left + right, axis=1), rhs)
            stg[p, 2 * q:2 * q + 2] = state.T.reshape(2, 64, 128)
        out_copy(l, p).start()

    def early_tail(l):
        @pl.when(core == 1)
        def _():
            c_tail(l).wait_recv()
            f_tail(l).start()

        @pl.when(core == 0)
        def _():
            f_tail(l).wait_recv()

    def late_tail(l):
        @pl.when(core == 0)
        def _():
            c_tail(l).wait_recv()
            f_tail(l).start()

        @pl.when(core == 1)
        def _():
            f_tail(l).wait_recv()

    def after_other(l, tail):
        for b in range(2):
            tails[l, :, :, pl.ds(pl.multiple_of(LOC * b + HALF * core, 128), HALF)] = tail[:, :, HALF * b:HALF * (b + 1)]
        tails[l, :, :, D_INNER:CONV_DIM] = tail[:, :, LOC:ACT]
        for c in tail_copies(l):
            c.start()

        @pl.when(l == 0)
        def _():
            xnx, bnx, _ = weight_copies(1)
            for c in xnx + [bnx]:
                c.start()

    def begin(l):
        def norm_body(p, c):
            v = r_out[p]
            ms = jnp.mean(v * v, axis=-1, keepdims=True)
            hbuf[NB * l + p, pl.ds(own_row, SEG), :] = (v * lax.rsqrt(ms + EPSILON) * pre_ref[pl.ds(l, 1), :]).astype(BF16)
            return c
        with jax.named_scope('norm'):
            lax.fori_loop(0, NB, norm_body, 0)

        c_par(l).start()

        @pl.when(core == 1)
        def _():
            c_tail(l).start()
        c_half(l, 0).start()

        @pl.when(core == 0)
        def _():
            c_tail(l).start()
        c_half(l, 1).start()

    def main(l):
        xc, bc, oc = weight_copies(l)

        for b in range(2):
            src = pl.multiple_of(LOC * b + HALF * core, 128)
            cwl[0:4, HALF * b:HALF * (b + 1)] = cw_ref[l, :, pl.ds(src, HALF)]
            cwl[4:5, HALF * b:HALF * (b + 1)] = cb_ref[pl.ds(l, 1), pl.ds(src, HALF)]
        cwl[0:4, LOC:ACT] = cw_ref[l, :, D_INNER:CONV_DIM]
        cwl[4:5, LOC:ACT] = cb_ref[pl.ds(l, 1), D_INNER:CONV_DIM]
        prm[0:1, 0:HEADS] = dtb_ref[pl.ds(l, 1), :]
        prm[1:2, 0:HEADS] = -jnp.exp(alog_ref[pl.ds(l, 1), :])

        def z_body(n, c):
            z_copy(l, n).wait()
            lhs = hbuf[pl.ds(NB * l, NB), pl.ds(own_row, SEG), :].reshape(NB * SEG, D_MODEL)
            z = round_bf16(dot_nt(lhs, wz[pl.ds(pl.multiple_of(512 * n, 512), 512), :]))
            sz[:, :, pl.ds(pl.multiple_of(512 * n, 512), 512)] = silu(z).reshape(NB, SEG, 512)
            return c
        with jax.named_scope('zproj'):
            lax.fori_loop(0, 6, z_body, 0)
        oc.start()

        @pl.when(l == 0)
        def _():
            for n in range(6):
                z_copy(1, n).start()

        with jax.named_scope('wait_h'):
            c_par(l).wait_recv()
            bc.wait()
            for c in xc:
                c.wait()

            @pl.when(chip == 1)
            def _():
                early_tail(l)
        with jax.named_scope('own_block'):
            block(l, 0, NB, own_blk, act_o, tail_o, cumt_o, dtt_o, cum_o)
        with jax.named_scope('intra'):
            lax.fori_loop(0, NB, lambda p, c: (intra_body(l, p), c)[1], 0)

        @pl.when(chip == 1)
        def _():
            with jax.named_scope('wait_r0'):
                c_half(l, 0).wait_recv()
                f_half(l, 0).start()
                late_tail(l)
                f_half(l, 0).wait_recv()

            def half_body(half, c):
                with jax.named_scope('oth_block'):
                    block(l, 2 * half, 2, oth_blk, act_r, tail_r, cumt_r, dtt_r, None)

                @pl.when(half == 0)
                def _():
                    with jax.named_scope('wait_c1'):
                        c_half(l, 1).wait_recv()
                        f_half(l, 1).start()
                with jax.named_scope('inter'):
                    lax.fori_loop(2 * half, 2 * half + 2, lambda p, c: (inter_body(l, p), c)[1], 0)

                @pl.when(half == 0)
                def _():
                    with jax.named_scope('wait_f1'):
                        f_half(l, 1).wait_recv()
                return c
            lax.fori_loop(0, 2, half_body, 0)
            with jax.named_scope('final'):
                lax.fori_loop(0, NB, lambda p, c: (final_body(l, p), c)[1], 0)
            after_other(l, tail_o)

        def gate_body(p, c):
            y_copy(l, p).wait()
            total = jnp.zeros((SEG, 1), F32)
            for b in range(2):
                for own in range(2):
                    cols = pl.ds(pl.multiple_of(LOC * b + HALF * (core if own else 1 - core), 128), HALF)
                    if own:
                        y = ybuf[p, pl.ds(pl.multiple_of(SEG * core, 16), SEG), HALF * b:HALF * (b + 1)]
                    else:
                        y = yrecv[NB * l + p, :, HALF * b:HALF * (b + 1)]
                    g = y.astype(F32) * sz[p, :, cols]
                    sz[p, :, cols] = g
                    total = total + jnp.sum(g * g, axis=-1, keepdims=True)
            scale = lax.rsqrt(total * (1.0 / D_INNER) + EPSILON)
            for b in range(4):
                cols = slice(HALF * b, HALF * (b + 1))
                gn[p, :, cols] = (sz[p, :, cols] * scale * gw_ref[l, :, cols]).astype(BF16)
            return c
        with jax.named_scope('gate'):
            lax.fori_loop(0, NB, gate_body, 0)
            oc.wait()

        def out_body(n, c):
            cols = pl.ds(pl.multiple_of(512 * n, 512), 512)
            o = dot(gn[...].reshape(NB * SEG, D_INNER), wout[:, cols])
            r_out[:, :, cols] = r_out[:, :, cols] + o.reshape(NB, SEG, 512)
            return c
        with jax.named_scope('outproj'):
            lax.fori_loop(0, 3, out_body, 0)

    def deferred(l):
        with jax.named_scope('wait_d'):
            early_tail(l)
            late_tail(l)

        def half_body(half, c):
            with jax.named_scope('wait_dh'):
                c_half(l, half).wait_recv()
                f_half(l, half).start()
                f_half(l, half).wait_recv()
            with jax.named_scope('oth_block'):
                block(l, 2 * half, 2, oth_blk, act_r, tail_r, cumt_r, dtt_r, None)
            with jax.named_scope('final'):
                lax.fori_loop(2 * half, 2 * half + 2, lambda p, c: (final_body(l, p), c)[1], 0)
            return c
        lax.fori_loop(0, 2, half_body, 0)
        after_other(l, tail_r)

    def step(l, carry):
        @pl.when(l < LAYERS)
        def _():
            begin(l)

        @pl.when(jnp.logical_and(chip == 0, l > 0))
        def _():
            deferred(l - 1)

        @pl.when(l < LAYERS)
        def _():
            main(l)
        return carry

    lax.fori_loop(0, LAYERS + 1, step, 0)
    for l in range(LAYERS):
        for c in [c_par(l), c_tail(l), c_half(l, 0), c_half(l, 1), f_tail(l), f_half(l, 0), f_half(l, 1)]:
            c.wait_send()
        for c in tail_copies(l):
            c.wait()
    for p in range(NB):
        pltpu.make_async_copy(stg.at[p], ssm_out.at[p, LAYERS - 1], osem.at[p]).wait()
    tail_out[...] = tails[...]


def solution(mesh):
    vmem = pl.BlockSpec(memory_space=pltpu.VMEM)
    hbm = pl.BlockSpec(memory_space=pl.ANY)
    smem = pl.BlockSpec(memory_space=pltpu.SMEM)

    def forward(resid, pre_norm, w_in, conv_w, conv_b, dt_bias, a_log, d_skip, gate_norm, w_out):
        r, ssm, tails = pl.pallas_call(
            kernel,
            out_shape=(
                jax.ShapeDtypeStruct((NB, SEG, D_MODEL), F32),
                jax.ShapeDtypeStruct((NB, LAYERS, 12, 64, 128), F32),
                jax.ShapeDtypeStruct((LAYERS, NB, 16, CONV_DIM), BF16),
            ),
            in_specs=[vmem, vmem, hbm, vmem, vmem, vmem, vmem, smem, vmem, hbm],
            out_specs=(vmem, hbm, vmem),
            scratch_shapes=[
                pltpu.VMEM((LAYERS * NB, ROWS, D_MODEL), BF16),
                pltpu.VMEM((NB, SEG, D_INNER), F32),
                pltpu.VMEM((D_INNER, D_MODEL), BF16),
                pltpu.VMEM((LOC, D_MODEL), BF16),
                pltpu.VMEM((384, D_MODEL), BF16),
                pltpu.VMEM((D_INNER, D_MODEL), BF16),
                pltpu.VMEM((4, NB, EXT, 128), F32),
                pltpu.VMEM((4, NB, EXT, 128), F32),
                pltpu.VMEM((BLK, LOC), F32),
                pltpu.VMEM((NB, BLK, ACT), BF16),
                pltpu.VMEM((NB, BLK, ACT), BF16),
                pltpu.VMEM((NB, BLK, LOC), F32),
                pltpu.VMEM((NB, BLK, LOC), BF16),
                pltpu.VMEM((LAYERS * NB, SEG, LOC), BF16),
                pltpu.VMEM((NB, SEG, D_INNER), BF16),
                pltpu.VMEM((NB, 12, 64, 128), F32),
                pltpu.VMEM((LAYERS, NB, 16, CONV_DIM), BF16),
                pltpu.VMEM((NB, 16, ACT), BF16),
                pltpu.VMEM((NB, 16, ACT), BF16),
                pltpu.VMEM((NB, BLK, BLK), F32),
                pltpu.VMEM((NB, 40, BLK), F32),
                pltpu.VMEM((NB, 40, BLK), F32),
                pltpu.VMEM((NB, 40, BLK), F32),
                pltpu.VMEM((NB, 40, BLK), F32),
                pltpu.VMEM((8, ACT), F32),
                pltpu.VMEM((8, 128), F32),
                pltpu.SemaphoreType.DMA((10,)),
                pltpu.SemaphoreType.DMA((LAYERS, 7)),
                pltpu.SemaphoreType.DMA((LAYERS, 7)),
                pltpu.SemaphoreType.DMA((LAYERS, NB)),
                pltpu.SemaphoreType.DMA((LAYERS, NB)),
                pltpu.SemaphoreType.DMA((LAYERS, 2)),
                pltpu.SemaphoreType.DMA((LAYERS, 2)),
                pltpu.SemaphoreType.DMA((NB,)),
            ],
            compiler_params=pltpu.CompilerParams(collective_id=0, has_side_effects=True, vmem_limit_bytes=67043328),
        )(resid, pre_norm, jnp.swapaxes(w_in, 1, 2), jnp.swapaxes(conv_w, 1, 2), conv_b, dt_bias, a_log, d_skip, gate_norm, w_out)
        conv_state = jnp.transpose(tails[:, :, 13:16, :], (1, 0, 3, 2))
        return r, ssm, conv_state

    return jax.shard_map(forward, mesh=mesh, in_specs=(P('dp', 'sp', None), P(), P(), P(), P(), P(), P(), P(), P(), P()), out_specs=(P('dp', 'sp', None), P('dp', None, 'sp', None, None), P('dp', None, None, None)), check_vma=False)
```

```python
import jax
import jax.numpy as jnp
from jax import lax
from jax.experimental import pallas as pl
from jax.experimental.pallas import tpu as pltpu
from jax.sharding import PartitionSpec as P

F32 = jnp.float32
BF16 = jnp.bfloat16
EPSILON = 1e-5
LAYERS = 2
NB = 4
SEG = 64
BLK = 128
HALO = 16
EXT = BLK + HALO
ROWS = HALO + 2 * BLK
D_MODEL = 1536
D_INNER = 3072
CONV_DIM = 3328
HEADS = 48
HALF = 768
LOC = 1536
ACT = LOC + 256
PAIRS = 12
NT = (((1,), (1,)), ((), ()))


def dot(a, b):
    return jnp.dot(a, b, preferred_element_type=F32)


def dot_nt(a, b):
    return lax.dot_general(a, b, NT, preferred_element_type=F32)


def round_bf16(v):
    return v.astype(BF16).astype(F32)


def silu(v):
    half = 0.5 * v
    return half * jnp.tanh(half) + half


def head_row(i):
    return i if i < 12 else i + 12


def kernel(resid_ref, pre_ref, w_in_ref, cw_ref, cb_ref, dtb_ref, alog_ref, dskip_ref, gw_ref, w_out_ref,
           r_out, ssm_out, tail_out,
           hbuf, sz, wz, wx, wbc, wout, rawa, rawb, states, bt_o, bt_r, act_o, act_r, yloc, ybuf, yrecv, gn, stg, tails, tail_o, tail_r,
           cum_o, cumt_o, cumt_r, dtt_o, dtt_r, cwl, prm,
           wsem, hsend, hrecv, ysend, yrecv_sem, tsend, trecv, osem):
    me = lax.axis_index('sp')
    chip = me // 2
    core = me % 2
    partner = chip * 2 + (1 - core)
    other = (1 - chip) * 2 + core
    chip_f = chip.astype(F32)
    core_f = core.astype(F32)

    def weight_copies(l):
        xc = [pltpu.make_async_copy(w_in_ref.at[l, pl.ds(pl.multiple_of(D_INNER + LOC * b + HALF * core, 16), HALF), :], wx.at[pl.ds(HALF * b, HALF), :], wsem.at[6 + b]) for b in range(2)]
        bc = [pltpu.make_async_copy(w_in_ref.at[l, pl.ds(src, n), :], wbc.at[pl.ds(dst, n), :], wsem.at[sem]) for src, n, dst, sem in ((2 * D_INNER, 128, 0, 8), (2 * D_INNER + 256, HEADS, 128, 9), (2 * D_INNER + 128, 128, 256, 10))]
        oc = pltpu.make_async_copy(w_out_ref.at[l], wout, wsem.at[11])
        return xc, bc, oc

    def z_copy(l, n):
        rows = pl.ds(pl.multiple_of(512 * n, 16), 512)
        return pltpu.make_async_copy(w_in_ref.at[l, rows, :], wz.at[rows, :], wsem.at[n])

    xc0, bc0, oc0 = weight_copies(0)
    for n in range(6):
        z_copy(0, n).start()

    barrier = pltpu.get_barrier_semaphore()
    for step in range(1, 4):
        pl.semaphore_signal(barrier, inc=1, device_id={'sp': (me + step) % 4}, device_id_type=pl.DeviceIdType.MESH)

    hbuf[:, 0:HALO, :] = jnp.zeros((LAYERS * NB, HALO, D_MODEL), BF16)
    wbc[176:256, :] = jnp.zeros((80, D_MODEL), BF16)
    prm[...] = jnp.zeros((8, 128), F32)
    r_out[...] = resid_ref[...]
    for c in bc0 + xc0:
        c.start()
    with jax.named_scope('barrier'):
        pl.semaphore_wait(barrier, 3)

    own_row = pl.multiple_of(HALO + BLK * chip + SEG * core, 16)
    oth_row = pl.multiple_of(HALO + BLK * (1 - chip) + SEG * core, 16)
    own_blk = pl.multiple_of(BLK * chip, 16)
    oth_blk = pl.multiple_of(BLK * (1 - chip), 16)

    iota_r = lax.broadcasted_iota(jnp.int32, (BLK, BLK), 0)
    iota_c = lax.broadcasted_iota(jnp.int32, (BLK, BLK), 1)

    def remote(src, dst, ssem, rsem, dev):
        return pltpu.make_async_remote_copy(src_ref=src, dst_ref=dst, send_sem=ssem, recv_sem=rsem, device_id={'sp': dev}, device_id_type=pl.DeviceIdType.MESH)

    tri = (iota_r >= iota_c).astype(F32)
    low = iota_c < 64

    def hslice(l, p0, n, row, size):
        return hbuf.at[pl.ds(NB * l + p0, n), pl.ds(row, size), :]

    def same(l, idx, p0, n, row, size, dev):
        ref = hslice(l, p0, n, row, size)
        return remote(ref, ref, hsend.at[l, idx], hrecv.at[l, idx], dev)

    def c_par(l):
        return same(l, 0, 0, NB, own_row, SEG, partner)

    def c_tail(l):
        return same(l, 1, 0, NB, own_row + 48, 16, other)

    def c_half(l, half):
        return same(l, 2 + half, 2 * half, 2, own_row, 48, other)

    def f_tail(l):
        return same(l, 4, 0, NB, oth_row + 48, 16, partner)

    def f_half(l, half):
        return same(l, 5 + half, 2 * half, 2, oth_row, 48, partner)

    def y_copy(l, p):
        src = ybuf.at[p, pl.ds(pl.multiple_of(SEG * (1 - core), 16), SEG), :]
        return remote(src, yrecv.at[NB * l + p], ysend.at[l, p], yrecv_sem.at[l, p], partner)

    def out_copy(l, p):
        return pltpu.make_async_copy(stg.at[p], ssm_out.at[p, l], osem.at[p])

    def tail_copies(l):
        res = []
        for b in range(2):
            ref = tails.at[l, :, :, pl.ds(pl.multiple_of(LOC * b + HALF * core, 128), HALF)]
            res.append(remote(ref, ref, tsend.at[l, b], trecv.at[l, b], partner))
        return res

    def conv_chunk(act, src, first, groups, i, p, dst):
        for g in range(groups):
            cols = slice(dst + 128 * g, dst + 128 * (g + 1))
            acc = cwl[0:1, cols] * src[first + g, i, 13:141, :]
            for k in range(1, 4):
                acc = acc + cwl[k:k + 1, cols] * src[first + g, i, 13 + k:141 + k, :]
            act[p, :, cols] = silu(acc + cwl[4:5, cols]).astype(BF16)

    def block(l, p0, np_, row, act, tail, cumt, dtt, cum, with_c):
        def project(w, rows, dst):
            lhs = hbuf[pl.ds(NB * l + p0, np_), pl.ds(row, EXT), :].reshape(np_ * EXT, D_MODEL)
            res = round_bf16(dot_nt(lhs, w[rows, :]))
            for g in range((rows.stop - rows.start) // 128):
                dst[g, 0:np_] = res[:, 128 * g:128 * (g + 1)].reshape(np_, EXT, 128)

        def finish_bc(src):
            for i in range(np_):
                p = p0 + i
                for g, dst in ((0, LOC), (2, LOC + 128))[:2 if with_c else 1]:
                    tail[p, :, dst:dst + 128] = src[g, i, BLK:EXT, :].astype(BF16)
                    conv_chunk(act, src, g, 1, i, p, dst)
                v = src[1, i, HALO:EXT, :] + prm[0:1, :]
                dt = round_bf16(jnp.maximum(v, 0.0) + jnp.log1p(jnp.exp(-jnp.abs(v))))
                logs = dt * prm[1:2, :]
                dt = dt * (1.0 - core_f) + pltpu.roll(dt, 116, 1) * core_f
                logs = logs * (1.0 - core_f) + pltpu.roll(logs, 116, 1) * core_f
                cums = jnp.dot(tri, logs, precision=lax.Precision.HIGHEST, preferred_element_type=F32)
                cumt[p] = cums.T[0:40]
                dtt[p] = dt.T[0:40]
                if cum is not None:
                    cum[p] = cums

        def finish_x(src, n):
            for i in range(np_):
                for g in range(4):
                    tail[p0 + i, :, 512 * n + 128 * g:512 * n + 128 * (g + 1)] = src[g, i, BLK:EXT, :].astype(BF16)
                conv_chunk(act, src, 0, 4, i, p0 + i, 512 * n)

        project(wbc, slice(0, 384 if with_c else 256), rawa)
        project(wx, slice(0, 512), rawb)
        finish_bc(rawa)
        project(wx, slice(512, 1024), rawa)
        finish_x(rawb, 0)
        project(wx, slice(1024, 1536), rawb)
        finish_x(rawa, 1)
        finish_x(rawb, 2)

    zero = jnp.zeros((), BF16)

    def split_pair(xp):
        return [jnp.where(low, xp, zero), jnp.where(low, zero, xp)]

    def decays(p, h, cumt, dtt, extra):
        row = cumt[p, pl.ds(h, 1), :]
        return dtt[p, pl.ds(h, 1), :] * jnp.exp(row[:, 127:128] - row + extra)

    def intra_body(l, p):
        bt_o[p] = act_o[p, :, LOC:LOC + 128].astype(F32).T
        cb = act_o[p, :, LOC + 128:ACT]
        scores = dot_nt(cb, act_o[p, :, LOC:LOC + 128]) * tri
        for j in range(PAIRS):
            mats = []
            for i in (2 * j, 2 * j + 1):
                h = head_row(i)
                col = jnp.broadcast_to(cum_o[p, :, h:h + 1], (BLK, BLK))
                mats.append((jnp.exp(jnp.minimum(col - cumt_o[p, h:h + 1, :], 0.0)) * (scores * dtt_o[p, h:h + 1, :])).astype(BF16))
            xp = act_o[p, :, 128 * j:128 * (j + 1)]
            blk = (0 if j < 6 else 24) + 12 * core + (2 * j) % 12
            dv = jnp.where(low[0:1], dskip_ref[l, blk], dskip_ref[l, blk + 1])
            y = dot(jnp.concatenate(mats, axis=1), jnp.concatenate(split_pair(xp), axis=0)) + dv * xp.astype(F32)
            yloc[p, :, 128 * j:128 * (j + 1)] = y
            ybuf[p, :, 128 * j:128 * (j + 1)] = y.astype(BF16)

    def inter_body(l, p):
        bt = act_r[p, :, LOC:LOC + 128].astype(F32).T
        bt_r[p] = bt
        cf = act_o[p, :, LOC + 128:ACT]
        for j in range(PAIRS):
            lhs = jnp.concatenate([(bt * decays(p, h, cumt_r, dtt_r, 0.0)).astype(BF16) for h in (head_row(2 * j), head_row(2 * j + 1))], axis=1)
            states[:, 128 * j:128 * (j + 1)] = dot(lhs, jnp.concatenate(split_pair(act_r[p, :, 128 * j:128 * (j + 1)]), axis=0))
        for jj in range(PAIRS // 2):
            o = dot(cf, states[:, 256 * jj:256 * (jj + 1)].astype(BF16))
            for s in range(2):
                j = 2 * jj + s
                ha, hb = head_row(2 * j), head_row(2 * j + 1)
                ca = jnp.broadcast_to(cum_o[p, :, ha:ha + 1], (BLK, BLK))
                cb = jnp.broadcast_to(cum_o[p, :, hb:hb + 1], (BLK, BLK))
                y = yloc[p, :, 128 * j:128 * (j + 1)] + o[:, 128 * s:128 * (s + 1)] * jnp.exp(jnp.where(low, ca, cb))
                ybuf[p, :, 128 * j:128 * (j + 1)] = y.astype(BF16)
        y_copy(l, p).start()

    def final_pair(p, q):
        h = 24 * chip + 2 * q
        cols = pl.ds(pl.multiple_of(128 * (6 * chip + q), 128), 128)
        left, right = [], []
        for hh in (h, h + 1):
            end_o = cumt_o[p, pl.ds(hh, 1), :][:, 127:128]
            end_r = cumt_r[p, pl.ds(hh, 1), :][:, 127:128]
            left.append((bt_o[p] * decays(p, hh, cumt_o, dtt_o, end_r * (1.0 - chip_f))).astype(BF16))
            right.append((bt_r[p] * decays(p, hh, cumt_r, dtt_r, end_o * chip_f)).astype(BF16))
        rhs = jnp.concatenate(split_pair(act_o[p, :, cols]) + split_pair(act_r[p, :, cols]), axis=0)
        state = dot(jnp.concatenate(left + right, axis=1), rhs)
        stg[p, pl.ds(2 * q, 2)] = state.T.reshape(2, 64, 128)

    def wait_out(l):
        @pl.when(l > 0)
        def _():
            for p in range(NB):
                out_copy(0, p).wait()

    def pass_tail(l):
        c_tail(l).wait_recv()
        f_tail(l).start()

    def pass_half(l, half):
        c_half(l, half).wait_recv()
        f_half(l, half).start()

    def bulk(l):
        c_half(l, 0).start()
        c_tail(l).start()
        c_half(l, 1).start()

    def after_other(l, tail):
        for b in range(2):
            tails[l, :, :, pl.ds(pl.multiple_of(LOC * b + HALF * core, 128), HALF)] = tail[:, :, HALF * b:HALF * (b + 1)]
        tails[l, :, :, D_INNER:CONV_DIM] = tail[:, :, LOC:ACT]
        for c in tail_copies(l):
            c.start()

        @pl.when(l == 0)
        def _():
            xnx, bnx, _ = weight_copies(1)
            for c in xnx + bnx:
                c.start()

    def begin(l):
        def norm_body(p, c):
            v = r_out[p]
            ms = jnp.mean(v * v, axis=-1, keepdims=True)
            hbuf[NB * l + p, pl.ds(own_row, SEG), :] = (v * lax.rsqrt(ms + EPSILON) * pre_ref[pl.ds(l, 1), :]).astype(BF16)
            return c
        with jax.named_scope('norm'):
            lax.fori_loop(0, NB, norm_body, 0)

        c_par(l).start()

        @pl.when(core == 1)
        def _():
            c_tail(l).start()
            c_half(l, 0).start()
            c_half(l, 1).start()

        @pl.when(jnp.logical_and(core == 0, l > 0))
        def _():
            bulk(l)

    def main(l):
        xc, bc, oc = weight_copies(l)

        for b in range(2):
            src = pl.multiple_of(LOC * b + HALF * core, 128)
            cwl[0:4, HALF * b:HALF * (b + 1)] = cw_ref[l, :, pl.ds(src, HALF)]
            cwl[4:5, HALF * b:HALF * (b + 1)] = cb_ref[pl.ds(l, 1), pl.ds(src, HALF)]
        cwl[0:4, LOC:ACT] = cw_ref[l, :, D_INNER:CONV_DIM]
        cwl[4:5, LOC:ACT] = cb_ref[pl.ds(l, 1), D_INNER:CONV_DIM]
        prm[0:1, 0:HEADS] = dtb_ref[pl.ds(l, 1), :]
        prm[1:2, 0:HEADS] = -jnp.exp(alog_ref[pl.ds(l, 1), :])

        def z_chunk(n):
            z_copy(l, n).wait()
            lhs = hbuf[pl.ds(NB * l, NB), pl.ds(own_row, SEG), :].reshape(NB * SEG, D_MODEL)
            cols = pl.ds(pl.multiple_of(512 * n, 512), 512)
            z = round_bf16(dot_nt(lhs, wz[cols, :]))
            sz[:, :, cols] = silu(z).reshape(NB, SEG, 512)

        def z_loop(lo, hi):
            lax.fori_loop(lo, hi, lambda n, c: (z_chunk(n), c)[1], 0)

        with jax.named_scope('zproj'):
            z_loop(0, 2)

            @pl.when(jnp.logical_and(core == 0, l == 0))
            def _():
                bulk(l)
            z_loop(2, jnp.where(l == 0, 6, 2))
        oc.start()

        @pl.when(l == 0)
        def _():
            for n in range(6):
                z_copy(1, n).start()

        with jax.named_scope('wait_h'):
            c_par(l).wait_recv()
            for c in bc + xc:
                c.wait()

            @pl.when(jnp.logical_and(chip == 1, core == 1))
            def _():
                pass_tail(l)

            @pl.when(jnp.logical_and(chip == 1, core == 0))
            def _():
                f_tail(l).wait_recv()
        with jax.named_scope('own_block'):
            block(l, 0, NB, own_blk, act_o, tail_o, cumt_o, dtt_o, cum_o, True)

        def intra_end(p):
            @pl.when(chip == 0)
            def _():
                y_copy(l, p).start()

            @pl.when(jnp.logical_and(chip == 1, p == 1))
            def _():
                pass_half(l, 0)

                @pl.when(core == 0)
                def _():
                    pass_tail(l)

        def intra_plain(p, c):
            intra_body(l, p)
            intra_end(p)
            return c

        def intra_z(p, c):
            z_chunk(2 + p)
            intra_body(l, p)
            intra_end(p)
            return c

        with jax.named_scope('intra'):
            @pl.when(l == 0)
            def _():
                lax.fori_loop(0, NB, intra_plain, 0)

            @pl.when(l > 0)
            def _():
                lax.fori_loop(0, NB, intra_z, 0)

        @pl.when(chip == 1)
        def _():
            with jax.named_scope('wait_r0'):
                f_half(l, 0).wait_recv()

                @pl.when(core == 1)
                def _():
                    f_tail(l).wait_recv()

            def half_body(half, c):
                with jax.named_scope('oth_block'):
                    block(l, 2 * half, 2, oth_blk, act_r, tail_r, cumt_r, dtt_r, None, False)

                @pl.when(half == 0)
                def _():
                    with jax.named_scope('wait_c1'):
                        pass_half(l, 1)
                with jax.named_scope('inter'):
                    lax.fori_loop(2 * half, 2 * half + 2, lambda p, c: (inter_body(l, p), c)[1], 0)

                @pl.when(half == 0)
                def _():
                    with jax.named_scope('wait_f1'):
                        f_half(l, 1).wait_recv()
                return c
            lax.fori_loop(0, 2, half_body, 0)
            after_other(l, tail_o)

        def gate_body(p, c):
            y_copy(l, p).wait()
            total = jnp.zeros((SEG, 1), F32)
            for b in range(2):
                for own in range(2):
                    cols = pl.ds(pl.multiple_of(LOC * b + HALF * (core if own else 1 - core), 128), HALF)
                    if own:
                        y = ybuf[p, pl.ds(pl.multiple_of(SEG * core, 16), SEG), HALF * b:HALF * (b + 1)]
                    else:
                        y = yrecv[NB * l + p, :, HALF * b:HALF * (b + 1)]
                    g = y.astype(F32) * sz[p, :, cols]
                    sz[p, :, cols] = g
                    total = total + jnp.sum(g * g, axis=-1, keepdims=True)
            scale = lax.rsqrt(total * (1.0 / D_INNER) + EPSILON)
            for b in range(4):
                cols = slice(HALF * b, HALF * (b + 1))
                gn[p, :, cols] = (sz[p, :, cols] * scale * gw_ref[l, :, cols]).astype(BF16)
            return c
        with jax.named_scope('gate'):
            lax.fori_loop(0, NB, gate_body, 0)
            oc.wait()

        def out_chunk(n):
            cols = pl.ds(pl.multiple_of(512 * n, 512), 512)
            o = dot(gn[...].reshape(NB * SEG, D_INNER), wout[:, cols])
            r_out[:, :, cols] = r_out[:, :, cols] + o.reshape(NB, SEG, 512)

        def out_final(n, c):
            out_chunk(n)
            for q in range(2):
                for p in range(NB):
                    final_pair(p, 2 * n + q)
            return c

        with jax.named_scope('outproj'):
            @pl.when(chip == 0)
            def _():
                lax.fori_loop(0, 3, lambda n, c: (out_chunk(n), c)[1], 0)

            @pl.when(chip == 1)
            def _():
                wait_out(l)
                lax.fori_loop(0, 3, out_final, 0)
                for p in range(NB):
                    out_copy(l, p).start()

        @pl.when(chip == 0)
        def _():
            with jax.named_scope('pass_d'):
                @pl.when(core == 1)
                def _():
                    pass_tail(l)
                pass_half(l, 0)

                @pl.when(core == 0)
                def _():
                    pass_tail(l)

    def deferred(l):
        with jax.named_scope('wait_d'):
            f_tail(l).wait_recv()
            wait_out(l)

        def half_body(half, c):
            with jax.named_scope('wait_dh'):
                f_half(l, half).wait_recv()
            with jax.named_scope('oth_block'):
                block(l, 2 * half, 2, oth_blk, act_r, tail_r, cumt_r, dtt_r, None, True)

            @pl.when(half == 0)
            def _():
                with jax.named_scope('wait_c1'):
                    pass_half(l, 1)

            def final_body(p, cc):
                bt_r[p] = act_r[p, :, LOC:LOC + 128].astype(F32).T
                for q in range(6):
                    final_pair(p, q)
                out_copy(l, p).start()
                return cc
            with jax.named_scope('final'):
                lax.fori_loop(2 * half, 2 * half + 2, final_body, 0)
            return c
        lax.fori_loop(0, 2, half_body, 0)
        after_other(l, tail_r)

    def step(l, carry):
        @pl.when(l < LAYERS)
        def _():
            begin(l)

        @pl.when(jnp.logical_and(chip == 0, l > 0))
        def _():
            deferred(l - 1)

        @pl.when(l < LAYERS)
        def _():
            main(l)
        return carry

    lax.fori_loop(0, LAYERS + 1, step, 0)
    for l in range(LAYERS):
        for c in [c_par(l), c_tail(l), c_half(l, 0), c_half(l, 1), f_tail(l), f_half(l, 0), f_half(l, 1)]:
            c.wait_send()
        for c in tail_copies(l):
            c.wait()
    for p in range(NB):
        pltpu.make_async_copy(stg.at[p], ssm_out.at[p, LAYERS - 1], osem.at[p]).wait()
    tail_out[...] = tails[...]


def copy_kernel(r_ref, ssm_ref, tail_ref, r_out, ssm_out, conv_out):
    r_out[...] = r_ref[...]
    ssm_out[...] = ssm_ref[...]
    for l in range(LAYERS):
        rows = tail_ref[l, 0].astype(F32)
        for k in range(3):
            conv_out[0, k, l:l + 1, :] = rows[13 + k:14 + k, :].astype(BF16)


def solution(mesh):
    vmem = pl.BlockSpec(memory_space=pltpu.VMEM)
    hbm = pl.BlockSpec(memory_space=pl.ANY)
    smem = pl.BlockSpec(memory_space=pltpu.SMEM)

    def forward(resid, pre_norm, w_in, conv_w, conv_b, dt_bias, a_log, d_skip, gate_norm, w_out):
        r, ssm, tails = pl.pallas_call(
            kernel,
            out_shape=(
                jax.ShapeDtypeStruct((NB, SEG, D_MODEL), F32),
                jax.ShapeDtypeStruct((NB, LAYERS, 12, 64, 128), F32),
                jax.ShapeDtypeStruct((LAYERS, NB, 16, CONV_DIM), BF16),
            ),
            in_specs=[vmem, vmem, hbm, vmem, vmem, vmem, vmem, smem, vmem, hbm],
            out_specs=(vmem, hbm, vmem),
            scratch_shapes=[
                pltpu.VMEM((LAYERS * NB, ROWS, D_MODEL), BF16),
                pltpu.VMEM((NB, SEG, D_INNER), F32),
                pltpu.VMEM((D_INNER, D_MODEL), BF16),
                pltpu.VMEM((LOC, D_MODEL), BF16),
                pltpu.VMEM((384, D_MODEL), BF16),
                pltpu.VMEM((D_INNER, D_MODEL), BF16),
                pltpu.VMEM((4, NB, EXT, 128), F32),
                pltpu.VMEM((4, NB, EXT, 128), F32),
                pltpu.VMEM((BLK, LOC), F32),
                pltpu.VMEM((NB, BLK, BLK), F32),
                pltpu.VMEM((NB, BLK, BLK), F32),
                pltpu.VMEM((NB, BLK, ACT), BF16),
                pltpu.VMEM((NB, BLK, ACT), BF16),
                pltpu.VMEM((NB, BLK, LOC), F32),
                pltpu.VMEM((NB, BLK, LOC), BF16),
                pltpu.VMEM((LAYERS * NB, SEG, LOC), BF16),
                pltpu.VMEM((NB, SEG, D_INNER), BF16),
                pltpu.VMEM((NB, 12, 64, 128), F32),
                pltpu.VMEM((LAYERS, NB, 16, CONV_DIM), BF16),
                pltpu.VMEM((NB, 16, ACT), BF16),
                pltpu.VMEM((NB, 16, ACT), BF16),
                pltpu.VMEM((NB, BLK, BLK), F32),
                pltpu.VMEM((NB, 40, BLK), F32),
                pltpu.VMEM((NB, 40, BLK), F32),
                pltpu.VMEM((NB, 40, BLK), F32),
                pltpu.VMEM((NB, 40, BLK), F32),
                pltpu.VMEM((8, ACT), F32),
                pltpu.VMEM((8, 128), F32),
                pltpu.SemaphoreType.DMA((12,)),
                pltpu.SemaphoreType.DMA((LAYERS, 7)),
                pltpu.SemaphoreType.DMA((LAYERS, 7)),
                pltpu.SemaphoreType.DMA((LAYERS, NB)),
                pltpu.SemaphoreType.DMA((LAYERS, NB)),
                pltpu.SemaphoreType.DMA((LAYERS, 2)),
                pltpu.SemaphoreType.DMA((LAYERS, 2)),
                pltpu.SemaphoreType.DMA((NB,)),
            ],
            compiler_params=pltpu.CompilerParams(collective_id=0, has_side_effects=True, vmem_limit_bytes=67043328),
        )(resid, pre_norm, jnp.swapaxes(w_in, 1, 2), jnp.swapaxes(conv_w, 1, 2), conv_b, dt_bias, a_log, d_skip, gate_norm, w_out)
        specs = (
            pl.BlockSpec((1, SEG, D_MODEL), lambda p: (p, 0, 0)),
            pl.BlockSpec((1, LAYERS, 12, 64, 128), lambda p: (p, 0, 0, 0, 0)),
        )
        r, ssm, conv = pl.pallas_call(
            copy_kernel,
            grid=(NB,),
            out_shape=(
                jax.ShapeDtypeStruct(r.shape, F32),
                jax.ShapeDtypeStruct(ssm.shape, F32),
                jax.ShapeDtypeStruct((NB, 3, LAYERS, CONV_DIM), BF16),
            ),
            in_specs=list(specs) + [pl.BlockSpec((LAYERS, 1, 16, CONV_DIM), lambda p: (0, p, 0, 0))],
            out_specs=specs + (pl.BlockSpec((1, 3, LAYERS, CONV_DIM), lambda p: (p, 0, 0, 0)),),
        )(r, ssm, tails)
        return r, ssm, jnp.transpose(conv, (0, 2, 3, 1))

    return jax.shard_map(forward, mesh=mesh, in_specs=(P('dp', 'sp', None), P(), P(), P(), P(), P(), P(), P(), P(), P()), out_specs=(P('dp', 'sp', None), P('dp', None, 'sp', None, None), P('dp', None, None, None)), check_vma=False)
```

```python
import jax
import jax.numpy as jnp
from jax import lax
from jax.experimental import pallas as pl
from jax.experimental.pallas import tpu as pltpu
from jax.sharding import PartitionSpec as P

F32 = jnp.float32
BF16 = jnp.bfloat16
EPSILON = 1e-5
LAYERS = 2
NB = 4
SEG = 64
BLK = 128
HALO = 16
EXT = BLK + HALO
ROWS = HALO + 2 * BLK
D_MODEL = 1536
D_INNER = 3072
CONV_DIM = 3328
HEADS = 48
HALF = 768
LOC = 1536
ACT = LOC + 256
PAIRS = 12
NT = (((1,), (1,)), ((), ()))


def dot(a, b):
    return jnp.dot(a, b, preferred_element_type=F32)


def dot_nt(a, b):
    return lax.dot_general(a, b, NT, preferred_element_type=F32)


def round_bf16(v):
    return v.astype(BF16).astype(F32)


def silu(v):
    half = 0.5 * v
    return half * jnp.tanh(half) + half


def head_row(i):
    return i if i < 12 else i + 12


def kernel(resid_hbm, pre_hbm, w_in_ref, cw_hbm, cb_hbm, dtb_hbm, alog_hbm, dskip_hbm, gw_hbm, w_out_ref,
           r_hbm, ssm_out, tail_out,
           r_out, pre_ref, cw_ref, cb_ref, dtb_ref, alog_ref, dskip_ref, gw_ref, hbuf, sz, wz, wx, wbc, wout, rawa, rawb, states, bt_o, bt_r, act_o, act_r, yloc, ybuf, yrecv, gn, stg, tails, tail_o, tail_r,
           cum_o, cumt_o, cumt_r, dtt_o, dtt_r, cwl, prm,
           wsem, hsend, hrecv, ysend, yrecv_sem, tsend, trecv, osem, psem, rsem, tout):
    me = lax.axis_index('sp')
    chip = me // 2
    core = me % 2
    partner = chip * 2 + (1 - core)
    other = (1 - chip) * 2 + core
    chip_f = chip.astype(F32)
    core_f = core.astype(F32)

    def weight_copies(l):
        xc = [pltpu.make_async_copy(w_in_ref.at[l, pl.ds(pl.multiple_of(D_INNER + LOC * b + HALF * core, 16), HALF), :], wx.at[pl.ds(HALF * b, HALF), :], wsem.at[6 + b]) for b in range(2)]
        bc = [pltpu.make_async_copy(w_in_ref.at[l, pl.ds(src, n), :], wbc.at[pl.ds(dst, n), :], wsem.at[sem]) for src, n, dst, sem in ((2 * D_INNER, 128, 0, 8), (2 * D_INNER + 256, HEADS, 128, 9), (2 * D_INNER + 128, 128, 256, 10))]
        oc = pltpu.make_async_copy(w_out_ref.at[l], wout, wsem.at[11])
        return xc, bc, oc

    def z_copy(l, n):
        rows = pl.ds(pl.multiple_of(512 * n, 16), 512)
        return pltpu.make_async_copy(w_in_ref.at[l, rows, :], wz.at[rows, :], wsem.at[n])

    params = [pltpu.make_async_copy(src, dst, psem.at[i]) for i, (src, dst) in enumerate(((resid_hbm, r_out), (pre_hbm, pre_ref), (cw_hbm, cw_ref), (cb_hbm, cb_ref), (dtb_hbm, dtb_ref), (alog_hbm, alog_ref), (dskip_hbm, dskip_ref), (gw_hbm, gw_ref)))]
    xc0, bc0, oc0 = weight_copies(0)
    params[0].start()
    params[1].start()
    z_copy(0, 0).start()
    for c in params[2:]:
        c.start()
    for n in range(1, 6):
        z_copy(0, n).start()

    barrier = pltpu.get_barrier_semaphore()
    for step in range(1, 4):
        pl.semaphore_signal(barrier, inc=1, device_id={'sp': (me + step) % 4}, device_id_type=pl.DeviceIdType.MESH)

    hbuf[:, 0:HALO, :] = jnp.zeros((LAYERS * NB, HALO, D_MODEL), BF16)
    wbc[176:256, :] = jnp.zeros((80, D_MODEL), BF16)
    prm[...] = jnp.zeros((8, 128), F32)
    for c in bc0 + xc0:
        c.start()
    with jax.named_scope('params'):
        for c in params:
            c.wait()
    with jax.named_scope('barrier'):
        pl.semaphore_wait(barrier, 3)

    own_row = pl.multiple_of(HALO + BLK * chip + SEG * core, 16)
    oth_row = pl.multiple_of(HALO + BLK * (1 - chip) + SEG * core, 16)
    own_blk = pl.multiple_of(BLK * chip, 16)
    oth_blk = pl.multiple_of(BLK * (1 - chip), 16)

    iota_r = lax.broadcasted_iota(jnp.int32, (BLK, BLK), 0)
    iota_c = lax.broadcasted_iota(jnp.int32, (BLK, BLK), 1)

    def remote(src, dst, ssem, rsem, dev):
        return pltpu.make_async_remote_copy(src_ref=src, dst_ref=dst, send_sem=ssem, recv_sem=rsem, device_id={'sp': dev}, device_id_type=pl.DeviceIdType.MESH)

    tri = (iota_r >= iota_c).astype(F32)
    low = iota_c < 64

    def hslice(l, p0, n, row, size):
        return hbuf.at[pl.ds(NB * l + p0, n), pl.ds(row, size), :]

    def same(l, idx, p0, n, row, size, dev):
        ref = hslice(l, p0, n, row, size)
        return remote(ref, ref, hsend.at[l, idx], hrecv.at[l, idx], dev)

    def c_par(l):
        return same(l, 0, 0, NB, own_row, SEG, partner)

    def c_tail(l):
        return same(l, 1, 0, NB, own_row + 48, 16, other)

    def c_half(l, half, size):
        return same(l, 2 + half, 2 * half, 2, own_row, size, other)

    def f_tail(l):
        return same(l, 4, 0, NB, oth_row + 48, 16, partner)

    def f_half(l, half, size):
        return same(l, 5 + half, 2 * half, 2, oth_row, size, partner)

    def by_core(fn):
        @pl.when(core == 0)
        def _():
            fn(64)

        @pl.when(core == 1)
        def _():
            fn(48)

    def wait_half(l, half):
        by_core(lambda n: f_half(l, half, 112 - n).wait_recv())

    def y_copy(l, p):
        src = ybuf.at[p, pl.ds(pl.multiple_of(SEG * (1 - core), 16), SEG), :]
        return remote(src, yrecv.at[NB * l + p], ysend.at[l, p], yrecv_sem.at[l, p], partner)

    def out_prompt(l, p):
        return pltpu.make_async_copy(stg.at[p], ssm_out.at[p, l], osem.at[p])

    def out_heads(l, n):
        return pltpu.make_async_copy(stg.at[:, pl.ds(4 * n, 4)], ssm_out.at[:, l, pl.ds(4 * n, 4)], osem.at[n])

    def r_copy(n):
        cols = pl.ds(pl.multiple_of(512 * n, 512), 512)
        return pltpu.make_async_copy(r_out.at[:, :, cols], r_hbm.at[:, :, cols], rsem.at[n])

    def tail_copy(l):
        return pltpu.make_async_copy(tails.at[l], tail_out.at[l], tout.at[l])

    def tail_copies(l):
        res = []
        for b in range(2):
            ref = tails.at[l, :, :, pl.ds(pl.multiple_of(LOC * b + HALF * core, 128), HALF)]
            res.append(remote(ref, ref, tsend.at[l, b], trecv.at[l, b], partner))
        return res

    def conv_chunk(act, src, first, groups, i, p, dst):
        for g in range(groups):
            cols = slice(dst + 128 * g, dst + 128 * (g + 1))
            acc = cwl[0:1, cols] * src[first + g, i, 13:141, :]
            for k in range(1, 4):
                acc = acc + cwl[k:k + 1, cols] * src[first + g, i, 13 + k:141 + k, :]
            act[p, :, cols] = silu(acc + cwl[4:5, cols]).astype(BF16)

    def block(l, p0, np_, row, act, tail, cumt, dtt, cum, with_c):
        def project(w, rows, dst):
            lhs = hbuf[pl.ds(NB * l + p0, np_), pl.ds(row, EXT), :].reshape(np_ * EXT, D_MODEL)
            res = round_bf16(dot_nt(lhs, w[rows, :]))
            for g in range((rows.stop - rows.start) // 128):
                dst[g, 0:np_] = res[:, 128 * g:128 * (g + 1)].reshape(np_, EXT, 128)

        def finish_bc(src):
            for i in range(np_):
                p = p0 + i
                for g, dst in ((0, LOC), (2, LOC + 128))[:2 if with_c else 1]:
                    tail[p, :, dst:dst + 128] = src[g, i, BLK:EXT, :].astype(BF16)
                    conv_chunk(act, src, g, 1, i, p, dst)
                v = src[1, i, HALO:EXT, :] + prm[0:1, :]
                dt = round_bf16(jnp.maximum(v, 0.0) + jnp.log1p(jnp.exp(-jnp.abs(v))))
                logs = dt * prm[1:2, :]
                dt = dt * (1.0 - core_f) + pltpu.roll(dt, 116, 1) * core_f
                logs = logs * (1.0 - core_f) + pltpu.roll(logs, 116, 1) * core_f
                cums = jnp.dot(tri, logs, precision=lax.Precision.HIGHEST, preferred_element_type=F32)
                cumt[p] = cums.T[0:40]
                dtt[p] = dt.T[0:40]
                if cum is not None:
                    cum[p] = cums

        def finish_x(src, n):
            for i in range(np_):
                for g in range(4):
                    tail[p0 + i, :, 512 * n + 128 * g:512 * n + 128 * (g + 1)] = src[g, i, BLK:EXT, :].astype(BF16)
                conv_chunk(act, src, 0, 4, i, p0 + i, 512 * n)

        project(wbc, slice(0, 384 if with_c else 256), rawa)
        project(wx, slice(0, 512), rawb)
        finish_bc(rawa)
        project(wx, slice(512, 1024), rawa)
        finish_x(rawb, 0)
        project(wx, slice(1024, 1536), rawb)
        finish_x(rawa, 1)
        finish_x(rawb, 2)

    zero = jnp.zeros((), BF16)

    def split_pair(xp):
        return [jnp.where(low, xp, zero), jnp.where(low, zero, xp)]

    def decays(p, h, cumt, dtt, extra):
        row = cumt[p, pl.ds(h, 1), :]
        return dtt[p, pl.ds(h, 1), :] * jnp.exp(row[:, 127:128] - row + extra)

    def intra_body(l, p):
        bt_o[p] = act_o[p, :, LOC:LOC + 128].astype(F32).T
        cb = act_o[p, :, LOC + 128:ACT]
        scores = dot_nt(cb, act_o[p, :, LOC:LOC + 128]) * tri
        for j in range(PAIRS):
            mats = []
            for i in (2 * j, 2 * j + 1):
                h = head_row(i)
                col = jnp.broadcast_to(cum_o[p, :, h:h + 1], (BLK, BLK))
                mats.append((jnp.exp(jnp.minimum(col - cumt_o[p, h:h + 1, :], 0.0)) * (scores * dtt_o[p, h:h + 1, :])).astype(BF16))
            xp = act_o[p, :, 128 * j:128 * (j + 1)]
            blk = (0 if j < 6 else 24) + 12 * core + (2 * j) % 12
            dv = jnp.where(low[0:1], dskip_ref[l, blk], dskip_ref[l, blk + 1])
            y = dot(jnp.concatenate(mats, axis=1), jnp.concatenate(split_pair(xp), axis=0)) + dv * xp.astype(F32)
            yloc[p, :, 128 * j:128 * (j + 1)] = y
            ybuf[p, :, 128 * j:128 * (j + 1)] = y.astype(BF16)

    def inter_body(l, p):
        bt = act_r[p, :, LOC:LOC + 128].astype(F32).T
        bt_r[p] = bt
        cf = act_o[p, :, LOC + 128:ACT]
        for j in range(PAIRS):
            lhs = jnp.concatenate([(bt * decays(p, h, cumt_r, dtt_r, 0.0)).astype(BF16) for h in (head_row(2 * j), head_row(2 * j + 1))], axis=1)
            states[:, 128 * j:128 * (j + 1)] = dot(lhs, jnp.concatenate(split_pair(act_r[p, :, 128 * j:128 * (j + 1)]), axis=0))
        for jj in range(PAIRS // 2):
            o = dot(cf, states[:, 256 * jj:256 * (jj + 1)].astype(BF16))
            for s in range(2):
                j = 2 * jj + s
                ha, hb = head_row(2 * j), head_row(2 * j + 1)
                ca = jnp.broadcast_to(cum_o[p, :, ha:ha + 1], (BLK, BLK))
                cb = jnp.broadcast_to(cum_o[p, :, hb:hb + 1], (BLK, BLK))
                y = yloc[p, :, 128 * j:128 * (j + 1)] + o[:, 128 * s:128 * (s + 1)] * jnp.exp(jnp.where(low, ca, cb))
                ybuf[p, :, 128 * j:128 * (j + 1)] = y.astype(BF16)
        y_copy(l, p).start()

    def final_pair(p, q):
        h = 24 * chip + 2 * q
        cols = pl.ds(pl.multiple_of(128 * (6 * chip + q), 128), 128)
        left, right = [], []
        for hh in (h, h + 1):
            end_o = cumt_o[p, pl.ds(hh, 1), :][:, 127:128]
            end_r = cumt_r[p, pl.ds(hh, 1), :][:, 127:128]
            left.append((bt_o[p] * decays(p, hh, cumt_o, dtt_o, end_r * (1.0 - chip_f))).astype(BF16))
            right.append((bt_r[p] * decays(p, hh, cumt_r, dtt_r, end_o * chip_f)).astype(BF16))
        rhs = jnp.concatenate(split_pair(act_o[p, :, cols]) + split_pair(act_r[p, :, cols]), axis=0)
        state = dot(jnp.concatenate(left + right, axis=1), rhs)
        stg[p, pl.ds(2 * q, 2)] = state.T.reshape(2, 64, 128)

    def pass_tail(l):
        c_tail(l).wait_recv()
        f_tail(l).start()

    def pass_half(l, half):
        def go(n):
            c_half(l, half, n).wait_recv()
            f_half(l, half, n).start()
        by_core(go)

    def bulk(l):
        c_half(l, 0, 64).start()
        c_half(l, 1, 64).start()

    def after_other(l, tail):
        for b in range(2):
            tails[l, :, :, pl.ds(pl.multiple_of(LOC * b + HALF * core, 128), HALF)] = tail[:, :, HALF * b:HALF * (b + 1)]
        tails[l, :, :, D_INNER:CONV_DIM] = tail[:, :, LOC:ACT]
        for c in tail_copies(l):
            c.start()

        @pl.when(l == 0)
        def _():
            xnx, bnx, _ = weight_copies(1)
            for c in xnx + bnx:
                c.start()

    def begin(l):
        def norm_body(p, c):
            v = r_out[p]
            ms = jnp.mean(v * v, axis=-1, keepdims=True)
            hbuf[NB * l + p, pl.ds(own_row, SEG), :] = (v * lax.rsqrt(ms + EPSILON) * pre_ref[pl.ds(l, 1), :]).astype(BF16)
            return c
        with jax.named_scope('norm'):
            lax.fori_loop(0, NB, norm_body, 0)

        c_par(l).start()

        @pl.when(core == 1)
        def _():
            c_tail(l).start()
            c_half(l, 0, 48).start()
            c_half(l, 1, 48).start()

        @pl.when(jnp.logical_and(core == 0, l > 0))
        def _():
            bulk(l)

        @pl.when(jnp.logical_and(jnp.logical_and(core == 1, chip == 1), l > 0))
        def _():
            pass_tail(l)

    def main(l):
        xc, bc, oc = weight_copies(l)

        for b in range(2):
            src = pl.multiple_of(LOC * b + HALF * core, 128)
            cwl[0:4, HALF * b:HALF * (b + 1)] = cw_ref[l, :, pl.ds(src, HALF)]
            cwl[4:5, HALF * b:HALF * (b + 1)] = cb_ref[pl.ds(l, 1), pl.ds(src, HALF)]
        cwl[0:4, LOC:ACT] = cw_ref[l, :, D_INNER:CONV_DIM]
        cwl[4:5, LOC:ACT] = cb_ref[pl.ds(l, 1), D_INNER:CONV_DIM]
        prm[0:1, 0:HEADS] = dtb_ref[pl.ds(l, 1), :]
        prm[1:2, 0:HEADS] = -jnp.exp(alog_ref[pl.ds(l, 1), :])

        def z_chunk(n):
            z_copy(l, n).wait()
            lhs = hbuf[pl.ds(NB * l, NB), pl.ds(own_row, SEG), :].reshape(NB * SEG, D_MODEL)
            cols = pl.ds(pl.multiple_of(512 * n, 512), 512)
            z = round_bf16(dot_nt(lhs, wz[cols, :]))
            sz[:, :, cols] = silu(z).reshape(NB, SEG, 512)

        def z_loop(lo, hi):
            lax.fori_loop(lo, hi, lambda n, c: (z_chunk(n), c)[1], 0)

        with jax.named_scope('zproj'):
            z_loop(0, 2)

            @pl.when(jnp.logical_and(core == 0, l == 0))
            def _():
                bulk(l)
            z_loop(2, jnp.where(l == 0, 6, 2))
        oc.start()

        @pl.when(l == 0)
        def _():
            for n in range(6):
                z_copy(1, n).start()

        with jax.named_scope('wait_h'):
            c_par(l).wait_recv()
            for c in bc + xc:
                c.wait()

            @pl.when(jnp.logical_and(jnp.logical_and(core == 1, chip == 1), l == 0))
            def _():
                pass_tail(l)

            @pl.when(jnp.logical_and(chip == 1, core == 0))
            def _():
                f_tail(l).wait_recv()
        with jax.named_scope('own_block'):
            block(l, 0, NB, own_blk, act_o, tail_o, cumt_o, dtt_o, cum_o, True)

        def intra_end(p):
            @pl.when(chip == 0)
            def _():
                y_copy(l, p).start()

            @pl.when(jnp.logical_and(chip == 1, p == 1))
            def _():
                pass_half(l, 0)

        def intra_plain(p, c):
            intra_body(l, p)
            intra_end(p)
            return c

        def intra_z(p, c):
            z_chunk(2 + p)
            intra_body(l, p)
            intra_end(p)
            return c

        with jax.named_scope('intra'):
            @pl.when(l == 0)
            def _():
                lax.fori_loop(0, NB, intra_plain, 0)

            @pl.when(l > 0)
            def _():
                lax.fori_loop(0, NB, intra_z, 0)

        @pl.when(chip == 1)
        def _():
            with jax.named_scope('wait_r0'):
                wait_half(l, 0)

            def half_body(half, c):
                with jax.named_scope('oth_block'):
                    block(l, 2 * half, 2, oth_blk, act_r, tail_r, cumt_r, dtt_r, None, False)

                @pl.when(half == 0)
                def _():
                    with jax.named_scope('wait_c1'):
                        pass_half(l, 1)
                with jax.named_scope('inter'):
                    lax.fori_loop(2 * half, 2 * half + 2, lambda p, c: (inter_body(l, p), c)[1], 0)

                @pl.when(half == 0)
                def _():
                    with jax.named_scope('wait_f1'):
                        wait_half(l, 1)
                return c
            lax.fori_loop(0, 2, half_body, 0)
            after_other(l, tail_o)

        def gate_body(p, c):
            y_copy(l, p).wait()
            total = jnp.zeros((SEG, 1), F32)
            for b in range(2):
                for own in range(2):
                    cols = pl.ds(pl.multiple_of(LOC * b + HALF * (core if own else 1 - core), 128), HALF)
                    if own:
                        y = ybuf[p, pl.ds(pl.multiple_of(SEG * core, 16), SEG), HALF * b:HALF * (b + 1)]
                    else:
                        y = yrecv[NB * l + p, :, HALF * b:HALF * (b + 1)]
                    g = y.astype(F32) * sz[p, :, cols]
                    sz[p, :, cols] = g
                    total = total + jnp.sum(g * g, axis=-1, keepdims=True)
            scale = lax.rsqrt(total * (1.0 / D_INNER) + EPSILON)
            for b in range(4):
                cols = slice(HALF * b, HALF * (b + 1))
                gn[p, :, cols] = (sz[p, :, cols] * scale * gw_ref[l, :, cols]).astype(BF16)
            return c
        with jax.named_scope('gate'):
            lax.fori_loop(0, NB, gate_body, 0)
            oc.wait()

        def out_chunk(n):
            cols = pl.ds(pl.multiple_of(512 * n, 512), 512)
            o = dot(gn[...].reshape(NB * SEG, D_INNER), wout[:, cols])
            r_out[:, :, cols] = r_out[:, :, cols] + o.reshape(NB, SEG, 512)

        def send_r(n):
            @pl.when(l == LAYERS - 1)
            def _():
                r_copy(n).start()

        def out_final(n, c):
            out_chunk(n)
            for q in range(2):
                for p in range(NB):
                    final_pair(p, 2 * n + q)
            out_heads(l, n).start()
            send_r(n)
            return c

        def out_plain(n, c):
            out_chunk(n)
            send_r(n)
            return c

        with jax.named_scope('outproj'):
            @pl.when(chip == 0)
            def _():
                lax.fori_loop(0, 3, out_plain, 0)

            @pl.when(chip == 1)
            def _():
                @pl.when(l > 0)
                def _():
                    for n in range(3):
                        out_heads(0, n).wait()
                lax.fori_loop(0, 3, out_final, 0)

        @pl.when(chip == 0)
        def _():
            with jax.named_scope('pass_d'):
                @pl.when(core == 1)
                def _():
                    pass_tail(l)
                pass_half(l, 0)

    def deferred(l):
        with jax.named_scope('wait_d'):
            @pl.when(core == 0)
            def _():
                f_tail(l).wait_recv()

            @pl.when(l > 0)
            def _():
                for p in range(NB):
                    out_prompt(0, p).wait()

        def half_body(half, c):
            with jax.named_scope('wait_dh'):
                wait_half(l, half)
            with jax.named_scope('oth_block'):
                block(l, 2 * half, 2, oth_blk, act_r, tail_r, cumt_r, dtt_r, None, True)

            @pl.when(half == 0)
            def _():
                with jax.named_scope('wait_c1'):
                    pass_half(l, 1)

            @pl.when(half == 1)
            def _():
                after_other(l, tail_r)

            def final_body(p, cc):
                bt_r[p] = act_r[p, :, LOC:LOC + 128].astype(F32).T
                for q in range(6):
                    final_pair(p, q)
                out_prompt(l, p).start()
                return cc
            with jax.named_scope('final'):
                lax.fori_loop(2 * half, 2 * half + 2, final_body, 0)
            return c
        lax.fori_loop(0, 2, half_body, 0)

    def step(l, carry):
        @pl.when(l < LAYERS)
        def _():
            begin(l)

        @pl.when(jnp.logical_and(chip == 0, l > 0))
        def _():
            deferred(l - 1)

        @pl.when(l < LAYERS)
        def _():
            main(l)
        return carry

    lax.fori_loop(0, LAYERS + 1, step, 0)
    for l in range(LAYERS):
        for c in tail_copies(l):
            c.wait()
        tail_copy(l).start()
    for l in range(LAYERS):
        c_par(l).wait_send()

        @pl.when(core == 1)
        def _():
            c_tail(l).wait_send()
            f_tail(l).wait_send()

        def sent(n):
            for half in range(2):
                c_half(l, half, n).wait_send()
                f_half(l, half, n).wait_send()
        by_core(sent)
        tail_copy(l).wait()

    @pl.when(chip == 0)
    def _():
        for p in range(NB):
            out_prompt(LAYERS - 1, p).wait()

    @pl.when(chip == 1)
    def _():
        for n in range(3):
            out_heads(LAYERS - 1, n).wait()
    for n in range(3):
        r_copy(n).wait()


def copy_kernel(r_ref, ssm_ref, tail_ref, r_out, ssm_out, conv_out, rbuf, sbuf, tbuf, cbuf, isem, osem):
    def copies(p):
        srcs = (r_ref.at[p], ssm_ref.at[p], tail_ref.at[:, p])
        bufs = (rbuf.at[p], sbuf.at[p], tbuf.at[p])
        dsts = (r_out.at[p], ssm_out.at[p], conv_out.at[p])
        outs = (rbuf.at[p], sbuf.at[p], cbuf.at[p])
        ins = [pltpu.make_async_copy(srcs[i], bufs[i], isem.at[p, i]) for i in range(3)]
        res = [pltpu.make_async_copy(outs[i], dsts[i], osem.at[p, i]) for i in range(3)]
        return ins, res

    for p in range(NB):
        for c in copies(p)[0]:
            c.start()
    for p in range(NB):
        ins, res = copies(p)
        for i in range(2):
            ins[i].wait()
            res[i].start()
        ins[2].wait()
        for l in range(LAYERS):
            rows = tbuf[p, l].astype(F32)
            for k in range(3):
                cbuf[p, k, l:l + 1, :] = rows[13 + k:14 + k, :].astype(BF16)
        res[2].start()
    for p in range(NB):
        for c in copies(p)[1]:
            c.wait()


def solution(mesh):
    hbm = pl.BlockSpec(memory_space=pl.ANY)

    def forward(resid, pre_norm, w_in, conv_w, conv_b, dt_bias, a_log, d_skip, gate_norm, w_out):
        r, ssm, tails = pl.pallas_call(
            kernel,
            out_shape=(
                jax.ShapeDtypeStruct((NB, SEG, D_MODEL), F32),
                jax.ShapeDtypeStruct((NB, LAYERS, 12, 64, 128), F32),
                jax.ShapeDtypeStruct((LAYERS, NB, 16, CONV_DIM), BF16),
            ),
            in_specs=[hbm] * 10,
            out_specs=(hbm, hbm, hbm),
            scratch_shapes=[
                pltpu.VMEM((NB, SEG, D_MODEL), F32),
                pltpu.VMEM((LAYERS, D_MODEL), F32),
                pltpu.VMEM((LAYERS, 4, CONV_DIM), F32),
                pltpu.VMEM((LAYERS, CONV_DIM), F32),
                pltpu.VMEM((LAYERS, HEADS), F32),
                pltpu.VMEM((LAYERS, HEADS), F32),
                pltpu.SMEM((LAYERS, HEADS), F32),
                pltpu.VMEM((LAYERS, 1, D_INNER), F32),
                pltpu.VMEM((LAYERS * NB, ROWS, D_MODEL), BF16),
                pltpu.VMEM((NB, SEG, D_INNER), F32),
                pltpu.VMEM((D_INNER, D_MODEL), BF16),
                pltpu.VMEM((LOC, D_MODEL), BF16),
                pltpu.VMEM((384, D_MODEL), BF16),
                pltpu.VMEM((D_INNER, D_MODEL), BF16),
                pltpu.VMEM((4, NB, EXT, 128), F32),
                pltpu.VMEM((4, NB, EXT, 128), F32),
                pltpu.VMEM((BLK, LOC), F32),
                pltpu.VMEM((NB, BLK, BLK), F32),
                pltpu.VMEM((NB, BLK, BLK), F32),
                pltpu.VMEM((NB, BLK, ACT), BF16),
                pltpu.VMEM((NB, BLK, ACT), BF16),
                pltpu.VMEM((NB, BLK, LOC), F32),
                pltpu.VMEM((NB, BLK, LOC), BF16),
                pltpu.VMEM((LAYERS * NB, SEG, LOC), BF16),
                pltpu.VMEM((NB, SEG, D_INNER), BF16),
                pltpu.VMEM((NB, 12, 64, 128), F32),
                pltpu.VMEM((LAYERS, NB, 16, CONV_DIM), BF16),
                pltpu.VMEM((NB, 16, ACT), BF16),
                pltpu.VMEM((NB, 16, ACT), BF16),
                pltpu.VMEM((NB, BLK, BLK), F32),
                pltpu.VMEM((NB, 40, BLK), F32),
                pltpu.VMEM((NB, 40, BLK), F32),
                pltpu.VMEM((NB, 40, BLK), F32),
                pltpu.VMEM((NB, 40, BLK), F32),
                pltpu.VMEM((8, ACT), F32),
                pltpu.VMEM((8, 128), F32),
                pltpu.SemaphoreType.DMA((12,)),
                pltpu.SemaphoreType.DMA((LAYERS, 7)),
                pltpu.SemaphoreType.DMA((LAYERS, 7)),
                pltpu.SemaphoreType.DMA((LAYERS, NB)),
                pltpu.SemaphoreType.DMA((LAYERS, NB)),
                pltpu.SemaphoreType.DMA((LAYERS, 2)),
                pltpu.SemaphoreType.DMA((LAYERS, 2)),
                pltpu.SemaphoreType.DMA((NB,)),
                pltpu.SemaphoreType.DMA((8,)),
                pltpu.SemaphoreType.DMA((3,)),
                pltpu.SemaphoreType.DMA((LAYERS,)),
            ],
            compiler_params=pltpu.CompilerParams(collective_id=0, has_side_effects=True, vmem_limit_bytes=67043328),
        )(resid, pre_norm, jnp.swapaxes(w_in, 1, 2), jnp.swapaxes(conv_w, 1, 2), conv_b, dt_bias, a_log, d_skip, gate_norm, w_out)
        r, ssm, conv = pl.pallas_call(
            copy_kernel,
            out_shape=(
                jax.ShapeDtypeStruct(r.shape, F32),
                jax.ShapeDtypeStruct(ssm.shape, F32),
                jax.ShapeDtypeStruct((NB, 3, LAYERS, CONV_DIM), BF16),
            ),
            in_specs=[hbm] * 3,
            out_specs=(hbm, hbm, hbm),
            scratch_shapes=[
                pltpu.VMEM((NB, SEG, D_MODEL), F32),
                pltpu.VMEM((NB, LAYERS, 12, 64, 128), F32),
                pltpu.VMEM((NB, LAYERS, 16, CONV_DIM), BF16),
                pltpu.VMEM((NB, 3, LAYERS, CONV_DIM), BF16),
                pltpu.SemaphoreType.DMA((NB, 3)),
                pltpu.SemaphoreType.DMA((NB, 3)),
            ],
        )(r, ssm, tails)
        return r, ssm, jnp.transpose(conv, (0, 2, 3, 1))

    return jax.shard_map(forward, mesh=mesh, in_specs=(P('dp', 'sp', None), P(), P(), P(), P(), P(), P(), P(), P(), P()), out_specs=(P('dp', 'sp', None), P('dp', None, 'sp', None, None), P('dp', None, None, None)), check_vma=False)
```

```python
import functools

import jax
import jax.numpy as jnp
from jax import lax
from jax.experimental import pallas as pl
from jax.experimental.pallas import tpu as pltpu
from jax.sharding import PartitionSpec as P

F32 = jnp.float32
BF16 = jnp.bfloat16
EPSILON = 1e-5
LAYERS = 2
NB = 4
SEG = 64
BLK = 128
HALO = 16
EXT = BLK + HALO
ROWS = HALO + 2 * BLK
D_MODEL = 1536
D_INNER = 3072
CONV_DIM = 3328
HEADS = 48
HALF = 768
LOC = 1536
ACT = LOC + 256
PAIRS = 12
VMEM_LIMIT = 57200000
NT = (((1,), (1,)), ((), ()))


def dot(a, b):
    return jnp.dot(a, b, preferred_element_type=F32)


def dot_nt(a, b):
    return lax.dot_general(a, b, NT, preferred_element_type=F32)


def round_bf16(v):
    return v.astype(BF16).astype(F32)


def silu(v):
    half = 0.5 * v
    return half * jnp.tanh(half) + half


def head_row(i):
    return i if i < 12 else i + 12


def kernel(resid_hbm, pre_hbm, w_in_ref, cw_hbm, cb_hbm, dtb_hbm, alog_hbm, dskip_hbm, gw_hbm, w_out_ref,
           r_hbm, ssm_out, tail_out,
           r_out, pre_ref, cw_ref, cb_ref, dtb_ref, alog_ref, dskip_ref, gw_ref, hbuf, sz, wz, wx, wbc, wout, rawa, rawb, states, bt_o, bt_r, act_o, act_r, yloc, ybuf, yrecv, gn, stg, tails, tail_o, tail_r,
           cum_o, cumt_o, cumt_r, dtt_o, dtt_r, cwl, prm,
           wsem, hsend, hrecv, ysend, yrecv_sem, tsend, trecv, osem, psem, rsem, tout):
    me = lax.axis_index('sp')
    chip = me // 2
    core = me % 2
    partner = chip * 2 + (1 - core)
    other = (1 - chip) * 2 + core
    chip_f = chip.astype(F32)
    core_f = core.astype(F32)

    def weight_copies(l):
        xc = [pltpu.make_async_copy(w_in_ref.at[l, pl.ds(pl.multiple_of(D_INNER + LOC * b + HALF * core, 16), HALF), :], wx.at[pl.ds(HALF * b, HALF), :], wsem.at[6 + b]) for b in range(2)]
        bc = [pltpu.make_async_copy(w_in_ref.at[l, pl.ds(src, n), :], wbc.at[pl.ds(dst, n), :], wsem.at[sem]) for src, n, dst, sem in ((2 * D_INNER, 128, 0, 8), (2 * D_INNER + 256, HEADS, 128, 9), (2 * D_INNER + 128, 128, 256, 10))]
        oc = pltpu.make_async_copy(w_out_ref.at[l], wout, wsem.at[11])
        return xc, bc, oc

    def z_copy(l, n):
        rows = pl.ds(pl.multiple_of(512 * n, 16), 512)
        return pltpu.make_async_copy(w_in_ref.at[l, rows, :], wz.at[rows, :], wsem.at[n])

    params = [pltpu.make_async_copy(src, dst, psem.at[i]) for i, (src, dst) in enumerate(((resid_hbm, r_out), (pre_hbm, pre_ref), (cw_hbm, cw_ref), (cb_hbm, cb_ref), (dtb_hbm, dtb_ref), (alog_hbm, alog_ref), (dskip_hbm, dskip_ref), (gw_hbm, gw_ref)))]
    xc0, bc0, oc0 = weight_copies(0)
    params[0].start()
    params[1].start()
    z_copy(0, 0).start()
    for c in params[2:]:
        c.start()
    for n in range(1, 6):
        z_copy(0, n).start()

    barrier = pltpu.get_barrier_semaphore()
    for step in range(1, 4):
        pl.semaphore_signal(barrier, inc=1, device_id={'sp': (me + step) % 4}, device_id_type=pl.DeviceIdType.MESH)

    hbuf[:, 0:HALO, :] = jnp.zeros((LAYERS * NB, HALO, D_MODEL), BF16)
    wbc[176:256, :] = jnp.zeros((80, D_MODEL), BF16)
    prm[...] = jnp.zeros((8, 128), F32)
    for c in bc0 + xc0:
        c.start()
    with jax.named_scope('params'):
        for c in params[:2]:
            c.wait()
    with jax.named_scope('barrier'):
        pl.semaphore_wait(barrier, 3)

    own_row = pl.multiple_of(HALO + BLK * chip + SEG * core, 16)
    oth_row = pl.multiple_of(HALO + BLK * (1 - chip) + SEG * core, 16)
    own_blk = pl.multiple_of(BLK * chip, 16)
    oth_blk = pl.multiple_of(BLK * (1 - chip), 16)

    iota_r = lax.broadcasted_iota(jnp.int32, (BLK, BLK), 0)
    iota_c = lax.broadcasted_iota(jnp.int32, (BLK, BLK), 1)

    def remote(src, dst, ssem, rsem, dev):
        return pltpu.make_async_remote_copy(src_ref=src, dst_ref=dst, send_sem=ssem, recv_sem=rsem, device_id={'sp': dev}, device_id_type=pl.DeviceIdType.MESH)

    tri = (iota_r >= iota_c).astype(F32)
    low = iota_c < 64

    def hslice(l, p0, n, row, size):
        return hbuf.at[pl.ds(NB * l + p0, n), pl.ds(row, size), :]

    def same(l, idx, p0, n, row, size, dev):
        ref = hslice(l, p0, n, row, size)
        return remote(ref, ref, hsend.at[l, idx], hrecv.at[l, idx], dev)

    def c_par(l):
        return same(l, 0, 0, NB, own_row, SEG, partner)

    def c_tail(l):
        return same(l, 1, 0, NB, own_row + 48, 16, other)

    def c_half(l, half, size):
        return same(l, 2 + half, 2 * half, 2, own_row, size, other)

    def f_tail(l):
        return same(l, 4, 0, NB, oth_row + 48, 16, partner)

    def f_half(l, half, size):
        return same(l, 5 + half, 2 * half, 2, oth_row, size, partner)

    def by_core(fn):
        @pl.when(core == 0)
        def _():
            fn(64)

        @pl.when(core == 1)
        def _():
            fn(48)

    def wait_half(l, half):
        by_core(lambda n: f_half(l, half, 112 - n).wait_recv())

    def y_copy(l, p):
        src = ybuf.at[p, pl.ds(pl.multiple_of(SEG * (1 - core), 16), SEG), :]
        return remote(src, yrecv.at[NB * l + p], ysend.at[l, p], yrecv_sem.at[l, p], partner)

    def out_prompt(l, p):
        return pltpu.make_async_copy(stg.at[p], ssm_out.at[p, l], osem.at[p])

    def out_heads(l, n):
        return pltpu.make_async_copy(stg.at[:, pl.ds(4 * n, 4)], ssm_out.at[:, l, pl.ds(4 * n, 4)], osem.at[n])

    def r_copy(n):
        cols = pl.ds(pl.multiple_of(512 * n, 512), 512)
        return pltpu.make_async_copy(r_out.at[:, :, cols], r_hbm.at[:, :, cols], rsem.at[n])

    def tail_copy(l):
        return pltpu.make_async_copy(tails.at[l], tail_out.at[l], tout.at[l])

    def tail_copies(l):
        res = []
        for b in range(2):
            ref = tails.at[l, :, :, pl.ds(pl.multiple_of(LOC * b + HALF * core, 128), HALF)]
            res.append(remote(ref, ref, tsend.at[l, b], trecv.at[l, b], partner))
        return res

    def conv_chunk(act, src, first, groups, i, p, dst):
        for g in range(groups):
            cols = slice(dst + 128 * g, dst + 128 * (g + 1))
            acc = cwl[0:1, cols] * src[first + g, i, 13:141, :]
            for k in range(1, 4):
                acc = acc + cwl[k:k + 1, cols] * src[first + g, i, 13 + k:141 + k, :]
            act[p, :, cols] = silu(acc + cwl[4:5, cols]).astype(BF16)

    def block(l, p0, np_, row, act, tail, cumt, dtt, cum, with_c, width):
        def project(w, rows, dst):
            lhs = hbuf[pl.ds(NB * l + p0, np_), pl.ds(row, EXT), :].reshape(np_ * EXT, D_MODEL)
            res = round_bf16(dot_nt(lhs, w[rows, :]))
            for g in range((rows.stop - rows.start) // 128):
                dst[g, 0:np_] = res[:, 128 * g:128 * (g + 1)].reshape(np_, EXT, 128)

        def finish_bc(src):
            for i in range(np_):
                p = p0 + i
                for g, dst in ((0, LOC), (2, LOC + 128))[:2 if with_c else 1]:
                    if tail is not None:
                        tail[p, :, dst:dst + 128] = src[g, i, BLK:EXT, :].astype(BF16)
                    conv_chunk(act, src, g, 1, i, p, dst)
                v = src[1, i, HALO:EXT, :] + prm[0:1, :]
                dt = round_bf16(jnp.maximum(v, 0.0) + jnp.log1p(jnp.exp(-jnp.abs(v))))
                logs = dt * prm[1:2, :]
                dt = dt * (1.0 - core_f) + pltpu.roll(dt, 116, 1) * core_f
                logs = logs * (1.0 - core_f) + pltpu.roll(logs, 116, 1) * core_f
                cums = jnp.dot(tri, logs, precision=lax.Precision.HIGHEST, preferred_element_type=F32)
                cumt[p] = cums.T[0:40]
                dtt[p] = dt.T[0:40]
                if cum is not None:
                    cum[p] = cums

        def finish_x(src, col, n):
            for i in range(np_):
                if tail is not None:
                    for g in range(n // 128):
                        tail[p0 + i, :, col + 128 * g:col + 128 * (g + 1)] = src[g, i, BLK:EXT, :].astype(BF16)
                conv_chunk(act, src, 0, n // 128, i, p0 + i, col)

        project(wbc, slice(0, 384 if with_c else 256), rawa)
        pending, nxt = (lambda: finish_bc(rawa)), rawb
        for col in range(0, width, 512):
            n = min(512, width - col)
            project(wx, slice(col, col + n), nxt)
            pending()
            pending = functools.partial(finish_x, nxt, col, n)
            nxt = rawa if nxt is rawb else rawb
        pending()

    def last_rows(l, tail):
        lhs = hbuf[pl.ds(NB * l, NB), ROWS - 16:ROWS, :].reshape(NB * 16, D_MODEL)
        for col in range(0, LOC, 512):
            tail[:, :, col:col + 512] = dot_nt(lhs, wx[col:col + 512, :]).astype(BF16).reshape(NB, 16, 512)
        res = dot_nt(lhs, wbc[...]).astype(BF16).reshape(NB, 16, 384)
        tail[:, :, LOC:LOC + 128] = res[:, :, 0:128]
        tail[:, :, LOC + 128:ACT] = res[:, :, 256:384]

    zero = jnp.zeros((), BF16)

    def split_pair(xp):
        return [jnp.where(low, xp, zero), jnp.where(low, zero, xp)]

    def decays(p, h, cumt, dtt, extra):
        row = cumt[p, pl.ds(h, 1), :]
        return dtt[p, pl.ds(h, 1), :] * jnp.exp(row[:, 127:128] - row + extra)

    def intra_body(l, p):
        bt_o[p] = act_o[p, :, LOC:LOC + 128].astype(F32).T
        cb = act_o[p, :, LOC + 128:ACT]
        scores = dot_nt(cb, act_o[p, :, LOC:LOC + 128]) * tri
        for j in range(PAIRS):
            mats = []
            for i in (2 * j, 2 * j + 1):
                h = head_row(i)
                col = jnp.broadcast_to(cum_o[p, :, h:h + 1], (BLK, BLK))
                mats.append((jnp.exp(jnp.minimum(col - cumt_o[p, h:h + 1, :], 0.0)) * (scores * dtt_o[p, h:h + 1, :])).astype(BF16))
            xp = act_o[p, :, 128 * j:128 * (j + 1)]
            blk = (0 if j < 6 else 24) + 12 * core + (2 * j) % 12
            dv = jnp.where(low[0:1], dskip_ref[l, blk], dskip_ref[l, blk + 1])
            y = dot(jnp.concatenate(mats, axis=1), jnp.concatenate(split_pair(xp), axis=0)) + dv * xp.astype(F32)
            yloc[p, :, 128 * j:128 * (j + 1)] = y
            ybuf[p, :, 128 * j:128 * (j + 1)] = y.astype(BF16)

    def inter_body(l, p):
        bt = act_r[p, :, LOC:LOC + 128].astype(F32).T
        bt_r[p] = bt
        cf = act_o[p, :, LOC + 128:ACT]
        for j in range(PAIRS):
            lhs = jnp.concatenate([(bt * decays(p, h, cumt_r, dtt_r, 0.0)).astype(BF16) for h in (head_row(2 * j), head_row(2 * j + 1))], axis=1)
            states[:, 128 * j:128 * (j + 1)] = dot(lhs, jnp.concatenate(split_pair(act_r[p, :, 128 * j:128 * (j + 1)]), axis=0))
        for jj in range(PAIRS // 2):
            o = dot(cf, states[:, 256 * jj:256 * (jj + 1)].astype(BF16))
            for s in range(2):
                j = 2 * jj + s
                ha, hb = head_row(2 * j), head_row(2 * j + 1)
                ca = jnp.broadcast_to(cum_o[p, :, ha:ha + 1], (BLK, BLK))
                cb = jnp.broadcast_to(cum_o[p, :, hb:hb + 1], (BLK, BLK))
                y = yloc[p, :, 128 * j:128 * (j + 1)] + o[:, 128 * s:128 * (s + 1)] * jnp.exp(jnp.where(low, ca, cb))
                ybuf[p, :, 128 * j:128 * (j + 1)] = y.astype(BF16)
        y_copy(l, p).start()

    def final_pair(p, q):
        h = 24 * chip + 2 * q
        cols = pl.ds(pl.multiple_of(128 * (6 * chip + q), 128), 128)
        left, right = [], []
        for hh in (h, h + 1):
            end_o = cumt_o[p, pl.ds(hh, 1), :][:, 127:128]
            end_r = cumt_r[p, pl.ds(hh, 1), :][:, 127:128]
            left.append((bt_o[p] * decays(p, hh, cumt_o, dtt_o, end_r * (1.0 - chip_f))).astype(BF16))
            right.append((bt_r[p] * decays(p, hh, cumt_r, dtt_r, end_o * chip_f)).astype(BF16))
        rhs = jnp.concatenate(split_pair(act_o[p, :, cols]) + split_pair(act_r[p, :, cols]), axis=0)
        state = dot(jnp.concatenate(left + right, axis=1), rhs)
        stg[p, pl.ds(2 * q, 2)] = state.T.reshape(2, 64, 128)

    def pass_tail(l):
        c_tail(l).wait_recv()
        f_tail(l).start()

    def pass_half(l, half):
        def go(n):
            c_half(l, half, n).wait_recv()
            f_half(l, half, n).start()
        by_core(go)

    def bulk(l):
        c_half(l, 0, 64).start()
        c_half(l, 1, 64).start()

    def after_other(l, tail):
        for b in range(2):
            tails[l, :, :, pl.ds(pl.multiple_of(LOC * b + HALF * core, 128), HALF)] = tail[:, :, HALF * b:HALF * (b + 1)]
        tails[l, :, :, D_INNER:CONV_DIM] = tail[:, :, LOC:ACT]
        for c in tail_copies(l):
            c.start()

    def next_weights(l):
        @pl.when(l == 0)
        def _():
            xnx, bnx, _ = weight_copies(1)
            for c in xnx + bnx:
                c.start()

    def begin(l):
        def norm_body(p, c):
            v = r_out[p]
            ms = jnp.mean(v * v, axis=-1, keepdims=True)
            hbuf[NB * l + p, pl.ds(own_row, SEG), :] = (v * lax.rsqrt(ms + EPSILON) * pre_ref[pl.ds(l, 1), :]).astype(BF16)
            return c
        with jax.named_scope('norm'):
            lax.fori_loop(0, NB, norm_body, 0)

        c_par(l).start()

        @pl.when(core == 1)
        def _():
            c_tail(l).start()
            c_half(l, 0, 48).start()
            c_half(l, 1, 48).start()

        @pl.when(jnp.logical_and(core == 0, l > 0))
        def _():
            bulk(l)

        @pl.when(jnp.logical_and(jnp.logical_and(core == 1, chip == 1), l > 0))
        def _():
            pass_tail(l)

    def main(l):
        xc, bc, oc = weight_copies(l)

        def z_chunk(n):
            lhs = hbuf[pl.ds(NB * l, NB), pl.ds(own_row, SEG), :].reshape(NB * SEG, D_MODEL)
            cols = slice(512 * n, 512 * (n + 1)) if isinstance(n, int) else pl.ds(pl.multiple_of(512 * n, 512), 512)
            z = round_bf16(dot_nt(lhs, wz[cols, :]))
            sz[:, :, cols] = silu(z).reshape(NB, SEG, 512)

        def z_group(lo):
            for n in range(lo, lo + 3):
                z_copy(l, n).wait()
            for n in range(lo, lo + 3):
                z_chunk(n)

        with jax.named_scope('zproj'):
            z_group(0)

            @pl.when(jnp.logical_and(core == 0, l == 0))
            def _():
                bulk(l)

            @pl.when(l == 0)
            def _():
                z_group(3)
        oc.start()

        @pl.when(l == 0)
        def _():
            for n in range(6):
                z_copy(1, n).start()

        @pl.when(l == 0)
        def _():
            for c in params[2:]:
                c.wait()

        for b in range(2):
            src = pl.multiple_of(LOC * b + HALF * core, 128)
            cwl[0:4, HALF * b:HALF * (b + 1)] = cw_ref[l, :, pl.ds(src, HALF)]
            cwl[4:5, HALF * b:HALF * (b + 1)] = cb_ref[pl.ds(l, 1), pl.ds(src, HALF)]
        cwl[0:4, LOC:ACT] = cw_ref[l, :, D_INNER:CONV_DIM]
        cwl[4:5, LOC:ACT] = cb_ref[pl.ds(l, 1), D_INNER:CONV_DIM]
        prm[0:1, 0:HEADS] = dtb_ref[pl.ds(l, 1), :]
        prm[1:2, 0:HEADS] = -jnp.exp(alog_ref[pl.ds(l, 1), :])

        with jax.named_scope('wait_h'):
            c_par(l).wait_recv()
            for c in bc + xc:
                c.wait()

            @pl.when(jnp.logical_and(jnp.logical_and(core == 1, chip == 1), l == 0))
            def _():
                pass_tail(l)

            @pl.when(jnp.logical_and(chip == 1, core == 0))
            def _():
                f_tail(l).wait_recv()
        with jax.named_scope('own_block'):
            block(l, 0, NB, own_blk, act_o, tail_o, cumt_o, dtt_o, cum_o, True, LOC)

        def intra_end(p):
            @pl.when(chip == 0)
            def _():
                y_copy(l, p).start()

            @pl.when(jnp.logical_and(chip == 1, p == 1))
            def _():
                pass_half(l, 0)

        def intra_plain(p, c):
            intra_body(l, p)
            intra_end(p)
            return c

        def intra_z(p, c):
            z_chunk(3 + p)
            intra_body(l, p)
            intra_end(p)
            return c

        with jax.named_scope('intra'):
            @pl.when(l > 0)
            def _():
                for n in range(3, 6):
                    z_copy(l, n).wait()
            split = jnp.where(l == 0, 0, 3)
            lax.fori_loop(0, split, intra_z, 0)
            lax.fori_loop(split, NB, intra_plain, 0)

        @pl.when(chip == 1)
        def _():
            with jax.named_scope('wait_r0'):
                wait_half(l, 0)

            def half_body(half, c):
                with jax.named_scope('oth_block'):
                    block(l, 2 * half, 2, oth_blk, act_r, None, cumt_r, dtt_r, None, False, LOC)

                @pl.when(half == 0)
                def _():
                    with jax.named_scope('wait_c1'):
                        pass_half(l, 1)
                with jax.named_scope('inter'):
                    lax.fori_loop(2 * half, 2 * half + 2, lambda p, c: (inter_body(l, p), c)[1], 0)

                @pl.when(half == 0)
                def _():
                    with jax.named_scope('wait_f1'):
                        wait_half(l, 1)
                return c
            lax.fori_loop(0, 2, half_body, 0)
            after_other(l, tail_o)
            next_weights(l)

        def gate_body(p, c):
            y_copy(l, p).wait()
            total = jnp.zeros((SEG, 1), F32)
            for b in range(2):
                for own in range(2):
                    cols = pl.ds(pl.multiple_of(LOC * b + HALF * (core if own else 1 - core), 128), HALF)
                    if own:
                        y = ybuf[p, pl.ds(pl.multiple_of(SEG * core, 16), SEG), HALF * b:HALF * (b + 1)]
                    else:
                        y = yrecv[NB * l + p, :, HALF * b:HALF * (b + 1)]
                    g = y.astype(F32) * sz[p, :, cols]
                    sz[p, :, cols] = g
                    total = total + jnp.sum(g * g, axis=-1, keepdims=True)
            scale = lax.rsqrt(total * (1.0 / D_INNER) + EPSILON)
            for b in range(4):
                cols = slice(HALF * b, HALF * (b + 1))
                gn[p, :, cols] = (sz[p, :, cols] * scale * gw_ref[l, :, cols]).astype(BF16)
            return c
        with jax.named_scope('gate'):
            lax.fori_loop(0, NB, gate_body, 0)
            oc.wait()

        def out_chunk(n):
            cols = pl.ds(pl.multiple_of(512 * n, 512), 512)
            o = dot(gn[...].reshape(NB * SEG, D_INNER), wout[:, cols])
            r_out[:, :, cols] = r_out[:, :, cols] + o.reshape(NB, SEG, 512)

        def send_r(n):
            @pl.when(l == LAYERS - 1)
            def _():
                r_copy(n).start()

        def out_final(n, c):
            out_chunk(n)
            for q in range(2):
                for p in range(NB):
                    final_pair(p, 2 * n + q)
            out_heads(l, n).start()
            send_r(n)
            return c

        def out_plain(n, c):
            out_chunk(n)
            send_r(n)
            return c

        with jax.named_scope('outproj'):
            @pl.when(chip == 0)
            def _():
                lax.fori_loop(0, 3, out_plain, 0)

            @pl.when(chip == 1)
            def _():
                @pl.when(l > 0)
                def _():
                    for n in range(3):
                        out_heads(0, n).wait()
                lax.fori_loop(0, 3, out_final, 0)

        @pl.when(chip == 0)
        def _():
            with jax.named_scope('pass_d'):
                @pl.when(core == 1)
                def _():
                    pass_tail(l)
                pass_half(l, 0)

    def deferred(l):
        with jax.named_scope('wait_d'):
            @pl.when(core == 0)
            def _():
                f_tail(l).wait_recv()

            @pl.when(l > 0)
            def _():
                for p in range(NB):
                    out_prompt(0, p).wait()
        with jax.named_scope('last_rows'):
            last_rows(l, tail_r)
            after_other(l, tail_r)

        def half_body(half, c):
            with jax.named_scope('wait_dh'):
                wait_half(l, half)
            with jax.named_scope('oth_block'):
                block(l, 2 * half, 2, oth_blk, act_r, None, cumt_r, dtt_r, None, False, HALF)

            @pl.when(half == 0)
            def _():
                with jax.named_scope('wait_c1'):
                    pass_half(l, 1)

            @pl.when(half == 1)
            def _():
                next_weights(l)

            def final_body(p, cc):
                bt_r[p] = act_r[p, :, LOC:LOC + 128].astype(F32).T
                for q in range(6):
                    final_pair(p, q)
                out_prompt(l, p).start()
                return cc
            with jax.named_scope('final'):
                lax.fori_loop(2 * half, 2 * half + 2, final_body, 0)
            return c
        lax.fori_loop(0, 2, half_body, 0)

    def step(l, carry):
        @pl.when(l < LAYERS)
        def _():
            begin(l)

        @pl.when(jnp.logical_and(chip == 0, l > 0))
        def _():
            deferred(l - 1)

        @pl.when(l < LAYERS)
        def _():
            main(l)
        return carry

    lax.fori_loop(0, LAYERS + 1, step, 0)
    for l in range(LAYERS):
        for c in tail_copies(l):
            c.wait()
        tail_copy(l).start()
    for l in range(LAYERS):
        c_par(l).wait_send()

        @pl.when(core == 1)
        def _():
            c_tail(l).wait_send()
            f_tail(l).wait_send()

        def sent(n):
            for half in range(2):
                c_half(l, half, n).wait_send()
                f_half(l, half, n).wait_send()
        by_core(sent)
        tail_copy(l).wait()

    @pl.when(chip == 0)
    def _():
        for p in range(NB):
            out_prompt(LAYERS - 1, p).wait()

    @pl.when(chip == 1)
    def _():
        for n in range(3):
            out_heads(LAYERS - 1, n).wait()
    for n in range(3):
        r_copy(n).wait()


def copy_kernel(r_ref, ssm_ref, tail_ref, r_out, ssm_out, conv_out, tbuf, cbuf, sems):
    whole = [pltpu.make_async_copy(r_ref, r_out, sems.at[0]), pltpu.make_async_copy(ssm_ref, ssm_out, sems.at[1])]
    load = pltpu.make_async_copy(tail_ref, tbuf, sems.at[2])
    load.start()
    for c in whole:
        c.start()
    load.wait()
    for p in range(NB):
        for l in range(LAYERS):
            rows = tbuf[l, p].astype(F32)
            for k in range(3):
                cbuf[p, k, l:l + 1, :] = rows[13 + k:14 + k, :].astype(BF16)
    store = pltpu.make_async_copy(cbuf, conv_out, sems.at[3])
    store.start()
    for c in whole + [store]:
        c.wait()


def solution(mesh):
    hbm = pl.BlockSpec(memory_space=pl.ANY)

    def forward(resid, pre_norm, w_in, conv_w, conv_b, dt_bias, a_log, d_skip, gate_norm, w_out):
        r, ssm, tails = pl.pallas_call(
            kernel,
            out_shape=(
                pltpu.VMEM((NB, SEG, D_MODEL), F32),
                pltpu.VMEM((NB, LAYERS, 12, 64, 128), F32),
                pltpu.VMEM((LAYERS, NB, 16, CONV_DIM), BF16),
            ),
            in_specs=[hbm] * 10,
            out_specs=(hbm, hbm, hbm),
            scratch_shapes=[
                pltpu.VMEM((NB, SEG, D_MODEL), F32),
                pltpu.VMEM((LAYERS, D_MODEL), F32),
                pltpu.VMEM((LAYERS, 4, CONV_DIM), F32),
                pltpu.VMEM((LAYERS, CONV_DIM), F32),
                pltpu.VMEM((LAYERS, HEADS), F32),
                pltpu.VMEM((LAYERS, HEADS), F32),
                pltpu.SMEM((LAYERS, HEADS), F32),
                pltpu.VMEM((LAYERS, 1, D_INNER), F32),
                pltpu.VMEM((LAYERS * NB, ROWS, D_MODEL), BF16),
                pltpu.VMEM((NB, SEG, D_INNER), F32),
                pltpu.VMEM((D_INNER, D_MODEL), BF16),
                pltpu.VMEM((LOC, D_MODEL), BF16),
                pltpu.VMEM((384, D_MODEL), BF16),
                pltpu.VMEM((D_INNER, D_MODEL), BF16),
                pltpu.VMEM((4, NB, EXT, 128), F32),
                pltpu.VMEM((4, NB, EXT, 128), F32),
                pltpu.VMEM((BLK, LOC), F32),
                pltpu.VMEM((NB, BLK, BLK), F32),
                pltpu.VMEM((NB, BLK, BLK), F32),
                pltpu.VMEM((NB, BLK, ACT), BF16),
                pltpu.VMEM((NB, BLK, ACT), BF16),
                pltpu.VMEM((NB, BLK, LOC), F32),
                pltpu.VMEM((NB, BLK, LOC), BF16),
                pltpu.VMEM((LAYERS * NB, SEG, LOC), BF16),
                pltpu.VMEM((NB, SEG, D_INNER), BF16),
                pltpu.VMEM((NB, 12, 64, 128), F32),
                pltpu.VMEM((LAYERS, NB, 16, CONV_DIM), BF16),
                pltpu.VMEM((NB, 16, ACT), BF16),
                pltpu.VMEM((NB, 16, ACT), BF16),
                pltpu.VMEM((NB, BLK, BLK), F32),
                pltpu.VMEM((NB, 40, BLK), F32),
                pltpu.VMEM((NB, 40, BLK), F32),
                pltpu.VMEM((NB, 40, BLK), F32),
                pltpu.VMEM((NB, 40, BLK), F32),
                pltpu.VMEM((8, ACT), F32),
                pltpu.VMEM((8, 128), F32),
                pltpu.SemaphoreType.DMA((12,)),
                pltpu.SemaphoreType.DMA((LAYERS, 7)),
                pltpu.SemaphoreType.DMA((LAYERS, 7)),
                pltpu.SemaphoreType.DMA((LAYERS, NB)),
                pltpu.SemaphoreType.DMA((LAYERS, NB)),
                pltpu.SemaphoreType.DMA((LAYERS, 2)),
                pltpu.SemaphoreType.DMA((LAYERS, 2)),
                pltpu.SemaphoreType.DMA((NB,)),
                pltpu.SemaphoreType.DMA((8,)),
                pltpu.SemaphoreType.DMA((3,)),
                pltpu.SemaphoreType.DMA((LAYERS,)),
            ],
            compiler_params=pltpu.CompilerParams(collective_id=0, has_side_effects=True, vmem_limit_bytes=VMEM_LIMIT),
        )(resid, pre_norm, jnp.swapaxes(w_in, 1, 2), jnp.swapaxes(conv_w, 1, 2), conv_b, dt_bias, a_log, d_skip, gate_norm, w_out)
        r, ssm, conv = pl.pallas_call(
            copy_kernel,
            out_shape=(
                jax.ShapeDtypeStruct(r.shape, F32),
                jax.ShapeDtypeStruct(ssm.shape, F32),
                jax.ShapeDtypeStruct((NB, 3, LAYERS, CONV_DIM), BF16),
            ),
            in_specs=[hbm] * 3,
            out_specs=(hbm, hbm, hbm),
            scratch_shapes=[
                pltpu.VMEM((LAYERS, NB, 16, CONV_DIM), BF16),
                pltpu.VMEM((NB, 3, LAYERS, CONV_DIM), BF16),
                pltpu.SemaphoreType.DMA((4,)),
            ],
            compiler_params=pltpu.CompilerParams(vmem_limit_bytes=4 * 1024 * 1024),
        )(r, ssm, tails)
        return r, ssm, jnp.transpose(conv, (0, 2, 3, 1))

    return jax.shard_map(forward, mesh=mesh, in_specs=(P('dp', 'sp', None), P(), P(), P(), P(), P(), P(), P(), P(), P()), out_specs=(P('dp', 'sp', None), P('dp', None, 'sp', None, None), P('dp', None, None, None)), check_vma=False)
```

```python
import functools

import jax
import jax.numpy as jnp
from jax import lax
from jax.experimental import pallas as pl
from jax.experimental.pallas import tpu as pltpu
from jax.sharding import PartitionSpec as P

F32 = jnp.float32
BF16 = jnp.bfloat16
EPSILON = 1e-5
LAYERS = 2
NB = 4
SEG = 64
BLK = 128
HALO = 16
EXT = BLK + HALO
ROWS = HALO + 2 * BLK
D_MODEL = 1536
D_INNER = 3072
CONV_DIM = 3328
HEADS = 48
HALF = 768
LOC = 1536
ACT = LOC + 256
PAIRS = 12
VMEM_LIMIT = 58400000
NT = (((1,), (1,)), ((), ()))


def dot(a, b):
    return jnp.dot(a, b, preferred_element_type=F32)


def dot_nt(a, b):
    return lax.dot_general(a, b, NT, preferred_element_type=F32)


def round_bf16(v):
    return v.astype(BF16).astype(F32)


def silu(v):
    half = 0.5 * v
    return half * jnp.tanh(half) + half


def head_row(i):
    return i if i < 12 else i + 12


def kernel(resid_hbm, pre_hbm, w_in_ref, cw_hbm, cb_hbm, dtb_hbm, alog_hbm, dskip_hbm, gw_hbm, w_out_ref,
           r_hbm, ssm_out, tail_out,
           r_out, pre_ref, cw_ref, cb_ref, dtb_ref, alog_ref, dskip_ref, gw_ref, hbuf, sz, wz, wx, wbc, wout, rawa, rawb, spread, scaled, act_o, act_r, yloc, ybuf, yrecv, gn, stg, tails, tail_o, tail_r,
           cum_o, cum_r, dt_o, dt_r, cumt_o, dtt_o, cwl, prm,
           wsem, hsend, hrecv, ysend, yrecv_sem, tsend, trecv, osem, psem, rsem, tout):
    me = lax.axis_index('sp')
    chip = me // 2
    core = me % 2
    partner = chip * 2 + (1 - core)
    other = (1 - chip) * 2 + core
    chip_f = chip.astype(F32)
    core_f = core.astype(F32)

    def weight_copies(l):
        xc = [pltpu.make_async_copy(w_in_ref.at[l, pl.ds(pl.multiple_of(D_INNER + LOC * b + HALF * core, 16), HALF), :], wx.at[pl.ds(HALF * b, HALF), :], wsem.at[6 + b]) for b in range(2)]
        bc = [pltpu.make_async_copy(w_in_ref.at[l, pl.ds(src, n), :], wbc.at[pl.ds(dst, n), :], wsem.at[sem]) for src, n, dst, sem in ((2 * D_INNER, 128, 0, 8), (2 * D_INNER + 256, HEADS, 128, 9), (2 * D_INNER + 128, 128, 256, 10))]
        oc = pltpu.make_async_copy(w_out_ref.at[l], wout, wsem.at[11])
        return xc, bc, oc

    def z_copy(l, n):
        rows = pl.ds(pl.multiple_of(512 * n, 16), 512)
        return pltpu.make_async_copy(w_in_ref.at[l, rows, :], wz.at[rows, :], wsem.at[n])

    params = [pltpu.make_async_copy(src, dst, psem.at[i]) for i, (src, dst) in enumerate(((resid_hbm, r_out), (pre_hbm, pre_ref), (cw_hbm, cw_ref), (cb_hbm, cb_ref), (dtb_hbm, dtb_ref), (alog_hbm, alog_ref), (dskip_hbm, dskip_ref), (gw_hbm, gw_ref)))]
    xc0, bc0, oc0 = weight_copies(0)
    params[0].start()
    params[1].start()
    z_copy(0, 0).start()
    for c in params[2:]:
        c.start()
    for n in range(1, 6):
        z_copy(0, n).start()

    barrier = pltpu.get_barrier_semaphore()
    for step in range(1, 4):
        pl.semaphore_signal(barrier, inc=1, device_id={'sp': (me + step) % 4}, device_id_type=pl.DeviceIdType.MESH)

    hbuf[:, 0:HALO, :] = jnp.zeros((LAYERS * NB, HALO, D_MODEL), BF16)
    wbc[176:256, :] = jnp.zeros((80, D_MODEL), BF16)
    prm[...] = jnp.zeros((8, 128), F32)
    for c in bc0 + xc0:
        c.start()
    rows_i = lax.broadcasted_iota(jnp.int32, (BLK, 64), 0)
    for i in range(24):
        h = head_row(i)
        hit = (rows_i == h) | (rows_i == h + 40) | (rows_i == h + 80)
        spread[:, 64 * i:64 * (i + 1)] = jnp.where(hit, 1.0, 0.0).astype(BF16)

    with jax.named_scope('params'):
        for c in params[:2]:
            c.wait()
    with jax.named_scope('barrier'):
        pl.semaphore_wait(barrier, 3)

    own_row = pl.multiple_of(HALO + BLK * chip + SEG * core, 16)
    oth_row = pl.multiple_of(HALO + BLK * (1 - chip) + SEG * core, 16)
    own_blk = pl.multiple_of(BLK * chip, 16)
    oth_blk = pl.multiple_of(BLK * (1 - chip), 16)

    iota_r = lax.broadcasted_iota(jnp.int32, (BLK, BLK), 0)
    iota_c = lax.broadcasted_iota(jnp.int32, (BLK, BLK), 1)

    def remote(src, dst, ssem, rsem, dev):
        return pltpu.make_async_remote_copy(src_ref=src, dst_ref=dst, send_sem=ssem, recv_sem=rsem, device_id={'sp': dev}, device_id_type=pl.DeviceIdType.MESH)

    tri = (iota_r >= iota_c).astype(F32)
    low = iota_c < 64

    def hslice(l, p0, n, row, size):
        return hbuf.at[pl.ds(NB * l + p0, n), pl.ds(row, size), :]

    def same(l, idx, p0, n, row, size, dev):
        ref = hslice(l, p0, n, row, size)
        return remote(ref, ref, hsend.at[l, idx], hrecv.at[l, idx], dev)

    def c_par(l):
        return same(l, 0, 0, NB, own_row, SEG, partner)

    def c_tail(l):
        return same(l, 1, 0, NB, own_row + 48, 16, other)

    def c_half(l, half, size):
        return same(l, 2 + half, 2 * half, 2, own_row, size, other)

    def f_tail(l):
        return same(l, 4, 0, NB, oth_row + 48, 16, partner)

    def f_half(l, half, size):
        return same(l, 5 + half, 2 * half, 2, oth_row, size, partner)

    def by_core(fn):
        @pl.when(core == 0)
        def _():
            fn(64)

        @pl.when(core == 1)
        def _():
            fn(48)

    def wait_half(l, half):
        by_core(lambda n: f_half(l, half, 112 - n).wait_recv())

    def y_copy(l, p):
        src = ybuf.at[p, pl.ds(pl.multiple_of(SEG * (1 - core), 16), SEG), :]
        return remote(src, yrecv.at[NB * l + p], ysend.at[l, p], yrecv_sem.at[l, p], partner)

    def out_prompt(l, p):
        return pltpu.make_async_copy(stg.at[p], ssm_out.at[p, l], osem.at[p])

    def r_copy(n):
        cols = pl.ds(pl.multiple_of(512 * n, 512), 512)
        return pltpu.make_async_copy(r_out.at[:, :, cols], r_hbm.at[:, :, cols], rsem.at[n])

    def tail_copy(l):
        return pltpu.make_async_copy(tails.at[l], tail_out.at[l], tout.at[l])

    def tail_copies(l):
        res = []
        for b in range(2):
            ref = tails.at[l, :, :, pl.ds(pl.multiple_of(LOC * b + HALF * core, 128), HALF)]
            res.append(remote(ref, ref, tsend.at[l, b], trecv.at[l, b], partner))
        return res

    def conv_chunk(act, src, first, groups, i, p, dst):
        for g in range(groups):
            cols = slice(dst + 128 * g, dst + 128 * (g + 1))
            acc = cwl[0:1, cols] * src[first + g, i, 13:141, :]
            for k in range(1, 4):
                acc = acc + cwl[k:k + 1, cols] * src[first + g, i, 13 + k:141 + k, :]
            act[p, :, cols] = silu(acc + cwl[4:5, cols]).astype(BF16)

    def block(l, p0, np_, row, act, tail, cum, dts, trans, with_c, widths):
        def project(w, rows, dst):
            lhs = hbuf[pl.ds(NB * l + p0, np_), pl.ds(row, EXT), :].reshape(np_ * EXT, D_MODEL)
            res = round_bf16(dot_nt(lhs, w[rows, :]))
            for g in range((rows.stop - rows.start) // 128):
                dst[g, 0:np_] = res[:, 128 * g:128 * (g + 1)].reshape(np_, EXT, 128)

        def finish_bc(src):
            for i in range(np_):
                p = p0 + i
                for g, dst in ((0, LOC), (2, LOC + 128))[:2 if with_c else 1]:
                    if tail is not None:
                        tail[p, :, dst:dst + 128] = src[g, i, BLK:EXT, :].astype(BF16)
                    conv_chunk(act, src, g, 1, i, p, dst)
                v = src[1, i, HALO:EXT, :] + prm[0:1, :]
                dt = round_bf16(jnp.maximum(v, 0.0) + jnp.log1p(jnp.exp(-jnp.abs(v))))
                logs = dt * prm[1:2, :]
                dt = dt * (1.0 - core_f) + pltpu.roll(dt, 116, 1) * core_f
                logs = logs * (1.0 - core_f) + pltpu.roll(logs, 116, 1) * core_f
                cums = jnp.dot(tri, logs, precision=lax.Precision.HIGHEST, preferred_element_type=F32)
                cum[p] = cums
                dts[p] = dt
                if trans is not None:
                    trans[0][p] = cums.T[0:40]
                    trans[1][p] = dt.T[0:40]

        def finish_x(src, col, n):
            for i in range(np_):
                if tail is not None:
                    for g in range(n // 128):
                        tail[p0 + i, :, col + 128 * g:col + 128 * (g + 1)] = src[g, i, BLK:EXT, :].astype(BF16)
                conv_chunk(act, src, 0, n // 128, i, p0 + i, col)

        project(wbc, slice(0, 384 if with_c else 256), rawa)
        pending, nxt = (lambda: finish_bc(rawa)), rawb
        col = 0
        for n in widths:
            project(wx, slice(col, col + n), nxt)
            pending()
            pending = functools.partial(finish_x, nxt, col, n)
            col += n
            nxt = rawa if nxt is rawb else rawb
        pending()

    def last_rows(l, tail):
        lhs = hbuf[pl.ds(NB * l, NB), ROWS - 16:ROWS, :].reshape(NB * 16, D_MODEL)
        for col in range(0, LOC, 512):
            tail[:, :, col:col + 512] = dot_nt(lhs, wx[col:col + 512, :]).astype(BF16).reshape(NB, 16, 512)
        res = dot_nt(lhs, wbc[...]).astype(BF16).reshape(NB, 16, 384)
        tail[:, :, LOC:LOC + 128] = res[:, :, 0:128]
        tail[:, :, LOC + 128:ACT] = res[:, :, 256:384]

    zero = jnp.zeros((), BF16)

    def split_pair(xp):
        return [jnp.where(low, xp, zero), jnp.where(low, zero, xp)]

    lane = lax.broadcasted_iota(jnp.int32, (BLK, BLK), 1)

    def three_terms(v):
        v = jnp.where(lane < 40, v, 0.0)
        hi = round_bf16(v)
        mid = round_bf16(v - hi)
        return (hi + pltpu.roll(mid, 40, 1) + pltpu.roll((v - hi) - mid, 80, 1)).astype(BF16)

    def weighted(act, p, cols, terms):
        return (act[p, :, cols].astype(F32) * dot(terms, spread[:, cols])).astype(BF16)

    def intra_body(l, p):
        cb = act_o[p, :, LOC + 128:ACT]
        scores = dot_nt(cb, act_o[p, :, LOC:LOC + 128]) * tri
        for j in range(PAIRS):
            mats = []
            for i in (2 * j, 2 * j + 1):
                h = head_row(i)
                col = jnp.broadcast_to(cum_o[p, :, h:h + 1], (BLK, BLK))
                mats.append((jnp.exp(jnp.minimum(col - cumt_o[p, h:h + 1, :], 0.0)) * (scores * dtt_o[p, h:h + 1, :])).astype(BF16))
            xp = act_o[p, :, 128 * j:128 * (j + 1)]
            blk = (0 if j < 6 else 24) + 12 * core + (2 * j) % 12
            dv = jnp.where(low[0:1], dskip_ref[l, blk], dskip_ref[l, blk + 1])
            y = dot(jnp.concatenate(mats, axis=1), jnp.concatenate(split_pair(xp), axis=0)) + dv * xp.astype(F32)
            yloc[p, :, 128 * j:128 * (j + 1)] = y
            ybuf[p, :, 128 * j:128 * (j + 1)] = y.astype(BF16)

    def inter_half(l, half):
        prompts = [(0, 2 * half, rawa), (1, 2 * half + 1, rawb)]
        bts, ends = [], []
        for i, p, _ in prompts:
            cum = cum_r[p]
            bts.append(act_r[p, :, LOC:LOC + 128].astype(F32).T.astype(BF16))
            ends.append(three_terms(dt_r[p] * jnp.exp(cum[127:128, :] - cum)))
        for i, p, _ in prompts:
            for j in range(6):
                cols = slice(256 * j, 256 * (j + 1))
                scaled[i, :, cols] = weighted(act_r, p, cols, ends[i])
        for i, p, states in prompts:
            for j in range(6):
                state = dot(bts[i], scaled[i, :, 256 * j:256 * (j + 1)])
                for k in range(2):
                    states[(2 * j + k) // 4, (2 * j + k) % 4, 0:BLK, :] = state[:, 128 * k:128 * (k + 1)]
        for i, p, states in prompts:
            cf = act_o[p, :, LOC + 128:ACT]
            start = three_terms(jnp.exp(cum_o[p]))
            for j in range(6):
                cols = slice(256 * j, 256 * (j + 1))
                state = jnp.concatenate([states[(2 * j + k) // 4, (2 * j + k) % 4, 0:BLK, :].astype(BF16) for k in range(2)], axis=1)
                y = yloc[p, :, cols] + dot(cf, state) * dot(start, spread[:, cols])
                ybuf[p, :, cols] = y.astype(BF16)
        for i, p, _ in prompts:
            y_copy(l, p).start()

    def final_inputs(p):
        co, cr = cum_o[p], cum_r[p]
        eo, er = co[127:128, :], cr[127:128, :]
        fo = three_terms(dt_o[p] * jnp.exp(eo - co + er * (1.0 - chip_f)))
        fr = three_terms(dt_r[p] * jnp.exp(er - cr + eo * chip_f))
        for j in range(3):
            cols = pl.ds(pl.multiple_of(HALF * chip + 256 * j, 256), 256)
            ybuf[p, :, 256 * j:256 * (j + 1)] = weighted(act_o, p, cols, fo)
            ybuf[p, :, HALF + 256 * j:HALF + 256 * (j + 1)] = weighted(act_r, p, cols, fr)

    def final_states(p):
        bts = jnp.concatenate([act[p, :, LOC:LOC + 128].astype(F32).T.astype(BF16) for act in (act_o, act_r)], axis=1)
        for j in range(3):
            state = dot(bts, jnp.concatenate([ybuf[p, :, 256 * j:256 * (j + 1)], ybuf[p, :, HALF + 256 * j:HALF + 256 * (j + 1)]], axis=0))
            stg[p, 4 * j:4 * j + 4] = state.T.reshape(4, 64, 128)

    def wait_states(l):
        @pl.when(l > 0)
        def _():
            for p in range(NB):
                out_prompt(0, p).wait()

    def pass_tail(l):
        c_tail(l).wait_recv()
        f_tail(l).start()

    def pass_half(l, half):
        def go(n):
            c_half(l, half, n).wait_recv()
            f_half(l, half, n).start()
        by_core(go)

    def bulk(l):
        c_half(l, 0, 64).start()
        c_half(l, 1, 64).start()

    def after_other(l, tail):
        for b in range(2):
            tails[l, :, :, pl.ds(pl.multiple_of(LOC * b + HALF * core, 128), HALF)] = tail[:, :, HALF * b:HALF * (b + 1)]
        tails[l, :, :, D_INNER:CONV_DIM] = tail[:, :, LOC:ACT]
        for c in tail_copies(l):
            c.start()

    def next_weights(l):
        @pl.when(l == 0)
        def _():
            xnx, bnx, _ = weight_copies(1)
            for c in xnx + bnx:
                c.start()

    def begin(l):
        def norm_body(p, c):
            v = r_out[p]
            ms = jnp.mean(v * v, axis=-1, keepdims=True)
            hbuf[NB * l + p, pl.ds(own_row, SEG), :] = (v * lax.rsqrt(ms + EPSILON) * pre_ref[pl.ds(l, 1), :]).astype(BF16)
            return c
        with jax.named_scope('norm'):
            lax.fori_loop(0, NB, norm_body, 0)

        c_par(l).start()

        @pl.when(core == 1)
        def _():
            c_tail(l).start()
            c_half(l, 0, 48).start()
            c_half(l, 1, 48).start()

        @pl.when(jnp.logical_and(core == 0, l > 0))
        def _():
            bulk(l)

        @pl.when(jnp.logical_and(jnp.logical_and(core == 1, chip == 1), l > 0))
        def _():
            pass_tail(l)

    def main(l):
        xc, bc, oc = weight_copies(l)

        def z_chunk(n):
            lhs = hbuf[pl.ds(NB * l, NB), pl.ds(own_row, SEG), :].reshape(NB * SEG, D_MODEL)
            cols = slice(512 * n, 512 * (n + 1)) if isinstance(n, int) else pl.ds(pl.multiple_of(512 * n, 512), 512)
            z = round_bf16(dot_nt(lhs, wz[cols, :]))
            sz[:, :, cols] = silu(z).reshape(NB, SEG, 512)

        def z_group(lo):
            for n in range(lo, lo + 3):
                z_copy(l, n).wait()
            for n in range(lo, lo + 3):
                z_chunk(n)

        with jax.named_scope('zproj'):
            z_group(0)

            @pl.when(jnp.logical_and(core == 0, l == 0))
            def _():
                bulk(l)

            @pl.when(l == 0)
            def _():
                z_group(3)
        oc.start()

        @pl.when(l == 0)
        def _():
            for n in range(6):
                z_copy(1, n).start()

        @pl.when(l == 0)
        def _():
            for c in params[2:]:
                c.wait()

        for b in range(2):
            src = pl.multiple_of(LOC * b + HALF * core, 128)
            cwl[0:4, HALF * b:HALF * (b + 1)] = cw_ref[l, :, pl.ds(src, HALF)]
            cwl[4:5, HALF * b:HALF * (b + 1)] = cb_ref[pl.ds(l, 1), pl.ds(src, HALF)]
        cwl[0:4, LOC:ACT] = cw_ref[l, :, D_INNER:CONV_DIM]
        cwl[4:5, LOC:ACT] = cb_ref[pl.ds(l, 1), D_INNER:CONV_DIM]
        prm[0:1, 0:HEADS] = dtb_ref[pl.ds(l, 1), :]
        prm[1:2, 0:HEADS] = -jnp.exp(alog_ref[pl.ds(l, 1), :])

        with jax.named_scope('wait_h'):
            c_par(l).wait_recv()
            for c in bc + xc:
                c.wait()

            @pl.when(jnp.logical_and(jnp.logical_and(core == 1, chip == 1), l == 0))
            def _():
                pass_tail(l)

            @pl.when(jnp.logical_and(chip == 1, core == 0))
            def _():
                f_tail(l).wait_recv()
        with jax.named_scope('own_block'):
            block(l, 0, NB, own_blk, act_o, tail_o, cum_o, dt_o, (cumt_o, dtt_o), True, (512, 512, 256, 256))

        def intra_end(p):
            @pl.when(chip == 0)
            def _():
                y_copy(l, p).start()

            @pl.when(jnp.logical_and(chip == 1, p == 1))
            def _():
                pass_half(l, 0)

        def intra_plain(p, c):
            intra_body(l, p)
            intra_end(p)
            return c

        def intra_z(p, c):
            z_chunk(3 + p)
            intra_body(l, p)
            intra_end(p)
            return c

        with jax.named_scope('intra'):
            @pl.when(l > 0)
            def _():
                for n in range(3, 6):
                    z_copy(l, n).wait()
            split = jnp.where(l == 0, 0, 3)
            lax.fori_loop(0, split, intra_z, 0)
            lax.fori_loop(split, NB, intra_plain, 0)

        @pl.when(chip == 1)
        def _():
            with jax.named_scope('wait_r0'):
                wait_half(l, 0)

            def half_body(half, c):
                with jax.named_scope('oth_block'):
                    block(l, 2 * half, 2, oth_blk, act_r, None, cum_r, dt_r, None, False, (512, 512, 256, 256))

                @pl.when(half == 0)
                def _():
                    with jax.named_scope('wait_c1'):
                        pass_half(l, 1)
                with jax.named_scope('inter'):
                    inter_half(l, half)

                @pl.when(half == 0)
                def _():
                    with jax.named_scope('wait_f1'):
                        wait_half(l, 1)
                return c
            lax.fori_loop(0, 2, half_body, 0)
            after_other(l, tail_o)
            next_weights(l)

        def gate_body(p, c):
            y_copy(l, p).wait()
            total = jnp.zeros((SEG, 1), F32)
            for b in range(2):
                for own in range(2):
                    cols = pl.ds(pl.multiple_of(LOC * b + HALF * (core if own else 1 - core), 128), HALF)
                    if own:
                        y = ybuf[p, pl.ds(pl.multiple_of(SEG * core, 16), SEG), HALF * b:HALF * (b + 1)]
                    else:
                        y = yrecv[NB * l + p, :, HALF * b:HALF * (b + 1)]
                    g = y.astype(F32) * sz[p, :, cols]
                    sz[p, :, cols] = g
                    total = total + jnp.sum(g * g, axis=-1, keepdims=True)
            scale = lax.rsqrt(total * (1.0 / D_INNER) + EPSILON)
            for b in range(4):
                cols = slice(HALF * b, HALF * (b + 1))
                gn[p, :, cols] = (sz[p, :, cols] * scale * gw_ref[l, :, cols]).astype(BF16)
            return c
        with jax.named_scope('gate'):
            lax.fori_loop(0, NB, gate_body, 0)
            oc.wait()

        def out_chunk(n):
            cols = slice(512 * n, 512 * (n + 1))
            o = dot(gn[...].reshape(NB * SEG, D_INNER), wout[:, cols])
            r_out[:, :, cols] = r_out[:, :, cols] + o.reshape(NB, SEG, 512)

        with jax.named_scope('outproj'):
            @pl.when(chip == 0)
            def _():
                for n in range(3):
                    out_chunk(n)

            @pl.when(chip == 1)
            def _():
                wait_states(l)
                final_inputs(0)
                final_inputs(1)
                out_chunk(0)
                final_states(0)
                final_states(1)
                final_inputs(2)
                final_inputs(3)
                out_chunk(1)
                final_states(2)
                final_states(3)
                out_chunk(2)
                for p in range(NB):
                    out_prompt(l, p).start()

            @pl.when(l == LAYERS - 1)
            def _():
                for n in range(3):
                    r_copy(n).start()

        @pl.when(chip == 0)
        def _():
            with jax.named_scope('pass_d'):
                @pl.when(core == 1)
                def _():
                    pass_tail(l)
                pass_half(l, 0)

    def deferred(l):
        with jax.named_scope('wait_d'):
            @pl.when(core == 0)
            def _():
                f_tail(l).wait_recv()

            wait_states(l)
        with jax.named_scope('last_rows'):
            last_rows(l, tail_r)
            after_other(l, tail_r)

        def half_body(half, c):
            with jax.named_scope('wait_dh'):
                wait_half(l, half)
            with jax.named_scope('oth_block'):
                block(l, 2 * half, 2, oth_blk, act_r, None, cum_r, dt_r, None, False, (512, 256))

            @pl.when(jnp.logical_and(half == 0, l == 0))
            def _():
                pass_half(l, 1)

            @pl.when(half == 1)
            def _():
                next_weights(l)

            with jax.named_scope('final'):
                for i in range(2):
                    final_inputs(2 * half + i)
                for i in range(2):
                    final_states(2 * half + i)
                for i in range(2):
                    out_prompt(l, 2 * half + i).start()

            @pl.when(jnp.logical_and(half == 0, l > 0))
            def _():
                with jax.named_scope('wait_c1'):
                    pass_half(l, 1)
            return c
        lax.fori_loop(0, 2, half_body, 0)

    def step(l, carry):
        @pl.when(l < LAYERS)
        def _():
            begin(l)

        @pl.when(jnp.logical_and(chip == 0, l > 0))
        def _():
            deferred(l - 1)

        @pl.when(l < LAYERS)
        def _():
            main(l)
        return carry

    lax.fori_loop(0, LAYERS + 1, step, 0)
    for l in range(LAYERS):
        for c in tail_copies(l):
            c.wait()
        tail_copy(l).start()
    for l in range(LAYERS):
        c_par(l).wait_send()

        @pl.when(core == 1)
        def _():
            c_tail(l).wait_send()
            f_tail(l).wait_send()

        def sent(n):
            for half in range(2):
                c_half(l, half, n).wait_send()
                f_half(l, half, n).wait_send()
        by_core(sent)
        tail_copy(l).wait()

    for p in range(NB):
        out_prompt(LAYERS - 1, p).wait()
    for n in range(3):
        r_copy(n).wait()


def copy_kernel(r_ref, ssm_ref, tail_ref, r_out, ssm_out, conv_out, tbuf, cbuf, sems):
    whole = [pltpu.make_async_copy(r_ref, r_out, sems.at[0]), pltpu.make_async_copy(ssm_ref, ssm_out, sems.at[1])]
    load = pltpu.make_async_copy(tail_ref, tbuf, sems.at[2])
    load.start()
    for c in whole:
        c.start()
    load.wait()
    for p in range(NB):
        for l in range(LAYERS):
            rows = tbuf[l, p].astype(F32)
            for k in range(3):
                cbuf[p, k, l:l + 1, :] = rows[13 + k:14 + k, :].astype(BF16)
    store = pltpu.make_async_copy(cbuf, conv_out, sems.at[3])
    store.start()
    for c in whole + [store]:
        c.wait()


def solution(mesh):
    hbm = pl.BlockSpec(memory_space=pl.ANY)

    def forward(resid, pre_norm, w_in, conv_w, conv_b, dt_bias, a_log, d_skip, gate_norm, w_out):
        r, ssm, tails = pl.pallas_call(
            kernel,
            out_shape=(
                pltpu.VMEM((NB, SEG, D_MODEL), F32),
                pltpu.VMEM((NB, LAYERS, 12, 64, 128), F32),
                pltpu.VMEM((LAYERS, NB, 16, CONV_DIM), BF16),
            ),
            in_specs=[hbm] * 10,
            out_specs=(hbm, hbm, hbm),
            scratch_shapes=[
                pltpu.VMEM((NB, SEG, D_MODEL), F32),
                pltpu.VMEM((LAYERS, D_MODEL), F32),
                pltpu.VMEM((LAYERS, 4, CONV_DIM), F32),
                pltpu.VMEM((LAYERS, CONV_DIM), F32),
                pltpu.VMEM((LAYERS, HEADS), F32),
                pltpu.VMEM((LAYERS, HEADS), F32),
                pltpu.SMEM((LAYERS, HEADS), F32),
                pltpu.VMEM((LAYERS, 1, D_INNER), F32),
                pltpu.VMEM((LAYERS * NB, ROWS, D_MODEL), BF16),
                pltpu.VMEM((NB, SEG, D_INNER), F32),
                pltpu.VMEM((D_INNER, D_MODEL), BF16),
                pltpu.VMEM((LOC, D_MODEL), BF16),
                pltpu.VMEM((384, D_MODEL), BF16),
                pltpu.VMEM((D_INNER, D_MODEL), BF16),
                pltpu.VMEM((4, NB, EXT, 128), F32),
                pltpu.VMEM((4, NB, EXT, 128), F32),
                pltpu.VMEM((BLK, LOC), BF16),
                pltpu.VMEM((2, BLK, LOC), BF16),
                pltpu.VMEM((NB, BLK, ACT), BF16),
                pltpu.VMEM((NB, BLK, ACT), BF16),
                pltpu.VMEM((NB, BLK, LOC), F32),
                pltpu.VMEM((NB, BLK, LOC), BF16),
                pltpu.VMEM((LAYERS * NB, SEG, LOC), BF16),
                pltpu.VMEM((NB, SEG, D_INNER), BF16),
                pltpu.VMEM((NB, 12, 64, 128), F32),
                pltpu.VMEM((LAYERS, NB, 16, CONV_DIM), BF16),
                pltpu.VMEM((NB, 16, ACT), BF16),
                pltpu.VMEM((NB, 16, ACT), BF16),
                pltpu.VMEM((NB, BLK, BLK), F32),
                pltpu.VMEM((NB, BLK, BLK), F32),
                pltpu.VMEM((NB, BLK, BLK), F32),
                pltpu.VMEM((NB, BLK, BLK), F32),
                pltpu.VMEM((NB, 40, BLK), F32),
                pltpu.VMEM((NB, 40, BLK), F32),
                pltpu.VMEM((8, ACT), F32),
                pltpu.VMEM((8, 128), F32),
                pltpu.SemaphoreType.DMA((12,)),
                pltpu.SemaphoreType.DMA((LAYERS, 7)),
                pltpu.SemaphoreType.DMA((LAYERS, 7)),
                pltpu.SemaphoreType.DMA((LAYERS, NB)),
                pltpu.SemaphoreType.DMA((LAYERS, NB)),
                pltpu.SemaphoreType.DMA((LAYERS, 2)),
                pltpu.SemaphoreType.DMA((LAYERS, 2)),
                pltpu.SemaphoreType.DMA((NB,)),
                pltpu.SemaphoreType.DMA((8,)),
                pltpu.SemaphoreType.DMA((3,)),
                pltpu.SemaphoreType.DMA((LAYERS,)),
            ],
            compiler_params=pltpu.CompilerParams(collective_id=0, has_side_effects=True, vmem_limit_bytes=VMEM_LIMIT),
        )(resid, pre_norm, jnp.swapaxes(w_in, 1, 2), jnp.swapaxes(conv_w, 1, 2), conv_b, dt_bias, a_log, d_skip, gate_norm, w_out)
        r, ssm, conv = pl.pallas_call(
            copy_kernel,
            out_shape=(
                jax.ShapeDtypeStruct(r.shape, F32),
                jax.ShapeDtypeStruct(ssm.shape, F32),
                jax.ShapeDtypeStruct((NB, 3, LAYERS, CONV_DIM), BF16),
            ),
            in_specs=[hbm] * 3,
            out_specs=(hbm, hbm, hbm),
            scratch_shapes=[
                pltpu.VMEM((LAYERS, NB, 16, CONV_DIM), BF16),
                pltpu.VMEM((NB, 3, LAYERS, CONV_DIM), BF16),
                pltpu.SemaphoreType.DMA((4,)),
            ],
            compiler_params=pltpu.CompilerParams(vmem_limit_bytes=4 * 1024 * 1024),
        )(r, ssm, tails)
        return r, ssm, jnp.transpose(conv, (0, 2, 3, 1))

    return jax.shard_map(forward, mesh=mesh, in_specs=(P('dp', 'sp', None), P(), P(), P(), P(), P(), P(), P(), P(), P()), out_specs=(P('dp', 'sp', None), P('dp', None, 'sp', None, None), P('dp', None, None, None)), check_vma=False)
```

```python
import functools

import jax
import jax.numpy as jnp
from jax import lax
from jax.experimental import pallas as pl
from jax.experimental.pallas import tpu as pltpu
from jax.sharding import PartitionSpec as P

F32 = jnp.float32
BF16 = jnp.bfloat16
EPSILON = 1e-5
LAYERS = 2
NB = 4
SEG = 64
BLK = 128
HALO = 16
EXT = BLK + HALO
ROWS = HALO + 2 * BLK
D_MODEL = 1536
D_INNER = 3072
CONV_DIM = 3328
HEADS = 48
HALF = 768
LOC = 1536
ACT = LOC + 256
PAIRS = 12
VMEM_LIMIT = 58400000
NT = (((1,), (1,)), ((), ()))


def dot(a, b):
    return jnp.dot(a, b, preferred_element_type=F32)


def dot_nt(a, b):
    return lax.dot_general(a, b, NT, preferred_element_type=F32)


def round_bf16(v):
    return v.astype(BF16).astype(F32)


def silu(v):
    half = 0.5 * v
    return half * jnp.tanh(half) + half


def head_row(i):
    return i if i < 12 else i + 12


def kernel(resid_hbm, pre_hbm, w_in_ref, cw_hbm, cb_hbm, dtb_hbm, alog_hbm, dskip_hbm, gw_hbm, w_out_ref,
           r_out, ssm_out, tail_out,
           pre_ref, cw_ref, cb_ref, dtb_ref, alog_ref, dskip_ref, gw_ref, hbuf, sz, wz, wx, wbc, wout, rawa, rawb, spread, scaled, act_o, act_r, yloc, ybuf, yrecv, gn, tails, tail_o, tail_r,
           cum_o, cum_r, dt_o, dt_r, cumt_o, dtt_o, cwl, prm,
           wsem, hsend, hrecv, ysend, yrecv_sem, tsend, trecv, psem, tout):
    me = lax.axis_index('sp')
    chip = me // 2
    core = me % 2
    partner = chip * 2 + (1 - core)
    other = (1 - chip) * 2 + core
    chip_f = chip.astype(F32)
    core_f = core.astype(F32)

    def weight_copies(l):
        xc = [pltpu.make_async_copy(w_in_ref.at[l, pl.ds(pl.multiple_of(D_INNER + LOC * b + HALF * core, 16), HALF), :], wx.at[pl.ds(HALF * b, HALF), :], wsem.at[6 + b]) for b in range(2)]
        bc = [pltpu.make_async_copy(w_in_ref.at[l, pl.ds(src, n), :], wbc.at[pl.ds(dst, n), :], wsem.at[sem]) for src, n, dst, sem in ((2 * D_INNER, 128, 0, 8), (2 * D_INNER + 256, HEADS, 128, 9), (2 * D_INNER + 128, 128, 256, 10))]
        oc = pltpu.make_async_copy(w_out_ref.at[l], wout, wsem.at[11])
        return xc, bc, oc

    def z_copy(l, n):
        rows = pl.ds(pl.multiple_of(512 * n, 16), 512)
        return pltpu.make_async_copy(w_in_ref.at[l, rows, :], wz.at[rows, :], wsem.at[n])

    params = [pltpu.make_async_copy(src, dst, psem.at[i]) for i, (src, dst) in enumerate(((resid_hbm, r_out), (pre_hbm, pre_ref), (cw_hbm, cw_ref), (cb_hbm, cb_ref), (dtb_hbm, dtb_ref), (alog_hbm, alog_ref), (dskip_hbm, dskip_ref), (gw_hbm, gw_ref)))]
    xc0, bc0, oc0 = weight_copies(0)
    params[0].start()
    params[1].start()
    z_copy(0, 0).start()
    for c in params[2:]:
        c.start()
    for n in range(1, 6):
        z_copy(0, n).start()

    barrier = pltpu.get_barrier_semaphore()
    for step in range(1, 4):
        pl.semaphore_signal(barrier, inc=1, device_id={'sp': (me + step) % 4}, device_id_type=pl.DeviceIdType.MESH)

    hbuf[:, 0:HALO, :] = jnp.zeros((LAYERS * NB, HALO, D_MODEL), BF16)
    wbc[176:256, :] = jnp.zeros((80, D_MODEL), BF16)
    prm[...] = jnp.zeros((8, 128), F32)
    for c in bc0 + xc0:
        c.start()
    rows_i = lax.broadcasted_iota(jnp.int32, (BLK, 64), 0)
    for i in range(24):
        h = head_row(i)
        hit = (rows_i == h) | (rows_i == h + 40) | (rows_i == h + 80)
        spread[:, 64 * i:64 * (i + 1)] = jnp.where(hit, 1.0, 0.0).astype(BF16)

    with jax.named_scope('params'):
        for c in params[:2]:
            c.wait()
    with jax.named_scope('barrier'):
        pl.semaphore_wait(barrier, 3)

    own_row = pl.multiple_of(HALO + BLK * chip + SEG * core, 16)
    oth_row = pl.multiple_of(HALO + BLK * (1 - chip) + SEG * core, 16)
    own_blk = pl.multiple_of(BLK * chip, 16)
    oth_blk = pl.multiple_of(BLK * (1 - chip), 16)

    iota_r = lax.broadcasted_iota(jnp.int32, (BLK, BLK), 0)
    iota_c = lax.broadcasted_iota(jnp.int32, (BLK, BLK), 1)

    def remote(src, dst, ssem, rsem, dev):
        return pltpu.make_async_remote_copy(src_ref=src, dst_ref=dst, send_sem=ssem, recv_sem=rsem, device_id={'sp': dev}, device_id_type=pl.DeviceIdType.MESH)

    tri = (iota_r >= iota_c).astype(F32)
    low = iota_c < 64

    def hslice(l, p0, n, row, size):
        return hbuf.at[pl.ds(NB * l + p0, n), pl.ds(row, size), :]

    def same(l, idx, p0, n, row, size, dev):
        ref = hslice(l, p0, n, row, size)
        return remote(ref, ref, hsend.at[l, idx], hrecv.at[l, idx], dev)

    def c_par(l):
        return same(l, 0, 0, NB, own_row, SEG, partner)

    def c_tail(l):
        return same(l, 1, 0, NB, own_row + 48, 16, other)

    def c_half(l, half, size):
        return same(l, 2 + half, 2 * half, 2, own_row, size, other)

    def f_tail(l):
        return same(l, 4, 0, NB, oth_row + 48, 16, partner)

    def f_half(l, half, size):
        return same(l, 5 + half, 2 * half, 2, oth_row, size, partner)

    def by_core(fn):
        @pl.when(core == 0)
        def _():
            fn(64)

        @pl.when(core == 1)
        def _():
            fn(48)

    def wait_half(l, half):
        by_core(lambda n: f_half(l, half, 112 - n).wait_recv())

    def y_copy(l, p):
        src = ybuf.at[p, pl.ds(pl.multiple_of(SEG * (1 - core), 16), SEG), :]
        return remote(src, yrecv.at[NB * l + p], ysend.at[l, p], yrecv_sem.at[l, p], partner)

    def tail_copy(l):
        return pltpu.make_async_copy(tails.at[l], tail_out.at[l], tout.at[l])

    def tail_copies(l):
        res = []
        for b in range(2):
            ref = tails.at[l, :, :, pl.ds(pl.multiple_of(LOC * b + HALF * core, 128), HALF)]
            res.append(remote(ref, ref, tsend.at[l, b], trecv.at[l, b], partner))
        return res

    def conv_chunk(act, src, first, groups, i, p, dst):
        for g in range(groups):
            cols = slice(dst + 128 * g, dst + 128 * (g + 1))
            acc = cwl[0:1, cols] * src[first + g, i, 13:141, :]
            for k in range(1, 4):
                acc = acc + cwl[k:k + 1, cols] * src[first + g, i, 13 + k:141 + k, :]
            act[p, :, cols] = silu(acc + cwl[4:5, cols]).astype(BF16)

    def block(l, p0, np_, row, act, tail, cum, dts, trans, with_c, widths):
        def project(w, rows, dst):
            lhs = hbuf[pl.ds(NB * l + p0, np_), pl.ds(row, EXT), :].reshape(np_ * EXT, D_MODEL)
            res = round_bf16(dot_nt(lhs, w[rows, :]))
            for g in range((rows.stop - rows.start) // 128):
                dst[g, 0:np_] = res[:, 128 * g:128 * (g + 1)].reshape(np_, EXT, 128)

        def finish_bc(src):
            for i in range(np_):
                p = p0 + i
                for g, dst in ((0, LOC), (2, LOC + 128))[:2 if with_c else 1]:
                    if tail is not None:
                        tail[p, :, dst:dst + 128] = src[g, i, BLK:EXT, :].astype(BF16)
                    conv_chunk(act, src, g, 1, i, p, dst)
                v = src[1, i, HALO:EXT, :] + prm[0:1, :]
                dt = round_bf16(jnp.maximum(v, 0.0) + jnp.log1p(jnp.exp(-jnp.abs(v))))
                logs = dt * prm[1:2, :]
                dt = dt * (1.0 - core_f) + pltpu.roll(dt, 116, 1) * core_f
                logs = logs * (1.0 - core_f) + pltpu.roll(logs, 116, 1) * core_f
                cums = jnp.dot(tri, logs, precision=lax.Precision.HIGHEST, preferred_element_type=F32)
                cum[p] = cums
                dts[p] = dt
                if trans is not None:
                    trans[0][p] = cums.T[0:40]
                    trans[1][p] = dt.T[0:40]

        def finish_x(src, col, n):
            for i in range(np_):
                if tail is not None:
                    for g in range(n // 128):
                        tail[p0 + i, :, col + 128 * g:col + 128 * (g + 1)] = src[g, i, BLK:EXT, :].astype(BF16)
                conv_chunk(act, src, 0, n // 128, i, p0 + i, col)

        project(wbc, slice(0, 384 if with_c else 256), rawa)
        pending, nxt = (lambda: finish_bc(rawa)), rawb
        col = 0
        for n in widths:
            project(wx, slice(col, col + n), nxt)
            pending()
            pending = functools.partial(finish_x, nxt, col, n)
            col += n
            nxt = rawa if nxt is rawb else rawb
        pending()

    def last_rows(l, tail):
        lhs = hbuf[pl.ds(NB * l, NB), ROWS - 16:ROWS, :].reshape(NB * 16, D_MODEL)
        for col in range(0, LOC, 512):
            tail[:, :, col:col + 512] = dot_nt(lhs, wx[col:col + 512, :]).astype(BF16).reshape(NB, 16, 512)
        res = dot_nt(lhs, wbc[...]).astype(BF16).reshape(NB, 16, 384)
        tail[:, :, LOC:LOC + 128] = res[:, :, 0:128]
        tail[:, :, LOC + 128:ACT] = res[:, :, 256:384]

    zero = jnp.zeros((), BF16)

    def split_pair(xp):
        return [jnp.where(low, xp, zero), jnp.where(low, zero, xp)]

    lane = lax.broadcasted_iota(jnp.int32, (BLK, BLK), 1)

    def three_terms(v):
        v = jnp.where(lane < 40, v, 0.0)
        hi = round_bf16(v)
        mid = round_bf16(v - hi)
        return (hi + pltpu.roll(mid, 40, 1) + pltpu.roll((v - hi) - mid, 80, 1)).astype(BF16)

    def weighted(act, p, cols, terms):
        return (act[p, :, cols].astype(F32) * dot(terms, spread[:, cols])).astype(BF16)

    def intra_body(l, p):
        cb = act_o[p, :, LOC + 128:ACT]
        scores = dot_nt(cb, act_o[p, :, LOC:LOC + 128]) * tri
        for j in range(PAIRS):
            mats = []
            for i in (2 * j, 2 * j + 1):
                h = head_row(i)
                col = jnp.broadcast_to(cum_o[p, :, h:h + 1], (BLK, BLK))
                mats.append((jnp.exp(jnp.minimum(col - cumt_o[p, h:h + 1, :], 0.0)) * (scores * dtt_o[p, h:h + 1, :])).astype(BF16))
            xp = act_o[p, :, 128 * j:128 * (j + 1)]
            blk = (0 if j < 6 else 24) + 12 * core + (2 * j) % 12
            dv = jnp.where(low[0:1], dskip_ref[l, blk], dskip_ref[l, blk + 1])
            y = dot(jnp.concatenate(mats, axis=1), jnp.concatenate(split_pair(xp), axis=0)) + dv * xp.astype(F32)
            yloc[p, :, 128 * j:128 * (j + 1)] = y
            ybuf[p, :, 128 * j:128 * (j + 1)] = y.astype(BF16)

    def inter_half(l, half):
        prompts = [(0, 2 * half, rawa), (1, 2 * half + 1, rawb)]
        bts, ends = [], []
        for i, p, _ in prompts:
            cum = cum_r[p]
            bts.append(act_r[p, :, LOC:LOC + 128].astype(F32).T.astype(BF16))
            ends.append(three_terms(dt_r[p] * jnp.exp(cum[127:128, :] - cum)))
        for i, p, _ in prompts:
            for j in range(6):
                cols = slice(256 * j, 256 * (j + 1))
                scaled[i, :, cols] = weighted(act_r, p, cols, ends[i])
        for i, p, states in prompts:
            for j in range(6):
                state = dot(bts[i], scaled[i, :, 256 * j:256 * (j + 1)])
                for k in range(2):
                    states[(2 * j + k) // 4, (2 * j + k) % 4, 0:BLK, :] = state[:, 128 * k:128 * (k + 1)]
        for i, p, states in prompts:
            cf = act_o[p, :, LOC + 128:ACT]
            start = three_terms(jnp.exp(cum_o[p]))
            for j in range(6):
                cols = slice(256 * j, 256 * (j + 1))
                state = jnp.concatenate([states[(2 * j + k) // 4, (2 * j + k) % 4, 0:BLK, :].astype(BF16) for k in range(2)], axis=1)
                y = yloc[p, :, cols] + dot(cf, state) * dot(start, spread[:, cols])
                ybuf[p, :, cols] = y.astype(BF16)
            y_copy(l, p).start()

    def final_inputs(p):
        co, cr = cum_o[p], cum_r[p]
        eo, er = co[127:128, :], cr[127:128, :]
        fo = three_terms(dt_o[p] * jnp.exp(eo - co + er * (1.0 - chip_f)))
        fr = three_terms(dt_r[p] * jnp.exp(er - cr + eo * chip_f))
        for j in range(3):
            cols = pl.ds(pl.multiple_of(HALF * chip + 256 * j, 256), 256)
            ybuf[p, :, 256 * j:256 * (j + 1)] = weighted(act_o, p, cols, fo)
            ybuf[p, :, HALF + 256 * j:HALF + 256 * (j + 1)] = weighted(act_r, p, cols, fr)

    def final_states(l, p):
        bts = jnp.concatenate([act[p, :, LOC:LOC + 128].astype(F32).T.astype(BF16) for act in (act_o, act_r)], axis=1)
        for j in range(3):
            state = dot(bts, jnp.concatenate([ybuf[p, :, 256 * j:256 * (j + 1)], ybuf[p, :, HALF + 256 * j:HALF + 256 * (j + 1)]], axis=0))
            ssm_out[p, l, 4 * j:4 * j + 4] = state.T.reshape(4, 64, 128)

    def pass_tail(l):
        c_tail(l).wait_recv()
        f_tail(l).start()

    def pass_half(l, half):
        def go(n):
            c_half(l, half, n).wait_recv()
            f_half(l, half, n).start()
        by_core(go)

    def bulk(l):
        c_half(l, 0, 64).start()
        c_half(l, 1, 64).start()

    def after_other(l, tail):
        for b in range(2):
            tails[l, :, :, pl.ds(pl.multiple_of(LOC * b + HALF * core, 128), HALF)] = tail[:, :, HALF * b:HALF * (b + 1)]
        tails[l, :, :, D_INNER:CONV_DIM] = tail[:, :, LOC:ACT]
        for c in tail_copies(l):
            c.start()

    def next_weights(l):
        @pl.when(l == 0)
        def _():
            xnx, bnx, _ = weight_copies(1)
            for c in xnx + bnx:
                c.start()

    def begin(l):
        def norm_body(p, c):
            v = r_out[p]
            ms = jnp.mean(v * v, axis=-1, keepdims=True)
            hbuf[NB * l + p, pl.ds(own_row, SEG), :] = (v * lax.rsqrt(ms + EPSILON) * pre_ref[pl.ds(l, 1), :]).astype(BF16)
            return c
        with jax.named_scope('norm'):
            lax.fori_loop(0, NB, norm_body, 0)

        c_par(l).start()

        @pl.when(core == 1)
        def _():
            c_tail(l).start()
            c_half(l, 0, 48).start()
            c_half(l, 1, 48).start()

        @pl.when(jnp.logical_and(core == 0, l > 0))
        def _():
            bulk(l)

        @pl.when(jnp.logical_and(jnp.logical_and(core == 1, chip == 1), l > 0))
        def _():
            pass_tail(l)

    def main(l):
        xc, bc, oc = weight_copies(l)

        def z_chunk(n):
            lhs = hbuf[pl.ds(NB * l, NB), pl.ds(own_row, SEG), :].reshape(NB * SEG, D_MODEL)
            cols = slice(512 * n, 512 * (n + 1)) if isinstance(n, int) else pl.ds(pl.multiple_of(512 * n, 512), 512)
            z = round_bf16(dot_nt(lhs, wz[cols, :]))
            sz[:, :, cols] = silu(z).reshape(NB, SEG, 512)

        def z_group(lo):
            for n in range(lo, lo + 3):
                z_copy(l, n).wait()
            for n in range(lo, lo + 3):
                z_chunk(n)

        with jax.named_scope('zproj'):
            z_group(0)

            @pl.when(jnp.logical_and(core == 0, l == 0))
            def _():
                bulk(l)

            @pl.when(l == 0)
            def _():
                z_group(3)
        oc.start()

        @pl.when(l == 0)
        def _():
            for n in range(6):
                z_copy(1, n).start()

        @pl.when(l == 0)
        def _():
            for c in params[2:]:
                c.wait()

        for b in range(2):
            src = pl.multiple_of(LOC * b + HALF * core, 128)
            cwl[0:4, HALF * b:HALF * (b + 1)] = cw_ref[l, :, pl.ds(src, HALF)]
            cwl[4:5, HALF * b:HALF * (b + 1)] = cb_ref[pl.ds(l, 1), pl.ds(src, HALF)]
        cwl[0:4, LOC:ACT] = cw_ref[l, :, D_INNER:CONV_DIM]
        cwl[4:5, LOC:ACT] = cb_ref[pl.ds(l, 1), D_INNER:CONV_DIM]
        prm[0:1, 0:HEADS] = dtb_ref[pl.ds(l, 1), :]
        prm[1:2, 0:HEADS] = -jnp.exp(alog_ref[pl.ds(l, 1), :])

        with jax.named_scope('wait_h'):
            c_par(l).wait_recv()
            for c in bc + xc:
                c.wait()

            @pl.when(jnp.logical_and(jnp.logical_and(core == 1, chip == 1), l == 0))
            def _():
                pass_tail(l)

            @pl.when(jnp.logical_and(chip == 1, core == 0))
            def _():
                f_tail(l).wait_recv()
        with jax.named_scope('own_block'):
            block(l, 0, NB, own_blk, act_o, tail_o, cum_o, dt_o, (cumt_o, dtt_o), True, (512, 512, 256, 256))

        def intra_end(p):
            @pl.when(chip == 0)
            def _():
                y_copy(l, p).start()

            @pl.when(jnp.logical_and(chip == 1, p == 1))
            def _():
                pass_half(l, 0)

        def intra_plain(p, c):
            intra_body(l, p)
            intra_end(p)
            return c

        def intra_z(p, c):
            z_chunk(3 + p)
            intra_body(l, p)
            intra_end(p)
            return c

        with jax.named_scope('intra'):
            @pl.when(l > 0)
            def _():
                for n in range(3, 6):
                    z_copy(l, n).wait()
            split = jnp.where(l == 0, 0, 3)
            lax.fori_loop(0, split, intra_z, 0)
            lax.fori_loop(split, NB, intra_plain, 0)

        @pl.when(chip == 1)
        def _():
            with jax.named_scope('wait_r0'):
                wait_half(l, 0)

            def half_body(half, c):
                with jax.named_scope('oth_block'):
                    block(l, 2 * half, 2, oth_blk, act_r, None, cum_r, dt_r, None, False, (512, 512, 512))

                @pl.when(half == 0)
                def _():
                    with jax.named_scope('wait_c1'):
                        pass_half(l, 1)
                with jax.named_scope('inter'):
                    inter_half(l, half)

                @pl.when(half == 0)
                def _():
                    with jax.named_scope('wait_f1'):
                        wait_half(l, 1)
                return c
            lax.fori_loop(0, 2, half_body, 0)
            after_other(l, tail_o)
            next_weights(l)

        def gate_body(p, c):
            y_copy(l, p).wait()
            total = jnp.zeros((SEG, 1), F32)
            for b in range(2):
                for own in range(2):
                    cols = pl.ds(pl.multiple_of(LOC * b + HALF * (core if own else 1 - core), 128), HALF)
                    if own:
                        y = ybuf[p, pl.ds(pl.multiple_of(SEG * core, 16), SEG), HALF * b:HALF * (b + 1)]
                    else:
                        y = yrecv[NB * l + p, :, HALF * b:HALF * (b + 1)]
                    g = y.astype(F32) * sz[p, :, cols]
                    sz[p, :, cols] = g
                    total = total + jnp.sum(g * g, axis=-1, keepdims=True)
            scale = lax.rsqrt(total * (1.0 / D_INNER) + EPSILON)
            for b in range(4):
                cols = slice(HALF * b, HALF * (b + 1))
                gn[p, :, cols] = (sz[p, :, cols] * scale * gw_ref[l, :, cols]).astype(BF16)
            return c
        with jax.named_scope('gate'):
            lax.fori_loop(0, NB, gate_body, 0)
            oc.wait()

        def out_chunk(n):
            cols = slice(512 * n, 512 * (n + 1))
            o = dot(gn[...].reshape(NB * SEG, D_INNER), wout[:, cols])
            r_out[:, :, cols] = r_out[:, :, cols] + o.reshape(NB, SEG, 512)

        with jax.named_scope('outproj'):
            @pl.when(chip == 0)
            def _():
                for n in range(3):
                    out_chunk(n)

            @pl.when(chip == 1)
            def _():
                final_inputs(0)
                final_inputs(1)
                out_chunk(0)
                final_states(l, 0)
                final_states(l, 1)
                final_inputs(2)
                final_inputs(3)
                out_chunk(1)
                final_states(l, 2)
                final_states(l, 3)
                out_chunk(2)

        @pl.when(chip == 0)
        def _():
            with jax.named_scope('pass_d'):
                @pl.when(core == 1)
                def _():
                    pass_tail(l)
                pass_half(l, 0)

    def deferred(l):
        with jax.named_scope('wait_d'):
            @pl.when(core == 0)
            def _():
                f_tail(l).wait_recv()

        with jax.named_scope('last_rows'):
            last_rows(l, tail_r)
            after_other(l, tail_r)

        def half_body(half, c):
            with jax.named_scope('wait_dh'):
                wait_half(l, half)
            with jax.named_scope('oth_block'):
                block(l, 2 * half, 2, oth_blk, act_r, None, cum_r, dt_r, None, False, (512, 256))

            @pl.when(jnp.logical_and(half == 0, l == 0))
            def _():
                pass_half(l, 1)

            @pl.when(half == 1)
            def _():
                next_weights(l)

            with jax.named_scope('final'):
                for i in range(2):
                    final_inputs(2 * half + i)
                for i in range(2):
                    final_states(l, 2 * half + i)

            @pl.when(jnp.logical_and(half == 0, l > 0))
            def _():
                with jax.named_scope('wait_c1'):
                    pass_half(l, 1)
            return c
        lax.fori_loop(0, 2, half_body, 0)

    def step(l, carry):
        @pl.when(l < LAYERS)
        def _():
            begin(l)

        @pl.when(jnp.logical_and(chip == 0, l > 0))
        def _():
            deferred(l - 1)

        @pl.when(l < LAYERS)
        def _():
            main(l)
        return carry

    lax.fori_loop(0, LAYERS + 1, step, 0)
    for l in range(LAYERS):
        for c in tail_copies(l):
            c.wait()
        tail_copy(l).start()
    for l in range(LAYERS):
        c_par(l).wait_send()

        @pl.when(core == 1)
        def _():
            c_tail(l).wait_send()
            f_tail(l).wait_send()

        def sent(n):
            for half in range(2):
                c_half(l, half, n).wait_send()
                f_half(l, half, n).wait_send()
        by_core(sent)
        tail_copy(l).wait()


def copy_kernel(r_ref, ssm_ref, tail_ref, r_out, ssm_out, conv_out, tbuf, cbuf, sems):
    whole = [pltpu.make_async_copy(r_ref, r_out, sems.at[0]), pltpu.make_async_copy(ssm_ref, ssm_out, sems.at[1])]
    load = pltpu.make_async_copy(tail_ref, tbuf, sems.at[2])
    load.start()
    for c in whole:
        c.start()
    load.wait()
    for p in range(NB):
        for l in range(LAYERS):
            rows = tbuf[l, p].astype(F32)
            for k in range(3):
                cbuf[p, k, l:l + 1, :] = rows[13 + k:14 + k, :].astype(BF16)
    store = pltpu.make_async_copy(cbuf, conv_out, sems.at[3])
    store.start()
    for c in whole + [store]:
        c.wait()


def solution(mesh):
    hbm = pl.BlockSpec(memory_space=pl.ANY)
    vmem = pl.BlockSpec(memory_space=pltpu.VMEM)

    def forward(resid, pre_norm, w_in, conv_w, conv_b, dt_bias, a_log, d_skip, gate_norm, w_out):
        r, ssm, tails = pl.pallas_call(
            kernel,
            out_shape=(
                pltpu.VMEM((NB, SEG, D_MODEL), F32),
                pltpu.VMEM((NB, LAYERS, 12, 64, 128), F32),
                pltpu.VMEM((LAYERS, NB, 16, CONV_DIM), BF16),
            ),
            in_specs=[hbm] * 10,
            out_specs=(vmem, vmem, hbm),
            scratch_shapes=[
                pltpu.VMEM((LAYERS, D_MODEL), F32),
                pltpu.VMEM((LAYERS, 4, CONV_DIM), F32),
                pltpu.VMEM((LAYERS, CONV_DIM), F32),
                pltpu.VMEM((LAYERS, HEADS), F32),
                pltpu.VMEM((LAYERS, HEADS), F32),
                pltpu.SMEM((LAYERS, HEADS), F32),
                pltpu.VMEM((LAYERS, 1, D_INNER), F32),
                pltpu.VMEM((LAYERS * NB, ROWS, D_MODEL), BF16),
                pltpu.VMEM((NB, SEG, D_INNER), F32),
                pltpu.VMEM((D_INNER, D_MODEL), BF16),
                pltpu.VMEM((LOC, D_MODEL), BF16),
                pltpu.VMEM((384, D_MODEL), BF16),
                pltpu.VMEM((D_INNER, D_MODEL), BF16),
                pltpu.VMEM((4, NB, EXT, 128), F32),
                pltpu.VMEM((4, NB, EXT, 128), F32),
                pltpu.VMEM((BLK, LOC), BF16),
                pltpu.VMEM((2, BLK, LOC), BF16),
                pltpu.VMEM((NB, BLK, ACT), BF16),
                pltpu.VMEM((NB, BLK, ACT), BF16),
                pltpu.VMEM((NB, BLK, LOC), F32),
                pltpu.VMEM((NB, BLK, LOC), BF16),
                pltpu.VMEM((LAYERS * NB, SEG, LOC), BF16),
                pltpu.VMEM((NB, SEG, D_INNER), BF16),
                pltpu.VMEM((LAYERS, NB, 16, CONV_DIM), BF16),
                pltpu.VMEM((NB, 16, ACT), BF16),
                pltpu.VMEM((NB, 16, ACT), BF16),
                pltpu.VMEM((NB, BLK, BLK), F32),
                pltpu.VMEM((NB, BLK, BLK), F32),
                pltpu.VMEM((NB, BLK, BLK), F32),
                pltpu.VMEM((NB, BLK, BLK), F32),
                pltpu.VMEM((NB, 40, BLK), F32),
                pltpu.VMEM((NB, 40, BLK), F32),
                pltpu.VMEM((8, ACT), F32),
                pltpu.VMEM((8, 128), F32),
                pltpu.SemaphoreType.DMA((12,)),
                pltpu.SemaphoreType.DMA((LAYERS, 7)),
                pltpu.SemaphoreType.DMA((LAYERS, 7)),
                pltpu.SemaphoreType.DMA((LAYERS, NB)),
                pltpu.SemaphoreType.DMA((LAYERS, NB)),
                pltpu.SemaphoreType.DMA((LAYERS, 2)),
                pltpu.SemaphoreType.DMA((LAYERS, 2)),
                pltpu.SemaphoreType.DMA((8,)),
                pltpu.SemaphoreType.DMA((LAYERS,)),
            ],
            compiler_params=pltpu.CompilerParams(collective_id=0, has_side_effects=True, vmem_limit_bytes=VMEM_LIMIT),
        )(resid, pre_norm, jnp.swapaxes(w_in, 1, 2), jnp.swapaxes(conv_w, 1, 2), conv_b, dt_bias, a_log, d_skip, gate_norm, w_out)
        r, ssm, conv = pl.pallas_call(
            copy_kernel,
            out_shape=(
                jax.ShapeDtypeStruct(r.shape, F32),
                jax.ShapeDtypeStruct(ssm.shape, F32),
                jax.ShapeDtypeStruct((NB, 3, LAYERS, CONV_DIM), BF16),
            ),
            in_specs=[hbm] * 3,
            out_specs=(hbm, hbm, hbm),
            scratch_shapes=[
                pltpu.VMEM((LAYERS, NB, 16, CONV_DIM), BF16),
                pltpu.VMEM((NB, 3, LAYERS, CONV_DIM), BF16),
                pltpu.SemaphoreType.DMA((4,)),
            ],
            compiler_params=pltpu.CompilerParams(vmem_limit_bytes=4 * 1024 * 1024),
        )(r, ssm, tails)
        return r, ssm, jnp.transpose(conv, (0, 2, 3, 1))

    return jax.shard_map(forward, mesh=mesh, in_specs=(P('dp', 'sp', None), P(), P(), P(), P(), P(), P(), P(), P(), P()), out_specs=(P('dp', 'sp', None), P('dp', None, 'sp', None, None), P('dp', None, None, None)), check_vma=False)
```

```python
import functools

import jax
import jax.numpy as jnp
from jax import lax
from jax.experimental import pallas as pl
from jax.experimental.pallas import tpu as pltpu
from jax.sharding import PartitionSpec as P

F32 = jnp.float32
BF16 = jnp.bfloat16
EPSILON = 1e-5
LAYERS = 2
NB = 4
SEG = 64
BLK = 128
HALO = 16
EXT = BLK + HALO
ROWS = HALO + 2 * BLK
D_MODEL = 1536
D_INNER = 3072
CONV_DIM = 3328
HEADS = 48
HALF = 768
LOC = 1536
ACT = LOC + 256
PAIRS = 12
VMEM_LIMIT = 58400000
NT = (((1,), (1,)), ((), ()))


def dot(a, b):
    return jnp.dot(a, b, preferred_element_type=F32)


def dot_nt(a, b):
    return lax.dot_general(a, b, NT, preferred_element_type=F32)


def round_bf16(v):
    return v.astype(BF16).astype(F32)


def silu(v):
    half = 0.5 * v
    return half * jnp.tanh(half) + half


def head_row(i):
    return i if i < 12 else i + 12


def kernel(resid_hbm, pre_hbm, w_in_ref, cw_hbm, cb_hbm, dtb_hbm, alog_hbm, dskip_hbm, gw_hbm, w_out_ref,
           r_out, ssm_out, tail_out,
           pre_ref, cw_ref, cb_ref, dtb_ref, alog_ref, dskip_ref, gw_ref, hbuf, sz, wz, wx, wbc, wout, rawa, rawb, spread, scaled, act_o, act_r, yloc, ybuf, yrecv, gn, tails, tail_o, tail_r,
           cum_o, cum_r, dt_o, dt_r, cumt_o, dtt_o, cwl, prm,
           wsem, hsend, hrecv, ysend, yrecv_sem, tsend, trecv, psem, tout):
    me = lax.axis_index('sp')
    chip = me // 2
    core = me % 2
    partner = chip * 2 + (1 - core)
    other = (1 - chip) * 2 + core
    chip_f = chip.astype(F32)
    core_f = core.astype(F32)

    def weight_copies(l):
        xc = [pltpu.make_async_copy(w_in_ref.at[l, pl.ds(pl.multiple_of(D_INNER + LOC * b + HALF * core, 16), HALF), :], wx.at[pl.ds(HALF * b, HALF), :], wsem.at[6 + b]) for b in range(2)]
        bc = [pltpu.make_async_copy(w_in_ref.at[l, pl.ds(src, n), :], wbc.at[pl.ds(dst, n), :], wsem.at[sem]) for src, n, dst, sem in ((2 * D_INNER, 128, 0, 8), (2 * D_INNER + 256, HEADS, 128, 9), (2 * D_INNER + 128, 128, 256, 10))]
        oc = pltpu.make_async_copy(w_out_ref.at[l], wout, wsem.at[11])
        return xc, bc, oc

    def z_copy(l, n):
        rows = pl.ds(pl.multiple_of(512 * n, 16), 512)
        return pltpu.make_async_copy(w_in_ref.at[l, rows, :], wz.at[rows, :], wsem.at[n])

    params = [pltpu.make_async_copy(src, dst, psem.at[i]) for i, (src, dst) in enumerate(((resid_hbm, r_out), (pre_hbm, pre_ref), (cw_hbm, cw_ref), (cb_hbm, cb_ref), (dtb_hbm, dtb_ref), (alog_hbm, alog_ref), (dskip_hbm, dskip_ref), (gw_hbm, gw_ref)))]
    xc0, bc0, oc0 = weight_copies(0)
    params[0].start()
    params[1].start()
    z_copy(0, 0).start()
    for c in params[2:]:
        c.start()
    for n in range(1, 6):
        z_copy(0, n).start()

    barrier = pltpu.get_barrier_semaphore()
    for step in range(1, 4):
        pl.semaphore_signal(barrier, inc=1, device_id={'sp': (me + step) % 4}, device_id_type=pl.DeviceIdType.MESH)

    hbuf[:, 0:HALO, :] = jnp.zeros((LAYERS * NB, HALO, D_MODEL), BF16)
    wbc[176:256, :] = jnp.zeros((80, D_MODEL), BF16)
    prm[...] = jnp.zeros((8, 128), F32)
    for c in bc0 + xc0:
        c.start()
    rows_i = lax.broadcasted_iota(jnp.int32, (BLK, 64), 0)
    for i in range(24):
        h = head_row(i)
        hit = (rows_i == h) | (rows_i == h + 40) | (rows_i == h + 80)
        spread[:, 64 * i:64 * (i + 1)] = jnp.where(hit, 1.0, 0.0).astype(BF16)

    with jax.named_scope('params'):
        for c in params[:2]:
            c.wait()
    with jax.named_scope('barrier'):
        pl.semaphore_wait(barrier, 3)

    own_row = pl.multiple_of(HALO + BLK * chip + SEG * core, 16)
    oth_row = pl.multiple_of(HALO + BLK * (1 - chip) + SEG * core, 16)
    own_blk = pl.multiple_of(BLK * chip, 16)
    oth_blk = pl.multiple_of(BLK * (1 - chip), 16)

    iota_r = lax.broadcasted_iota(jnp.int32, (BLK, BLK), 0)
    iota_c = lax.broadcasted_iota(jnp.int32, (BLK, BLK), 1)

    def remote(src, dst, ssem, rsem, dev):
        return pltpu.make_async_remote_copy(src_ref=src, dst_ref=dst, send_sem=ssem, recv_sem=rsem, device_id={'sp': dev}, device_id_type=pl.DeviceIdType.MESH)

    tri = (iota_r >= iota_c).astype(F32)
    low = iota_c < 64

    def hslice(l, p0, n, row, size):
        return hbuf.at[pl.ds(NB * l + p0, n), pl.ds(row, size), :]

    def same(l, idx, p0, n, row, size, dev):
        ref = hslice(l, p0, n, row, size)
        return remote(ref, ref, hsend.at[l, idx], hrecv.at[l, idx], dev)

    def c_par(l):
        return same(l, 0, 0, NB, own_row, SEG, partner)

    def c_tail(l):
        return same(l, 1, 0, NB, own_row + 48, 16, other)

    def c_half(l, half, size):
        return same(l, 2 + half, 2 * half, 2, own_row, size, other)

    def f_tail(l):
        return same(l, 4, 0, NB, oth_row + 48, 16, partner)

    def f_half(l, half, size):
        return same(l, 5 + half, 2 * half, 2, oth_row, size, partner)

    def by_core(fn):
        @pl.when(core == 0)
        def _():
            fn(64)

        @pl.when(core == 1)
        def _():
            fn(48)

    def wait_half(l, half):
        by_core(lambda n: f_half(l, half, 112 - n).wait_recv())

    def y_copy(l, p):
        src = ybuf.at[p, pl.ds(pl.multiple_of(SEG * (1 - core), 16), SEG), :]
        return remote(src, yrecv.at[NB * l + p], ysend.at[l, p], yrecv_sem.at[l, p], partner)

    def tail_copy(l):
        return pltpu.make_async_copy(tails.at[l], tail_out.at[l], tout.at[l])

    def tail_copies(l):
        res = []
        for b in range(2):
            ref = tails.at[l, :, :, pl.ds(pl.multiple_of(LOC * b + HALF * core, 128), HALF)]
            res.append(remote(ref, ref, tsend.at[l, b], trecv.at[l, b], partner))
        return res

    def conv_chunk(act, src, first, groups, i, p, dst):
        for g in range(groups):
            cols = slice(dst + 128 * g, dst + 128 * (g + 1))
            acc = cwl[0:1, cols] * src[first + g, i, 13:141, :]
            for k in range(1, 4):
                acc = acc + cwl[k:k + 1, cols] * src[first + g, i, 13 + k:141 + k, :]
            act[p, :, cols] = silu(acc + cwl[4:5, cols]).astype(BF16)

    def block(l, p0, np_, row, act, tail, cum, dts, trans, with_c, widths):
        def project(w, rows, dst):
            lhs = hbuf[pl.ds(NB * l + p0, np_), pl.ds(row, EXT), :].reshape(np_ * EXT, D_MODEL)
            res = round_bf16(dot_nt(lhs, w[rows, :]))
            for g in range((rows.stop - rows.start) // 128):
                dst[g, 0:np_] = res[:, 128 * g:128 * (g + 1)].reshape(np_, EXT, 128)

        def finish_bc(src):
            for i in range(np_):
                p = p0 + i
                for g, dst in ((0, LOC), (2, LOC + 128))[:2 if with_c else 1]:
                    if tail is not None:
                        tail[p, :, dst:dst + 128] = src[g, i, BLK:EXT, :].astype(BF16)
                    conv_chunk(act, src, g, 1, i, p, dst)
                v = src[1, i, HALO:EXT, :] + prm[0:1, :]
                dt = round_bf16(jnp.maximum(v, 0.0) + jnp.log1p(jnp.exp(-jnp.abs(v))))
                logs = dt * prm[1:2, :]
                dt = dt * (1.0 - core_f) + pltpu.roll(dt, 116, 1) * core_f
                logs = logs * (1.0 - core_f) + pltpu.roll(logs, 116, 1) * core_f
                cums = jnp.dot(tri, logs, precision=lax.Precision.HIGHEST, preferred_element_type=F32)
                cum[p] = cums
                dts[p] = dt
                if trans is not None:
                    trans[0][p] = cums.T[0:40]
                    trans[1][p] = dt.T[0:40]

        def finish_x(src, col, n):
            for i in range(np_):
                if tail is not None:
                    for g in range(n // 128):
                        tail[p0 + i, :, col + 128 * g:col + 128 * (g + 1)] = src[g, i, BLK:EXT, :].astype(BF16)
                conv_chunk(act, src, 0, n // 128, i, p0 + i, col)

        project(wbc, slice(0, 384 if with_c else 256), rawa)
        pending, nxt = (lambda: finish_bc(rawa)), rawb
        col = 0
        for n in widths:
            project(wx, slice(col, col + n), nxt)
            pending()
            pending = functools.partial(finish_x, nxt, col, n)
            col += n
            nxt = rawa if nxt is rawb else rawb
        pending()

    def last_rows(l, tail):
        lhs = hbuf[pl.ds(NB * l, NB), ROWS - 16:ROWS, :].reshape(NB * 16, D_MODEL)
        for col in range(0, LOC, 512):
            tail[:, :, col:col + 512] = dot_nt(lhs, wx[col:col + 512, :]).astype(BF16).reshape(NB, 16, 512)
        res = dot_nt(lhs, wbc[...]).astype(BF16).reshape(NB, 16, 384)
        tail[:, :, LOC:LOC + 128] = res[:, :, 0:128]
        tail[:, :, LOC + 128:ACT] = res[:, :, 256:384]

    zero = jnp.zeros((), BF16)

    def split_pair(xp):
        return [jnp.where(low, xp, zero), jnp.where(low, zero, xp)]

    lane = lax.broadcasted_iota(jnp.int32, (BLK, BLK), 1)

    def three_terms(v):
        v = jnp.where(lane < 40, v, 0.0)
        hi = round_bf16(v)
        mid = round_bf16(v - hi)
        return (hi + pltpu.roll(mid, 40, 1) + pltpu.roll((v - hi) - mid, 80, 1)).astype(BF16)

    def weighted(act, p, cols, terms):
        return (act[p, :, cols].astype(F32) * dot(terms, spread[:, cols])).astype(BF16)

    def intra_body(l, p):
        cb = act_o[p, :, LOC + 128:ACT]
        scores = dot_nt(cb, act_o[p, :, LOC:LOC + 128]) * tri
        for j in range(PAIRS):
            mats = []
            for i in (2 * j, 2 * j + 1):
                h = head_row(i)
                col = jnp.broadcast_to(cum_o[p, :, h:h + 1], (BLK, BLK))
                mats.append((jnp.exp(jnp.minimum(col - cumt_o[p, h:h + 1, :], 0.0)) * (scores * dtt_o[p, h:h + 1, :])).astype(BF16))
            xp = act_o[p, :, 128 * j:128 * (j + 1)]
            blk = (0 if j < 6 else 24) + 12 * core + (2 * j) % 12
            dv = jnp.where(low[0:1], dskip_ref[l, blk], dskip_ref[l, blk + 1])
            y = dot(jnp.concatenate(mats, axis=1), jnp.concatenate(split_pair(xp), axis=0)) + dv * xp.astype(F32)
            yloc[p, :, 128 * j:128 * (j + 1)] = y
            ybuf[p, :, 128 * j:128 * (j + 1)] = y.astype(BF16)

    def inter_half(l, half):
        prompts = [(0, 2 * half, rawa), (1, 2 * half + 1, rawb)]
        bts, ends = [], []
        for i, p, _ in prompts:
            cum = cum_r[p]
            bts.append(act_r[p, :, LOC:LOC + 128].astype(F32).T.astype(BF16))
            ends.append(three_terms(dt_r[p] * jnp.exp(cum[127:128, :] - cum)))
        for i, p, _ in prompts:
            for j in range(6):
                cols = slice(256 * j, 256 * (j + 1))
                scaled[i, :, cols] = weighted(act_r, p, cols, ends[i])
        for i, p, states in prompts:
            for j in range(6):
                state = dot(bts[i], scaled[i, :, 256 * j:256 * (j + 1)])
                for k in range(2):
                    states[(2 * j + k) // 4, (2 * j + k) % 4, 0:BLK, :] = state[:, 128 * k:128 * (k + 1)]
        for i, p, states in prompts:
            cf = act_o[p, :, LOC + 128:ACT]
            start = three_terms(jnp.exp(cum_o[p]))
            for j in range(6):
                cols = slice(256 * j, 256 * (j + 1))
                state = jnp.concatenate([states[(2 * j + k) // 4, (2 * j + k) % 4, 0:BLK, :].astype(BF16) for k in range(2)], axis=1)
                y = yloc[p, :, cols] + dot(cf, state) * dot(start, spread[:, cols])
                ybuf[p, :, cols] = y.astype(BF16)
            y_copy(l, p).start()

    def final_inputs(p, buf):
        co, cr = cum_o[p], cum_r[p]
        eo, er = co[127:128, :], cr[127:128, :]
        fo = three_terms(dt_o[p] * jnp.exp(eo - co + er * (1.0 - chip_f)))
        fr = three_terms(dt_r[p] * jnp.exp(er - cr + eo * chip_f))
        for j in range(3):
            cols = pl.ds(pl.multiple_of(HALF * chip + 256 * j, 256), 256)
            buf[:, 256 * j:256 * (j + 1)] = weighted(act_o, p, cols, fo)
            buf[:, HALF + 256 * j:HALF + 256 * (j + 1)] = weighted(act_r, p, cols, fr)

    def final_states(l, p, buf):
        bts = jnp.concatenate([act[p, :, LOC:LOC + 128].astype(F32).T.astype(BF16) for act in (act_o, act_r)], axis=1)
        for j in range(3):
            state = dot(bts, jnp.concatenate([buf[:, 256 * j:256 * (j + 1)], buf[:, HALF + 256 * j:HALF + 256 * (j + 1)]], axis=0))
            ssm_out[p, l, 4 * j:4 * j + 4] = state.T.reshape(4, 64, 128)

    def pass_tail(l):
        c_tail(l).wait_recv()
        f_tail(l).start()

    def pass_half(l, half):
        def go(n):
            c_half(l, half, n).wait_recv()
            f_half(l, half, n).start()
        by_core(go)

    def bulk(l):
        c_half(l, 0, 64).start()
        c_half(l, 1, 64).start()

    def after_other(l, tail):
        for b in range(2):
            tails[l, :, :, pl.ds(pl.multiple_of(LOC * b + HALF * core, 128), HALF)] = tail[:, :, HALF * b:HALF * (b + 1)]
        tails[l, :, :, D_INNER:CONV_DIM] = tail[:, :, LOC:ACT]
        for c in tail_copies(l):
            c.start()

    def finish_tails(l):
        for c in tail_copies(l):
            c.wait()
        tail_copy(l).start()

    def next_weights(l):
        @pl.when(l == 0)
        def _():
            xnx, bnx, _ = weight_copies(1)
            for c in xnx + bnx:
                c.start()

    def begin(l):
        def norm_body(p, c):
            v = r_out[p]
            ms = jnp.mean(v * v, axis=-1, keepdims=True)
            hbuf[NB * l + p, pl.ds(own_row, SEG), :] = (v * lax.rsqrt(ms + EPSILON) * pre_ref[pl.ds(l, 1), :]).astype(BF16)
            return c
        with jax.named_scope('norm'):
            lax.fori_loop(0, NB, norm_body, 0)

        c_par(l).start()

        @pl.when(core == 1)
        def _():
            c_tail(l).start()
            c_half(l, 0, 48).start()
            c_half(l, 1, 48).start()

        @pl.when(jnp.logical_and(core == 0, l > 0))
        def _():
            bulk(l)

        @pl.when(jnp.logical_and(jnp.logical_and(core == 1, chip == 1), l > 0))
        def _():
            pass_tail(l)

    def main(l):
        xc, bc, oc = weight_copies(l)

        def z_chunk(n):
            lhs = hbuf[pl.ds(NB * l, NB), pl.ds(own_row, SEG), :].reshape(NB * SEG, D_MODEL)
            cols = slice(512 * n, 512 * (n + 1)) if isinstance(n, int) else pl.ds(pl.multiple_of(512 * n, 512), 512)
            z = round_bf16(dot_nt(lhs, wz[cols, :]))
            sz[:, :, cols] = silu(z).reshape(NB, SEG, 512)

        def z_group(lo):
            for n in range(lo, lo + 3):
                z_copy(l, n).wait()
            for n in range(lo, lo + 3):
                z_chunk(n)

        with jax.named_scope('zproj'):
            z_group(0)

            @pl.when(jnp.logical_and(core == 0, l == 0))
            def _():
                bulk(l)

            @pl.when(l == 0)
            def _():
                z_group(3)
        oc.start()

        @pl.when(l == 0)
        def _():
            for n in range(6):
                z_copy(1, n).start()

        @pl.when(l == 0)
        def _():
            for c in params[2:]:
                c.wait()

        for b in range(2):
            src = pl.multiple_of(LOC * b + HALF * core, 128)
            cwl[0:4, HALF * b:HALF * (b + 1)] = cw_ref[l, :, pl.ds(src, HALF)]
            cwl[4:5, HALF * b:HALF * (b + 1)] = cb_ref[pl.ds(l, 1), pl.ds(src, HALF)]
        cwl[0:4, LOC:ACT] = cw_ref[l, :, D_INNER:CONV_DIM]
        cwl[4:5, LOC:ACT] = cb_ref[pl.ds(l, 1), D_INNER:CONV_DIM]
        prm[0:1, 0:HEADS] = dtb_ref[pl.ds(l, 1), :]
        prm[1:2, 0:HEADS] = -jnp.exp(alog_ref[pl.ds(l, 1), :])

        with jax.named_scope('wait_h'):
            c_par(l).wait_recv()
            for c in bc + xc:
                c.wait()

            @pl.when(jnp.logical_and(jnp.logical_and(core == 1, chip == 1), l == 0))
            def _():
                pass_tail(l)

            @pl.when(jnp.logical_and(chip == 1, core == 0))
            def _():
                f_tail(l).wait_recv()
        with jax.named_scope('own_block'):
            block(l, 0, NB, own_blk, act_o, tail_o, cum_o, dt_o, (cumt_o, dtt_o), True, (512, 512, 256, 256))

        def intra_end(p):
            @pl.when(chip == 0)
            def _():
                y_copy(l, p).start()

            @pl.when(jnp.logical_and(chip == 1, p == 1))
            def _():
                pass_half(l, 0)

        def intra_plain(p, c):
            intra_body(l, p)
            intra_end(p)
            return c

        def intra_z(p, c):
            z_chunk(3 + p)
            intra_body(l, p)
            intra_end(p)
            return c

        with jax.named_scope('intra'):
            @pl.when(l > 0)
            def _():
                for n in range(3, 6):
                    z_copy(l, n).wait()
            split = jnp.where(l == 0, 0, 3)
            lax.fori_loop(0, split, intra_z, 0)
            lax.fori_loop(split, NB, intra_plain, 0)

        @pl.when(chip == 1)
        def _():
            with jax.named_scope('wait_r0'):
                wait_half(l, 0)

            def half_body(half, c):
                with jax.named_scope('oth_block'):
                    block(l, 2 * half, 2, oth_blk, act_r, None, cum_r, dt_r, None, False, (512, 512, 512))

                @pl.when(jnp.logical_and(half == 0, jnp.logical_or(core == 1, l > 0)))
                def _():
                    with jax.named_scope('wait_c1'):
                        pass_half(l, 1)
                with jax.named_scope('inter'):
                    inter_half(l, half)

                @pl.when(jnp.logical_and(half == 0, l == 0))
                def _():
                    with jax.named_scope('final0'):
                        for i in range(2):
                            final_inputs(i, scaled.at[i])
                        for i in range(2):
                            final_states(l, i, scaled.at[i])

                    @pl.when(core == 0)
                    def _():
                        pass_half(l, 1)

                @pl.when(half == 0)
                def _():
                    with jax.named_scope('wait_f1'):
                        wait_half(l, 1)
                return c
            lax.fori_loop(0, 2, half_body, 0)
            after_other(l, tail_o)
            next_weights(l)

        def gate_body(p, c):
            y_copy(l, p).wait()
            total = jnp.zeros((SEG, 1), F32)
            for b in range(2):
                for own in range(2):
                    cols = pl.ds(pl.multiple_of(LOC * b + HALF * (core if own else 1 - core), 128), HALF)
                    if own:
                        y = ybuf[p, pl.ds(pl.multiple_of(SEG * core, 16), SEG), HALF * b:HALF * (b + 1)]
                    else:
                        y = yrecv[NB * l + p, :, HALF * b:HALF * (b + 1)]
                    g = y.astype(F32) * sz[p, :, cols]
                    sz[p, :, cols] = g
                    total = total + jnp.sum(g * g, axis=-1, keepdims=True)
            scale = lax.rsqrt(total * (1.0 / D_INNER) + EPSILON)
            for b in range(4):
                cols = slice(HALF * b, HALF * (b + 1))
                gn[p, :, cols] = (sz[p, :, cols] * scale * gw_ref[l, :, cols]).astype(BF16)
            return c
        with jax.named_scope('gate'):
            lax.fori_loop(0, NB, gate_body, 0)
            oc.wait()

            @pl.when(chip == 1)
            def _():
                finish_tails(l)

        def out_chunk(n):
            cols = slice(512 * n, 512 * (n + 1))
            o = dot(gn[...].reshape(NB * SEG, D_INNER), wout[:, cols])
            r_out[:, :, cols] = r_out[:, :, cols] + o.reshape(NB, SEG, 512)

        with jax.named_scope('outproj'):
            @pl.when(chip == 0)
            def _():
                for n in range(3):
                    out_chunk(n)

            @pl.when(chip == 1)
            def _():
                @pl.when(l == 0)
                def _():
                    final_inputs(2, ybuf.at[2])
                    final_inputs(3, ybuf.at[3])
                    out_chunk(0)
                    final_states(l, 2, ybuf.at[2])
                    final_states(l, 3, ybuf.at[3])
                    out_chunk(1)
                    out_chunk(2)

                @pl.when(l > 0)
                def _():
                    final_inputs(0, ybuf.at[0])
                    final_inputs(1, ybuf.at[1])
                    out_chunk(0)
                    final_states(l, 0, ybuf.at[0])
                    final_states(l, 1, ybuf.at[1])
                    final_inputs(2, ybuf.at[2])
                    final_inputs(3, ybuf.at[3])
                    out_chunk(1)
                    final_states(l, 2, ybuf.at[2])
                    final_states(l, 3, ybuf.at[3])
                    out_chunk(2)

        @pl.when(chip == 0)
        def _():
            with jax.named_scope('pass_d'):
                @pl.when(core == 1)
                def _():
                    pass_tail(l)
                pass_half(l, 0)

    def deferred(l):
        with jax.named_scope('wait_d'):
            @pl.when(core == 0)
            def _():
                f_tail(l).wait_recv()

        with jax.named_scope('last_rows'):
            last_rows(l, tail_r)
            after_other(l, tail_r)

        def half_body(half, c):
            with jax.named_scope('wait_dh'):
                wait_half(l, half)
            with jax.named_scope('oth_block'):
                block(l, 2 * half, 2, oth_blk, act_r, None, cum_r, dt_r, None, False, (512, 256))

            @pl.when(jnp.logical_and(half == 0, l == 0))
            def _():
                pass_half(l, 1)

            @pl.when(half == 1)
            def _():
                next_weights(l)
                finish_tails(l)

            with jax.named_scope('final'):
                for i in range(2):
                    final_inputs(2 * half + i, ybuf.at[2 * half + i])
                for i in range(2):
                    final_states(l, 2 * half + i, ybuf.at[2 * half + i])

            @pl.when(jnp.logical_and(half == 0, l > 0))
            def _():
                with jax.named_scope('wait_c1'):
                    pass_half(l, 1)
            return c
        lax.fori_loop(0, 2, half_body, 0)

    def step(l, carry):
        @pl.when(l < LAYERS)
        def _():
            begin(l)

        @pl.when(jnp.logical_and(chip == 0, l > 0))
        def _():
            deferred(l - 1)

        @pl.when(l < LAYERS)
        def _():
            main(l)
        return carry

    lax.fori_loop(0, LAYERS + 1, step, 0)
    for l in range(LAYERS):
        c_par(l).wait_send()

        @pl.when(core == 1)
        def _():
            c_tail(l).wait_send()
            f_tail(l).wait_send()

        def sent(n):
            for half in range(2):
                c_half(l, half, n).wait_send()
                f_half(l, half, n).wait_send()
        by_core(sent)
        tail_copy(l).wait()


def copy_kernel(r_ref, ssm_ref, tail_ref, r_out, ssm_out, conv_out, cbuf, sems):
    whole = [pltpu.make_async_copy(r_ref, r_out, sems.at[0]), pltpu.make_async_copy(ssm_ref, ssm_out, sems.at[1])]
    for c in whole:
        c.start()
    for p in range(NB):
        for l in range(LAYERS):
            rows = tail_ref[l, p].astype(F32)
            for k in range(3):
                cbuf[p, k, l:l + 1, :] = rows[13 + k:14 + k, :].astype(BF16)
    store = pltpu.make_async_copy(cbuf, conv_out, sems.at[2])
    store.start()
    for c in whole + [store]:
        c.wait()


def solution(mesh):
    hbm = pl.BlockSpec(memory_space=pl.ANY)
    vmem = pl.BlockSpec(memory_space=pltpu.VMEM)

    def forward(resid, pre_norm, w_in, conv_w, conv_b, dt_bias, a_log, d_skip, gate_norm, w_out):
        r, ssm, tails = pl.pallas_call(
            kernel,
            out_shape=(
                pltpu.VMEM((NB, SEG, D_MODEL), F32),
                pltpu.VMEM((NB, LAYERS, 12, 64, 128), F32),
                pltpu.VMEM((LAYERS, NB, 16, CONV_DIM), BF16),
            ),
            in_specs=[hbm] * 10,
            out_specs=(vmem, vmem, hbm),
            scratch_shapes=[
                pltpu.VMEM((LAYERS, D_MODEL), F32),
                pltpu.VMEM((LAYERS, 4, CONV_DIM), F32),
                pltpu.VMEM((LAYERS, CONV_DIM), F32),
                pltpu.VMEM((LAYERS, HEADS), F32),
                pltpu.VMEM((LAYERS, HEADS), F32),
                pltpu.SMEM((LAYERS, HEADS), F32),
                pltpu.VMEM((LAYERS, 1, D_INNER), F32),
                pltpu.VMEM((LAYERS * NB, ROWS, D_MODEL), BF16),
                pltpu.VMEM((NB, SEG, D_INNER), F32),
                pltpu.VMEM((D_INNER, D_MODEL), BF16),
                pltpu.VMEM((LOC, D_MODEL), BF16),
                pltpu.VMEM((384, D_MODEL), BF16),
                pltpu.VMEM((D_INNER, D_MODEL), BF16),
                pltpu.VMEM((4, NB, EXT, 128), F32),
                pltpu.VMEM((4, NB, EXT, 128), F32),
                pltpu.VMEM((BLK, LOC), BF16),
                pltpu.VMEM((2, BLK, LOC), BF16),
                pltpu.VMEM((NB, BLK, ACT), BF16),
                pltpu.VMEM((NB, BLK, ACT), BF16),
                pltpu.VMEM((NB, BLK, LOC), F32),
                pltpu.VMEM((NB, BLK, LOC), BF16),
                pltpu.VMEM((LAYERS * NB, SEG, LOC), BF16),
                pltpu.VMEM((NB, SEG, D_INNER), BF16),
                pltpu.VMEM((LAYERS, NB, 16, CONV_DIM), BF16),
                pltpu.VMEM((NB, 16, ACT), BF16),
                pltpu.VMEM((NB, 16, ACT), BF16),
                pltpu.VMEM((NB, BLK, BLK), F32),
                pltpu.VMEM((NB, BLK, BLK), F32),
                pltpu.VMEM((NB, BLK, BLK), F32),
                pltpu.VMEM((NB, BLK, BLK), F32),
                pltpu.VMEM((NB, 40, BLK), F32),
                pltpu.VMEM((NB, 40, BLK), F32),
                pltpu.VMEM((8, ACT), F32),
                pltpu.VMEM((8, 128), F32),
                pltpu.SemaphoreType.DMA((12,)),
                pltpu.SemaphoreType.DMA((LAYERS, 7)),
                pltpu.SemaphoreType.DMA((LAYERS, 7)),
                pltpu.SemaphoreType.DMA((LAYERS, NB)),
                pltpu.SemaphoreType.DMA((LAYERS, NB)),
                pltpu.SemaphoreType.DMA((LAYERS, 2)),
                pltpu.SemaphoreType.DMA((LAYERS, 2)),
                pltpu.SemaphoreType.DMA((8,)),
                pltpu.SemaphoreType.DMA((LAYERS,)),
            ],
            compiler_params=pltpu.CompilerParams(collective_id=0, has_side_effects=True, vmem_limit_bytes=VMEM_LIMIT),
        )(resid, pre_norm, jnp.swapaxes(w_in, 1, 2), jnp.swapaxes(conv_w, 1, 2), conv_b, dt_bias, a_log, d_skip, gate_norm, w_out)
        r, ssm, conv = pl.pallas_call(
            copy_kernel,
            out_shape=(
                jax.ShapeDtypeStruct(r.shape, F32),
                jax.ShapeDtypeStruct(ssm.shape, F32),
                jax.ShapeDtypeStruct((NB, 3, LAYERS, CONV_DIM), BF16),
            ),
            in_specs=[hbm, hbm, vmem],
            out_specs=(hbm, hbm, hbm),
            scratch_shapes=[
                pltpu.VMEM((NB, 3, LAYERS, CONV_DIM), BF16),
                pltpu.SemaphoreType.DMA((3,)),
            ],
            compiler_params=pltpu.CompilerParams(vmem_limit_bytes=4 * 1024 * 1024),
        )(r, ssm, tails)
        return r, ssm, jnp.transpose(conv, (0, 2, 3, 1))

    return jax.shard_map(forward, mesh=mesh, in_specs=(P('dp', 'sp', None), P(), P(), P(), P(), P(), P(), P(), P(), P()), out_specs=(P('dp', 'sp', None), P('dp', None, 'sp', None, None), P('dp', None, None, None)), check_vma=False)
```

```python
import functools

import jax
import jax.numpy as jnp
from jax import lax
from jax.experimental import pallas as pl
from jax.experimental.pallas import tpu as pltpu
from jax.sharding import PartitionSpec as P

F32 = jnp.float32
BF16 = jnp.bfloat16
EPSILON = 1e-5
LAYERS = 2
NB = 4
SEG = 64
BLK = 128
HALO = 16
EXT = BLK + HALO
ROWS = HALO + 2 * BLK
D_MODEL = 1536
D_INNER = 3072
CONV_DIM = 3328
HEADS = 48
HALF = 768
LOC = 1536
ACT = LOC + 256
PAIRS = 12
VMEM_LIMIT = 58400000
NT = (((1,), (1,)), ((), ()))


def dot(a, b):
    return jnp.dot(a, b, preferred_element_type=F32)


def dot_nt(a, b):
    return lax.dot_general(a, b, NT, preferred_element_type=F32)


def round_bf16(v):
    return v.astype(BF16).astype(F32)


def silu(v):
    half = 0.5 * v
    return half * jnp.tanh(half) + half


def head_row(i):
    return i if i < 12 else i + 12


def kernel(resid_hbm, pre_hbm, w_in_ref, cw_hbm, cb_hbm, dtb_hbm, alog_hbm, dskip_hbm, gw_hbm, w_out_ref,
           r_out, ssm_out, tail_out,
           pre_ref, cw_ref, cb_ref, dtb_ref, alog_ref, dskip_ref, gw_ref, hbuf, sz, wz, wx, wbc, wout, rawa, rawb, spread, scaled, act_o, act_r, yloc, ybuf, yrecv, gn, tails, tail_o, tail_r,
           cum_o, cum_r, dt_o, dt_r, cumt_o, dtt_o, cwl, prm,
           wsem, hsend, hrecv, ysend, yrecv_sem, tsend, trecv, psem, tout):
    me = lax.axis_index('sp')
    chip = me // 2
    core = me % 2
    partner = chip * 2 + (1 - core)
    other = (1 - chip) * 2 + core
    chip_f = chip.astype(F32)
    core_f = core.astype(F32)

    def weight_copies(l):
        xc = [pltpu.make_async_copy(w_in_ref.at[l, pl.ds(pl.multiple_of(D_INNER + LOC * b + HALF * core, 16), HALF), :], wx.at[pl.ds(HALF * b, HALF), :], wsem.at[6 + b]) for b in range(2)]
        bc = [pltpu.make_async_copy(w_in_ref.at[l, pl.ds(src, n), :], wbc.at[pl.ds(dst, n), :], wsem.at[sem]) for src, n, dst, sem in ((2 * D_INNER, 128, 0, 8), (2 * D_INNER + 256, HEADS, 128, 9), (2 * D_INNER + 128, 128, 256, 10))]
        oc = pltpu.make_async_copy(w_out_ref.at[l], wout, wsem.at[11])
        return xc, bc, oc

    def z_copy(l, n):
        rows = pl.ds(pl.multiple_of(512 * n, 16), 512)
        return pltpu.make_async_copy(w_in_ref.at[l, rows, :], wz.at[rows, :], wsem.at[n])

    params = [pltpu.make_async_copy(src, dst, psem.at[i]) for i, (src, dst) in enumerate(((resid_hbm, r_out), (pre_hbm, pre_ref), (cw_hbm, cw_ref), (cb_hbm, cb_ref), (dtb_hbm, dtb_ref), (alog_hbm, alog_ref), (dskip_hbm, dskip_ref), (gw_hbm, gw_ref)))]
    xc0, bc0, oc0 = weight_copies(0)
    params[0].start()
    params[1].start()
    z_copy(0, 0).start()
    for c in params[2:]:
        c.start()
    for n in range(1, 6):
        z_copy(0, n).start()

    barrier = pltpu.get_barrier_semaphore()
    for step in range(1, 4):
        pl.semaphore_signal(barrier, inc=1, device_id={'sp': (me + step) % 4}, device_id_type=pl.DeviceIdType.MESH)

    hbuf[:, 0:HALO, :] = jnp.zeros((LAYERS * NB, HALO, D_MODEL), BF16)
    wbc[176:256, :] = jnp.zeros((80, D_MODEL), BF16)
    prm[...] = jnp.zeros((8, 128), F32)
    for c in bc0 + xc0:
        c.start()
    rows_i = lax.broadcasted_iota(jnp.int32, (BLK, 64), 0)
    for i in range(24):
        h = head_row(i)
        hit = (rows_i == h) | (rows_i == h + 40) | (rows_i == h + 80)
        spread[:, 64 * i:64 * (i + 1)] = jnp.where(hit, 1.0, 0.0).astype(BF16)

    with jax.named_scope('params'):
        for c in params[:2]:
            c.wait()
    with jax.named_scope('barrier'):
        pl.semaphore_wait(barrier, 3)

    own_row = pl.multiple_of(HALO + BLK * chip + SEG * core, 16)
    oth_row = pl.multiple_of(HALO + BLK * (1 - chip) + SEG * core, 16)
    own_blk = pl.multiple_of(BLK * chip, 16)
    oth_blk = pl.multiple_of(BLK * (1 - chip), 16)

    iota_r = lax.broadcasted_iota(jnp.int32, (BLK, BLK), 0)
    iota_c = lax.broadcasted_iota(jnp.int32, (BLK, BLK), 1)

    def remote(src, dst, ssem, rsem, dev):
        return pltpu.make_async_remote_copy(src_ref=src, dst_ref=dst, send_sem=ssem, recv_sem=rsem, device_id={'sp': dev}, device_id_type=pl.DeviceIdType.MESH)

    tri = (iota_r >= iota_c).astype(F32)
    low = iota_c < 64

    def hslice(l, p0, n, row, size):
        return hbuf.at[pl.ds(NB * l + p0, n), pl.ds(row, size), :]

    def same(l, idx, p0, n, row, size, dev):
        ref = hslice(l, p0, n, row, size)
        return remote(ref, ref, hsend.at[l, idx], hrecv.at[l, idx], dev)

    def c_par(l):
        return same(l, 0, 0, NB, own_row, SEG, partner)

    def c_tail(l):
        return same(l, 1, 0, NB, own_row + 48, 16, other)

    def c_half(l, half, size):
        return same(l, 2 + half, 2 * half, 2, own_row, size, other)

    def f_tail(l):
        return same(l, 4, 0, NB, oth_row + 48, 16, partner)

    def f_half(l, half, size):
        return same(l, 5 + half, 2 * half, 2, oth_row, size, partner)

    def by_core(fn):
        @pl.when(core == 0)
        def _():
            fn(64)

        @pl.when(core == 1)
        def _():
            fn(48)

    def wait_half(l, half):
        by_core(lambda n: f_half(l, half, 112 - n).wait_recv())

    def y_copy(l, p):
        src = ybuf.at[p, pl.ds(pl.multiple_of(SEG * (1 - core), 16), SEG), :]
        return remote(src, yrecv.at[NB * l + p], ysend.at[l, p], yrecv_sem.at[l, p], partner)

    def tail_copy(l):
        return pltpu.make_async_copy(tails.at[l], tail_out.at[l], tout.at[l])

    def tail_copies(l):
        res = []
        for b in range(2):
            ref = tails.at[l, :, :, pl.ds(pl.multiple_of(LOC * b + HALF * core, 128), HALF)]
            res.append(remote(ref, ref, tsend.at[l, b], trecv.at[l, b], partner))
        return res

    def conv_chunk(act, src, first, groups, i, p, dst):
        for g in range(groups):
            cols = slice(dst + 128 * g, dst + 128 * (g + 1))
            acc = cwl[0:1, cols] * src[first + g, i, 13:141, :]
            for k in range(1, 4):
                acc = acc + cwl[k:k + 1, cols] * src[first + g, i, 13 + k:141 + k, :]
            act[p, :, cols] = silu(acc + cwl[4:5, cols]).astype(BF16)

    def block(l, p0, np_, row, act, tail, cum, dts, trans, with_c, widths):
        def project(w, rows, dst):
            lhs = hbuf[pl.ds(NB * l + p0, np_), pl.ds(row, EXT), :].reshape(np_ * EXT, D_MODEL)
            res = round_bf16(dot_nt(lhs, w[rows, :]))
            for g in range((rows.stop - rows.start) // 128):
                dst[g, 0:np_] = res[:, 128 * g:128 * (g + 1)].reshape(np_, EXT, 128)

        def finish_bc(src):
            for i in range(np_):
                p = p0 + i
                for g, dst in ((0, LOC), (2, LOC + 128))[:2 if with_c else 1]:
                    if tail is not None:
                        tail[p, :, dst:dst + 128] = src[g, i, BLK:EXT, :].astype(BF16)
                    conv_chunk(act, src, g, 1, i, p, dst)
                v = src[1, i, HALO:EXT, :] + prm[0:1, :]
                dt = round_bf16(jnp.maximum(v, 0.0) + jnp.log1p(jnp.exp(-jnp.abs(v))))
                logs = dt * prm[1:2, :]
                dt = dt * (1.0 - core_f) + pltpu.roll(dt, 116, 1) * core_f
                logs = logs * (1.0 - core_f) + pltpu.roll(logs, 116, 1) * core_f
                cums = jnp.dot(tri, logs, precision=lax.Precision.HIGHEST, preferred_element_type=F32)
                cum[p] = cums
                dts[p] = dt
                if trans is not None:
                    trans[0][p] = cums.T[0:40]
                    trans[1][p] = dt.T[0:40]

        def finish_x(src, col, n):
            for i in range(np_):
                if tail is not None:
                    for g in range(n // 128):
                        tail[p0 + i, :, col + 128 * g:col + 128 * (g + 1)] = src[g, i, BLK:EXT, :].astype(BF16)
                conv_chunk(act, src, 0, n // 128, i, p0 + i, col)

        project(wbc, slice(0, 384 if with_c else 256), rawa)
        pending, nxt = (lambda: finish_bc(rawa)), rawb
        col = 0
        for n in widths:
            project(wx, slice(col, col + n), nxt)
            pending()
            pending = functools.partial(finish_x, nxt, col, n)
            col += n
            nxt = rawa if nxt is rawb else rawb
        pending()

    def last_rows(l, tail):
        lhs = hbuf[pl.ds(NB * l, NB), ROWS - 16:ROWS, :].reshape(NB * 16, D_MODEL)
        for col in range(0, LOC, 512):
            tail[:, :, col:col + 512] = dot_nt(lhs, wx[col:col + 512, :]).astype(BF16).reshape(NB, 16, 512)
        res = dot_nt(lhs, wbc[...]).astype(BF16).reshape(NB, 16, 384)
        tail[:, :, LOC:LOC + 128] = res[:, :, 0:128]
        tail[:, :, LOC + 128:ACT] = res[:, :, 256:384]

    zero = jnp.zeros((), BF16)

    def split_pair(xp):
        return [jnp.where(low, xp, zero), jnp.where(low, zero, xp)]

    lane = lax.broadcasted_iota(jnp.int32, (BLK, BLK), 1)

    def three_terms(v):
        v = jnp.where(lane < 40, v, 0.0)
        hi = round_bf16(v)
        mid = round_bf16(v - hi)
        return (hi + pltpu.roll(mid, 40, 1) + pltpu.roll((v - hi) - mid, 80, 1)).astype(BF16)

    def weighted(act, p, cols, terms):
        return (act[p, :, cols].astype(F32) * dot(terms, spread[:, cols])).astype(BF16)

    def intra_body(l, p):
        cb = act_o[p, :, LOC + 128:ACT]
        scores = dot_nt(cb, act_o[p, :, LOC:LOC + 128]) * tri
        for j in range(PAIRS):
            mats = []
            for i in (2 * j, 2 * j + 1):
                h = head_row(i)
                col = jnp.broadcast_to(cum_o[p, :, h:h + 1], (BLK, BLK))
                mats.append((jnp.exp(jnp.minimum(col - cumt_o[p, h:h + 1, :], 0.0)) * (scores * dtt_o[p, h:h + 1, :])).astype(BF16))
            xp = act_o[p, :, 128 * j:128 * (j + 1)]
            blk = (0 if j < 6 else 24) + 12 * core + (2 * j) % 12
            dv = jnp.where(low[0:1], dskip_ref[l, blk], dskip_ref[l, blk + 1])
            y = dot(jnp.concatenate(mats, axis=1), jnp.concatenate(split_pair(xp), axis=0)) + dv * xp.astype(F32)
            yloc[p, :, 128 * j:128 * (j + 1)] = y
            ybuf[p, :, 128 * j:128 * (j + 1)] = y.astype(BF16)

    def inter_half(l, half):
        prompts = [(0, 2 * half, rawa), (1, 2 * half + 1, rawb)]
        bts, ends = [], []
        for i, p, _ in prompts:
            cum = cum_r[p]
            bts.append(act_r[p, :, LOC:LOC + 128].astype(F32).T.astype(BF16))
            ends.append(three_terms(dt_r[p] * jnp.exp(cum[127:128, :] - cum)))
        for i, p, _ in prompts:
            for j in range(6):
                cols = slice(256 * j, 256 * (j + 1))
                scaled[i, :, cols] = weighted(act_r, p, cols, ends[i])
        for i, p, states in prompts:
            for j in range(6):
                state = dot(bts[i], scaled[i, :, 256 * j:256 * (j + 1)])
                for k in range(2):
                    states[(2 * j + k) // 4, (2 * j + k) % 4, 0:BLK, :] = state[:, 128 * k:128 * (k + 1)]
        for i, p, states in prompts:
            cf = act_o[p, :, LOC + 128:ACT]
            start = three_terms(jnp.exp(cum_o[p]))
            for j in range(6):
                cols = slice(256 * j, 256 * (j + 1))
                state = jnp.concatenate([states[(2 * j + k) // 4, (2 * j + k) % 4, 0:BLK, :].astype(BF16) for k in range(2)], axis=1)
                y = yloc[p, :, cols] + dot(cf, state) * dot(start, spread[:, cols])
                ybuf[p, :, cols] = y.astype(BF16)
        for i, p, _ in prompts:
            y_copy(l, p).start()

    def final_inputs(p, buf):
        co, cr = cum_o[p], cum_r[p]
        eo, er = co[127:128, :], cr[127:128, :]
        fo = three_terms(dt_o[p] * jnp.exp(eo - co + er * (1.0 - chip_f)))
        fr = three_terms(dt_r[p] * jnp.exp(er - cr + eo * chip_f))
        for j in range(3):
            cols = pl.ds(pl.multiple_of(HALF * chip + 256 * j, 256), 256)
            buf[:, 256 * j:256 * (j + 1)] = weighted(act_o, p, cols, fo)
            buf[:, HALF + 256 * j:HALF + 256 * (j + 1)] = weighted(act_r, p, cols, fr)

    def final_states(l, p, buf):
        bts = jnp.concatenate([act[p, :, LOC:LOC + 128].astype(F32).T.astype(BF16) for act in (act_o, act_r)], axis=1)
        for j in range(3):
            state = dot(bts, jnp.concatenate([buf[:, 256 * j:256 * (j + 1)], buf[:, HALF + 256 * j:HALF + 256 * (j + 1)]], axis=0))
            ssm_out[p, l, 4 * j:4 * j + 4] = state.T.reshape(4, 64, 128)

    def pass_tail(l):
        c_tail(l).wait_recv()
        f_tail(l).start()

    def pass_half(l, half):
        def go(n):
            c_half(l, half, n).wait_recv()
            f_half(l, half, n).start()
        by_core(go)

    def bulk(l):
        c_half(l, 0, 64).start()
        c_half(l, 1, 64).start()

    def after_other(l, tail):
        for b in range(2):
            tails[l, :, :, pl.ds(pl.multiple_of(LOC * b + HALF * core, 128), HALF)] = tail[:, :, HALF * b:HALF * (b + 1)]
        tails[l, :, :, D_INNER:CONV_DIM] = tail[:, :, LOC:ACT]
        for c in tail_copies(l):
            c.start()

    def finish_tails(l):
        for c in tail_copies(l):
            c.wait()
        tail_copy(l).start()

    def next_weights(l):
        @pl.when(l == 0)
        def _():
            xnx, bnx, _ = weight_copies(1)
            for c in xnx + bnx:
                c.start()

    def begin(l):
        def norm_body(p, c):
            v = r_out[p]
            ms = jnp.mean(v * v, axis=-1, keepdims=True)
            hbuf[NB * l + p, pl.ds(own_row, SEG), :] = (v * lax.rsqrt(ms + EPSILON) * pre_ref[pl.ds(l, 1), :]).astype(BF16)
            return c
        with jax.named_scope('norm'):
            lax.fori_loop(0, NB, norm_body, 0)

        c_par(l).start()

        @pl.when(core == 1)
        def _():
            c_tail(l).start()
            c_half(l, 0, 48).start()
            c_half(l, 1, 48).start()

        @pl.when(jnp.logical_and(core == 0, l > 0))
        def _():
            bulk(l)

        @pl.when(jnp.logical_and(jnp.logical_and(core == 1, chip == 1), l > 0))
        def _():
            pass_tail(l)

    def main(l):
        xc, bc, oc = weight_copies(l)

        def z_chunk(n):
            lhs = hbuf[pl.ds(NB * l, NB), pl.ds(own_row, SEG), :].reshape(NB * SEG, D_MODEL)
            cols = slice(512 * n, 512 * (n + 1)) if isinstance(n, int) else pl.ds(pl.multiple_of(512 * n, 512), 512)
            z = round_bf16(dot_nt(lhs, wz[cols, :]))
            sz[:, :, cols] = silu(z).reshape(NB, SEG, 512)

        def z_group(lo):
            for n in range(lo, lo + 3):
                z_copy(l, n).wait()
            for n in range(lo, lo + 3):
                z_chunk(n)

        with jax.named_scope('zproj'):
            z_group(0)

            @pl.when(jnp.logical_and(core == 0, l == 0))
            def _():
                bulk(l)

            @pl.when(l == 0)
            def _():
                z_group(3)
        oc.start()

        @pl.when(l == 0)
        def _():
            for n in range(6):
                z_copy(1, n).start()

        @pl.when(l == 0)
        def _():
            for c in params[2:]:
                c.wait()

        for b in range(2):
            src = pl.multiple_of(LOC * b + HALF * core, 128)
            cwl[0:4, HALF * b:HALF * (b + 1)] = cw_ref[l, :, pl.ds(src, HALF)]
            cwl[4:5, HALF * b:HALF * (b + 1)] = cb_ref[pl.ds(l, 1), pl.ds(src, HALF)]
        cwl[0:4, LOC:ACT] = cw_ref[l, :, D_INNER:CONV_DIM]
        cwl[4:5, LOC:ACT] = cb_ref[pl.ds(l, 1), D_INNER:CONV_DIM]
        prm[0:1, 0:HEADS] = dtb_ref[pl.ds(l, 1), :]
        prm[1:2, 0:HEADS] = -jnp.exp(alog_ref[pl.ds(l, 1), :])

        with jax.named_scope('wait_h'):
            c_par(l).wait_recv()
            for c in bc + xc:
                c.wait()

            @pl.when(jnp.logical_and(jnp.logical_and(core == 1, chip == 1), l == 0))
            def _():
                pass_tail(l)

            @pl.when(jnp.logical_and(chip == 1, core == 0))
            def _():
                f_tail(l).wait_recv()
        with jax.named_scope('own_block'):
            block(l, 0, NB, own_blk, act_o, tail_o, cum_o, dt_o, (cumt_o, dtt_o), True, (512, 512, 256, 256))

        def intra_end(p):
            @pl.when(chip == 0)
            def _():
                y_copy(l, p).start()

            @pl.when(jnp.logical_and(chip == 1, p == 1))
            def _():
                pass_half(l, 0)

        def intra_plain(p, c):
            intra_body(l, p)
            intra_end(p)
            return c

        def intra_z(p, c):
            z_chunk(3 + p)
            intra_body(l, p)
            intra_end(p)
            return c

        with jax.named_scope('intra'):
            @pl.when(l > 0)
            def _():
                for n in range(3, 6):
                    z_copy(l, n).wait()
            split = jnp.where(l == 0, 0, 3)
            lax.fori_loop(0, split, intra_z, 0)
            lax.fori_loop(split, NB, intra_plain, 0)

        @pl.when(chip == 1)
        def _():
            with jax.named_scope('wait_r0'):
                wait_half(l, 0)

            def half_body(half, c):
                with jax.named_scope('oth_block'):
                    block(l, 2 * half, 2, oth_blk, act_r, None, cum_r, dt_r, None, False, (512, 512, 512))

                @pl.when(jnp.logical_and(half == 0, jnp.logical_or(core == 1, l > 0)))
                def _():
                    with jax.named_scope('wait_c1'):
                        pass_half(l, 1)
                with jax.named_scope('inter'):
                    inter_half(l, half)

                @pl.when(jnp.logical_and(half == 0, l == 0))
                def _():
                    with jax.named_scope('final0'):
                        for i in range(2):
                            final_inputs(i, scaled.at[i])
                        for i in range(2):
                            final_states(l, i, scaled.at[i])

                    @pl.when(core == 0)
                    def _():
                        pass_half(l, 1)

                @pl.when(half == 0)
                def _():
                    with jax.named_scope('wait_f1'):
                        wait_half(l, 1)
                return c
            lax.fori_loop(0, 2, half_body, 0)
            after_other(l, tail_o)
            next_weights(l)

        def gate_body(p, c):
            y_copy(l, p).wait()
            total = jnp.zeros((SEG, 1), F32)
            for b in range(2):
                for own in range(2):
                    cols = pl.ds(pl.multiple_of(LOC * b + HALF * (core if own else 1 - core), 128), HALF)
                    if own:
                        y = ybuf[p, pl.ds(pl.multiple_of(SEG * core, 16), SEG), HALF * b:HALF * (b + 1)]
                    else:
                        y = yrecv[NB * l + p, :, HALF * b:HALF * (b + 1)]
                    g = y.astype(F32) * sz[p, :, cols]
                    sz[p, :, cols] = g
                    total = total + jnp.sum(g * g, axis=-1, keepdims=True)
            scale = lax.rsqrt(total * (1.0 / D_INNER) + EPSILON)
            for b in range(4):
                cols = slice(HALF * b, HALF * (b + 1))
                gn[p, :, cols] = (sz[p, :, cols] * scale * gw_ref[l, :, cols]).astype(BF16)
            return c
        with jax.named_scope('gate'):
            lax.fori_loop(0, NB, gate_body, 0)
            oc.wait()

            @pl.when(chip == 1)
            def _():
                finish_tails(l)

        def out_chunk(n):
            cols = slice(512 * n, 512 * (n + 1))
            o = dot(gn[...].reshape(NB * SEG, D_INNER), wout[:, cols])
            r_out[:, :, cols] = r_out[:, :, cols] + o.reshape(NB, SEG, 512)

        with jax.named_scope('outproj'):
            @pl.when(chip == 0)
            def _():
                for n in range(3):
                    out_chunk(n)

            @pl.when(chip == 1)
            def _():
                @pl.when(l == 0)
                def _():
                    final_inputs(2, ybuf.at[2])
                    final_inputs(3, ybuf.at[3])
                    out_chunk(0)
                    final_states(l, 2, ybuf.at[2])
                    final_states(l, 3, ybuf.at[3])
                    out_chunk(1)
                    out_chunk(2)

                @pl.when(l > 0)
                def _():
                    final_inputs(0, ybuf.at[0])
                    final_inputs(1, ybuf.at[1])
                    out_chunk(0)
                    final_states(l, 0, ybuf.at[0])
                    final_states(l, 1, ybuf.at[1])
                    final_inputs(2, ybuf.at[2])
                    final_inputs(3, ybuf.at[3])
                    out_chunk(1)
                    final_states(l, 2, ybuf.at[2])
                    final_states(l, 3, ybuf.at[3])
                    out_chunk(2)

        @pl.when(chip == 0)
        def _():
            with jax.named_scope('pass_d'):
                @pl.when(core == 1)
                def _():
                    pass_tail(l)
                pass_half(l, 0)

    def deferred(l):
        with jax.named_scope('wait_d'):
            @pl.when(core == 0)
            def _():
                f_tail(l).wait_recv()

        with jax.named_scope('last_rows'):
            last_rows(l, tail_r)
            after_other(l, tail_r)

        def half_body(half, c):
            with jax.named_scope('wait_dh'):
                wait_half(l, half)
            with jax.named_scope('oth_block'):
                block(l, 2 * half, 2, oth_blk, act_r, None, cum_r, dt_r, None, False, (512, 256))

            @pl.when(jnp.logical_and(half == 0, l == 0))
            def _():
                pass_half(l, 1)

            @pl.when(half == 1)
            def _():
                next_weights(l)
                finish_tails(l)

            with jax.named_scope('final'):
                for i in range(2):
                    final_inputs(2 * half + i, ybuf.at[2 * half + i])
                for i in range(2):
                    final_states(l, 2 * half + i, ybuf.at[2 * half + i])

            @pl.when(jnp.logical_and(half == 0, l > 0))
            def _():
                with jax.named_scope('wait_c1'):
                    pass_half(l, 1)
            return c
        lax.fori_loop(0, 2, half_body, 0)

    def step(l, carry):
        @pl.when(l < LAYERS)
        def _():
            begin(l)

        @pl.when(jnp.logical_and(chip == 0, l > 0))
        def _():
            deferred(l - 1)

        @pl.when(l < LAYERS)
        def _():
            main(l)
        return carry

    lax.fori_loop(0, LAYERS + 1, step, 0)
    for l in range(LAYERS):
        c_par(l).wait_send()

        @pl.when(core == 1)
        def _():
            c_tail(l).wait_send()
            f_tail(l).wait_send()

        def sent(n):
            for half in range(2):
                c_half(l, half, n).wait_send()
                f_half(l, half, n).wait_send()
        by_core(sent)
        tail_copy(l).wait()


def copy_kernel(r_ref, ssm_ref, tail_ref, r_out, ssm_out, conv_out, cbuf, sems):
    whole = [pltpu.make_async_copy(r_ref, r_out, sems.at[0]), pltpu.make_async_copy(ssm_ref, ssm_out, sems.at[1])]
    for c in whole:
        c.start()
    for p in range(NB):
        for l in range(LAYERS):
            rows = tail_ref[l, p].astype(F32)
            for k in range(3):
                cbuf[p, k, l:l + 1, :] = rows[13 + k:14 + k, :].astype(BF16)
    store = pltpu.make_async_copy(cbuf, conv_out, sems.at[2])
    store.start()
    for c in whole + [store]:
        c.wait()


def solution(mesh):
    hbm = pl.BlockSpec(memory_space=pl.ANY)
    vmem = pl.BlockSpec(memory_space=pltpu.VMEM)

    def forward(resid, pre_norm, w_in, conv_w, conv_b, dt_bias, a_log, d_skip, gate_norm, w_out):
        r, ssm, tails = pl.pallas_call(
            kernel,
            out_shape=(
                pltpu.VMEM((NB, SEG, D_MODEL), F32),
                pltpu.VMEM((NB, LAYERS, 12, 64, 128), F32),
                pltpu.VMEM((LAYERS, NB, 16, CONV_DIM), BF16),
            ),
            in_specs=[hbm] * 10,
            out_specs=(vmem, vmem, hbm),
            scratch_shapes=[
                pltpu.VMEM((LAYERS, D_MODEL), F32),
                pltpu.VMEM((LAYERS, 4, CONV_DIM), F32),
                pltpu.VMEM((LAYERS, CONV_DIM), F32),
                pltpu.VMEM((LAYERS, HEADS), F32),
                pltpu.VMEM((LAYERS, HEADS), F32),
                pltpu.SMEM((LAYERS, HEADS), F32),
                pltpu.VMEM((LAYERS, 1, D_INNER), F32),
                pltpu.VMEM((LAYERS * NB, ROWS, D_MODEL), BF16),
                pltpu.VMEM((NB, SEG, D_INNER), F32),
                pltpu.VMEM((D_INNER, D_MODEL), BF16),
                pltpu.VMEM((LOC, D_MODEL), BF16),
                pltpu.VMEM((384, D_MODEL), BF16),
                pltpu.VMEM((D_INNER, D_MODEL), BF16),
                pltpu.VMEM((4, NB, EXT, 128), F32),
                pltpu.VMEM((4, NB, EXT, 128), F32),
                pltpu.VMEM((BLK, LOC), BF16),
                pltpu.VMEM((2, BLK, LOC), BF16),
                pltpu.VMEM((NB, BLK, ACT), BF16),
                pltpu.VMEM((NB, BLK, ACT), BF16),
                pltpu.VMEM((NB, BLK, LOC), F32),
                pltpu.VMEM((NB, BLK, LOC), BF16),
                pltpu.VMEM((LAYERS * NB, SEG, LOC), BF16),
                pltpu.VMEM((NB, SEG, D_INNER), BF16),
                pltpu.VMEM((LAYERS, NB, 16, CONV_DIM), BF16),
                pltpu.VMEM((NB, 16, ACT), BF16),
                pltpu.VMEM((NB, 16, ACT), BF16),
                pltpu.VMEM((NB, BLK, BLK), F32),
                pltpu.VMEM((NB, BLK, BLK), F32),
                pltpu.VMEM((NB, BLK, BLK), F32),
                pltpu.VMEM((NB, BLK, BLK), F32),
                pltpu.VMEM((NB, 40, BLK), F32),
                pltpu.VMEM((NB, 40, BLK), F32),
                pltpu.VMEM((8, ACT), F32),
                pltpu.VMEM((8, 128), F32),
                pltpu.SemaphoreType.DMA((12,)),
                pltpu.SemaphoreType.DMA((LAYERS, 7)),
                pltpu.SemaphoreType.DMA((LAYERS, 7)),
                pltpu.SemaphoreType.DMA((LAYERS, NB)),
                pltpu.SemaphoreType.DMA((LAYERS, NB)),
                pltpu.SemaphoreType.DMA((LAYERS, 2)),
                pltpu.SemaphoreType.DMA((LAYERS, 2)),
                pltpu.SemaphoreType.DMA((8,)),
                pltpu.SemaphoreType.DMA((LAYERS,)),
            ],
            compiler_params=pltpu.CompilerParams(collective_id=0, has_side_effects=True, vmem_limit_bytes=VMEM_LIMIT),
        )(resid, pre_norm, jnp.swapaxes(w_in, 1, 2), jnp.swapaxes(conv_w, 1, 2), conv_b, dt_bias, a_log, d_skip, gate_norm, w_out)
        r, ssm, conv = pl.pallas_call(
            copy_kernel,
            out_shape=(
                jax.ShapeDtypeStruct(r.shape, F32),
                jax.ShapeDtypeStruct(ssm.shape, F32),
                jax.ShapeDtypeStruct((NB, 3, LAYERS, CONV_DIM), BF16),
            ),
            in_specs=[hbm, hbm, vmem],
            out_specs=(hbm, hbm, hbm),
            scratch_shapes=[
                pltpu.VMEM((NB, 3, LAYERS, CONV_DIM), BF16),
                pltpu.SemaphoreType.DMA((3,)),
            ],
            compiler_params=pltpu.CompilerParams(vmem_limit_bytes=4 * 1024 * 1024),
        )(r, ssm, tails)
        return r, ssm, jnp.transpose(conv, (0, 2, 3, 1))

    return jax.shard_map(forward, mesh=mesh, in_specs=(P('dp', 'sp', None), P(), P(), P(), P(), P(), P(), P(), P(), P()), out_specs=(P('dp', 'sp', None), P('dp', None, 'sp', None, None), P('dp', None, None, None)), check_vma=False)
```
